256 devices in a mesh: orb: 128 (over x_lo, z, y, core), grid: 2 (over x_hi).
Axes of the slice: x: 4 (x_hi: 2, x_lo: 2; x = x_hi * 2 + x_lo), y: 4, z: 8, core: 2. Of those that a mesh axis runs over, the one named last changes fastest.
Arguments:
- orbitals: bfloat16 [256, 11520], P('orb', 'grid'), may hold values from -1.5 to 1.5
- occupation: bfloat16 [256], P('orb'), may hold values from 0.29882812 to 1
Outputs:
- potentials: float32 [256, 11520], P('orb', 'grid')
- projectors: float32 [256, 11520], P('orb', 'grid')
The draws below stay inside these ranges and needn't reach their ends.
All inputs are finite; a program needn't handle non-finite values.
Results may differ from the reference program's by a relative error of at most 0.0025.
Values may be sent and summed in bfloat16 or wider, within the bound.
A program may use at most 64 MiB of HBM per device.

```python
import math
import jax
import jax.numpy as jnp
from jax import lax

NX = 20
NY = 24
NZ = 24
NORB = 256
NPTS = 11520


def shard_levels(rng, shape, split, smallest, top_value):
    def one(position, shards_of):
        heights = jax.random.uniform(jax.random.fold_in(jax.random.fold_in(rng, 6), position), (shards_of,), jnp.float32, smallest / len(split), top_value / len(split))
        return jnp.repeat(jnp.exp(heights), shape[position] // shards_of).reshape((-1,) + (1,) * (len(shape) - position - 1))

    factor_of = one(*split[0])
    for cut in split[1:]:
        factor_of = factor_of * one(*cut)
    return factor_of


def centred(own_key, extent, scale, bound, shards=(), held_as=jnp.bfloat16):
    array = jax.random.normal(own_key, extent, jnp.float32) * scale
    if len(shards) > 0:
        array = shard_levels(own_key, extent, shards, -0.22, 0.18) * array
    return jnp.clip(array, min=-bound, max=bound).astype(held_as)


def setup_inputs(seed: int = 0) -> dict:
    key_of = jax.random.split(jax.random.key(seed), 3)
    orbitals = centred(key_of[0], (NORB, NPTS), 0.25, 1.5, ((0, 128), (1, 2)))
    occupation = jnp.clip(0.29882812 + 0.7011719 * jax.random.uniform(key_of[1], (NORB,), jnp.float32) ** shard_levels(key_of[1], (NORB,), ((0, 128),), -0.2, 0.2), 0.29882812, 1.0).astype(jnp.bfloat16)
    return dict(orbitals=orbitals, occupation=occupation)


def hartley_table(length):
    index = jnp.arange(length, dtype=jnp.int32)
    product = index[:, None] * index[None, :] % length
    angle = 2.0 * math.pi / length * product.astype(jnp.float32)
    return (jnp.cos(angle) + jnp.sin(angle)).astype(jnp.bfloat16)

def signed_square(length):
    index = jnp.arange(length, dtype=jnp.int32)
    signed = jnp.where(index <= length // 2, index, index - length).astype(jnp.float32)
    return (2.0 * math.pi * signed / length) ** 2

def coulomb_kernel(size_x, size_y, size_z):
    total = signed_square(size_x)[:, None, None] + signed_square(size_y)[None, :, None] + signed_square(size_z)[None, None, :]
    safe = jnp.where(total > 0, total, 1.0)
    return jnp.where(total > 0, 1.0 / safe, 0.0) / (size_x * size_y * size_z)

def solve_pairs(density, table_x, table_y, table_z, kernel):
    fx = table_x.astype(jnp.float32)
    fy = table_y.astype(jnp.float32)
    fz = table_z.astype(jnp.float32)
    section = jnp.einsum('ax,pxyz->payz', fx, density.astype(jnp.float32)).astype(jnp.bfloat16)
    section = jnp.einsum('by,pxyz->pxbz', fy, section.astype(jnp.float32)).astype(jnp.bfloat16)
    spectrum = jnp.einsum('cz,pxyz->pxyc', fz, section.astype(jnp.float32))
    section = (spectrum * kernel).astype(jnp.bfloat16)
    section = jnp.einsum('cz,pxyz->pxyc', fz, section.astype(jnp.float32)).astype(jnp.bfloat16)
    section = jnp.einsum('by,pxyz->pxbz', fy, section.astype(jnp.float32)).astype(jnp.bfloat16)
    return jnp.einsum('ax,pxyz->payz', fx, section.astype(jnp.float32))

def reference(orbitals, occupation):
    table_x = hartley_table(NX)
    table_y = hartley_table(NY)
    table_z = hartley_table(NZ)
    kernel = coulomb_kernel(NX, NY, NZ)
    source = orbitals.astype(jnp.float32)
    weights = occupation.astype(jnp.float32)
    group = math.gcd(NORB, 32)
    blocks = source.reshape(NORB // group, group, NPTS)
    block_weights = weights.reshape(NORB // group, group)

    def potential_of(target):

        def accumulate(running, inputs):
            block, block_weight = inputs
            density = (target[None, :] * block).astype(jnp.bfloat16).reshape(group, NX, NY, NZ)
            potential = solve_pairs(density, table_x, table_y, table_z, kernel).reshape(group, NPTS)
            return (running - jnp.sum(block_weight[:, None] * potential * block, axis=0), None)
        running, unused = lax.scan(accumulate, jnp.zeros((NPTS,), jnp.float32), (blocks, block_weights))
        return running
    potentials = lax.map(potential_of, source)
    gram = lax.dot_general(source, potentials, (((1,), (1,)), ((), ())), precision=lax.Precision.HIGHEST) / NPTS
    factor = jnp.linalg.cholesky(-gram)
    inverse = lax.linalg.triangular_solve(factor, jnp.eye(NORB, dtype=jnp.float32), left_side=True, lower=True)
    projectors = jnp.dot(inverse, potentials, precision=lax.Precision.HIGHEST)
    return (potentials, projectors)
```

```python
import functools
import math

import jax
import jax.numpy as jnp
import numpy as np
from jax import lax
from jax.experimental import pallas as pl
from jax.experimental.pallas import tpu as pltpu
from jax.sharding import Mesh
from jax.sharding import PartitionSpec as P

NX = 20
NY = 24
NZ = 24
NORB = 256
NPTS = 11520
HALF = NPTS // 2
MODES = 512
ROWS = 384
AXES = ("xl", "z", "y", "c", "h")
ORB = ("xl", "z", "y", "c")
MESH = pl.DeviceIdType.MESH
F32 = jnp.float32
BF16 = jnp.bfloat16


def rounded(a):
    return np.asarray(a, np.float32).astype(jnp.bfloat16).astype(np.float32)


def hartley_table(length):
    index = np.arange(length)
    angle = 2.0 * math.pi / length * (index[:, None] * index[None, :] % length)
    return rounded(np.cos(angle) + np.sin(angle))


def signed_square(length):
    index = np.arange(length)
    signed = np.where(index <= length // 2, index, index - length)
    return (2.0 * math.pi * signed / length) ** 2


def coulomb_kernel():
    total = (
        signed_square(NX)[:, None, None]
        + signed_square(NY)[None, :, None]
        + signed_square(NZ)[None, None, :]
    )
    return np.where(total > 0, 1.0 / np.where(total > 0, total, 1.0), 0.0) / NPTS


def two_parts(a):
    high = rounded(a)
    return high, rounded(a - high)


def tables():
    cx, cy, cz = hartley_table(NX), hartley_table(NY), hartley_table(NZ)
    kernel = coulomb_kernel()
    ac = NX * NZ
    tx = np.zeros((128, MODES), np.float32)
    tx[:NX, :ac] = np.repeat(cx, NZ, axis=1)
    tz = np.zeros((128, MODES), np.float32)
    tz[:NZ, :ac] = np.tile(cz, (1, NX))
    ty = np.zeros((128, 128), np.float32)
    tk = np.zeros((128, MODES), np.float32)
    k_high, k_low = two_parts(kernel.transpose(1, 0, 2).reshape(NY, ac))
    for at, part in ((0, k_high), (32, k_high), (64, k_low)):
        ty[:NY, at : at + NY] = cy
        tk[at : at + NY, :ac] = part
    phi = np.einsum("ax,cz->acxz", cx, cz).reshape(ac, NX, NZ)
    right = np.zeros((MODES, 2, 256), np.float32)
    for h in range(2):
        right[:ac, h, :240] = phi[:, 10 * h : 10 * h + 10].reshape(ac, 240)
    r_high, r_low = two_parts(right.reshape(MODES, 512))
    bf = lambda a: jnp.asarray(a, BF16)
    return bf(tx), bf(tz), bf(ty), bf(tk), bf(r_high), bf(r_low), jnp.asarray(ty[:32], F32)


def permutations():
    true = np.arange(NORB).reshape(2, 8, 8, 2)
    order_a = true.transpose(0, 2, 1, 3).reshape(-1)
    order_b = true.transpose(1, 0, 2, 3).reshape(-1)
    eye = np.eye(NORB, dtype=np.float32)
    return tuple(jnp.asarray(eye[:, o], BF16) for o in (order_a, order_b))


def split2(a):
    high = a.astype(BF16)
    return high, (a - high.astype(F32)).astype(BF16)


def dot(a, b, dims=(1, 0)):
    return lax.dot_general(
        a, b, (((dims[0],), (dims[1],)), ((), ())), preferred_element_type=F32
    )


def me():
    return tuple(lax.axis_index(a) for a in AXES)


def of_plane(pid, z):
    return ((pid // 8) % 2, z, (pid // 2) % 4, pid % 2, pid // 16)


def copy(src, dst, send_sem, recv_sem, device):
    return pltpu.make_async_remote_copy(
        src_ref=src, dst_ref=dst, send_sem=send_sem, recv_sem=recv_sem,
        device_id=device, device_id_type=MESH,
    )


def rows(start, size):
    return pl.ds(pl.multiple_of(start, size), size)


def each(count, body):
    lax.fori_loop(0, count, lambda i, carry: (body(i), carry)[1], 0)


def gather_kernel(s1, s2, o1, o2, r1, r2, za_s, za_r, pa_s, pa_r, pg_s, pg_r, zg_s, zg_r):
    xl, z, y, c, h = me()
    p = xl * 8 + y * 2 + c
    pid = h * 16 + p

    z_dev = lambda t: (xl, t, y, c, h)
    half_dev = lambda t: of_plane(h * 16 + t, z)
    plane_dev = lambda t: of_plane(t, z)
    z_peer = lambda d: (z + d) % 8
    p_peer = lambda d: (p + d) % 16
    pid_peer = lambda d: (pid + d) % 32

    barrier = pltpu.get_barrier_semaphore()

    def hello(dev):
        pl.semaphore_signal(barrier, inc=1, device_id=dev, device_id_type=MESH)

    each(7, lambda d: hello(z_dev(z_peer(d + 1))))
    each(31, lambda d: hello(plane_dev(pid_peer(d + 1))))
    pl.semaphore_wait(barrier, 38)

    def z_send(t):
        return copy(s1.at[t], r1.at[rows(z * 16, 16)], za_s.at[t], za_r.at[z], z_dev(t))

    def z_recv(t):
        return copy(s1.at[t], r1.at[rows(t * 16, 16)], za_s.at[t], za_r.at[t], z_dev(t))

    def p_send(t):
        return copy(s2.at[t], r2.at[rows(p * 8, 8)], pa_s.at[t], pa_r.at[p], half_dev(t))

    def p_recv(t):
        return copy(s2.at[t], r2.at[rows(t * 8, 8)], pa_s.at[t], pa_r.at[t], half_dev(t))

    each(7, lambda d: z_send(z_peer(d + 1)).start())
    each(15, lambda d: p_send(p_peer(d + 1)).start())
    r1[rows(z * 16, 16)] = s1[z]
    r2[rows(p * 8, 8)] = s2[p]
    each(7, lambda d: z_recv(z_peer(d + 1)).wait_recv())
    for t in range(3):
        o1[h, rows(p * 16, 16), t * 256 : (t + 1) * 256] = jnp.concatenate(
            [r1[pl.ds(2 * t + k, 16, stride=8), :] for k in range(2)], axis=1
        ).astype(BF16)

    def g_send(t):
        mine = o1.at[h, rows(p * 16, 16)]
        return copy(mine, mine, pg_s.at[t], pg_r.at[pid], plane_dev(t))

    def g_recv(t):
        theirs = o1.at[t // 16, rows((t % 16) * 16, 16)]
        return copy(theirs, theirs, pg_s.at[t], pg_r.at[t], plane_dev(t))

    each(31, lambda d: g_send(pid_peer(d + 1)).start())
    each(15, lambda d: p_recv(p_peer(d + 1)).wait_recv())
    for k in range(4):
        o2[z, :, k * 128 : (k + 1) * 128] = r2[pl.ds(k, 32, stride=4), :].astype(BF16)

    def zg_send(t):
        return copy(o2.at[z], o2.at[z], zg_s.at[t], zg_r.at[z], z_dev(t))

    def zg_recv(t):
        return copy(o2.at[t], o2.at[t], zg_s.at[t], zg_r.at[t], z_dev(t))

    each(7, lambda d: zg_send(z_peer(d + 1)).start())
    each(7, lambda d: zg_recv(z_peer(d + 1)).wait_recv())
    each(31, lambda d: g_recv(pid_peer(d + 1)).wait_recv())
    each(7, lambda d: z_send(z_peer(d + 1)).wait_send())
    each(15, lambda d: p_send(p_peer(d + 1)).wait_send())
    each(31, lambda d: g_send(pid_peer(d + 1)).wait_send())
    each(7, lambda d: zg_send(z_peer(d + 1)).wait_send())


def potential_kernel(where, o1, o2, perm_a, perm_b, tx, tz, ty, tk, rh, rl, cy, v_out, g_out, green):
    p, h, z = where[0], where[1], where[2]
    row = lax.broadcasted_iota(jnp.int32, (ROWS, 128), 0)
    lane = lax.broadcasted_iota(jnp.int32, (ROWS, 128), 1)

    def over(a, n):
        return ((a.astype(F32) + 0.5) * (1.0 / n)).astype(jnp.int32)

    zz = over(row, 48)
    s = row - zz * 48
    cell = h * HALF + s * 128 + zz * 16 + p
    x = over(cell, NY * NZ)
    yz = cell - x * (NY * NZ)
    y = over(yz, NZ)
    z_cell = yz - y * NZ
    x = jnp.where(s < 45, x, 127)
    hot = lambda a: jnp.where(a == lane, 1.0, 0.0).astype(BF16)
    left = dot(hot(x), tx[...]) * dot(hot(z_cell), tz[...])
    y_rows = dot(hot(y), ty[...])
    middle = (lane >= 32) & (lane < 64)
    for t in range(3):
        q = y_rows * cy[pl.ds(z * 3 + t, 1), :]
        q_high, q_low = split2(q)
        mix = jnp.where(middle, q_low.astype(F32), q_high.astype(F32)).astype(BF16)
        l_high, l_low = split2(left * dot(mix, tk[...]))
        g = dot(l_high, rh[...]) + dot(l_low, rh[...]) + dot(l_high, rl[...])
        for hh in range(2):
            green[hh, :, t * 256 : (t + 1) * 256] = g[:, hh * 256 : (hh + 1) * 256]

    o_rows = dot(perm_b[...], o2[...])
    occ = o_rows[:, ROWS:]
    o_rows = o_rows[:, :ROWS]
    w = jnp.concatenate([o_rows[:, k * 128 : (k + 1) * 128] * occ for k in range(3)], axis=1)
    w = w.astype(BF16).T
    v = jnp.zeros((ROWS, NORB), F32)
    for hh in range(2):
        orb = dot(perm_a[...], o1[hh]).astype(BF16)
        m_high, m_low = split2(green[hh] * dot(w, orb))
        v = v + dot(m_high, orb, (1, 1)) + dot(m_low, orb, (1, 1))
    v_out[...] = v
    v_high, v_low = split2(v)
    o_b = o_rows.astype(BF16)
    g_out[...] = (dot(o_b, v_high) + dot(o_b, v_low)) * (1.0 / NPTS)


def reduce_kernel(gp, v, gram, vs, rg, rv, s8, rz, ga_s, ga_r, va_s, va_r, gz_s, gz_r, gg_s, gg_r):
    xl, z, y, c, h = me()
    pid = h * 16 + xl * 8 + y * 2 + c
    z_dev = lambda t: (xl, t, y, c, h)
    plane_dev = lambda t: of_plane(t, z)
    z_peer = lambda d: (z + d) % 8
    pid_peer = lambda d: (pid + d) % 32
    barrier = pltpu.get_barrier_semaphore()

    def hello(dev):
        pl.semaphore_signal(barrier, inc=1, device_id=dev, device_id_type=MESH)

    each(7, lambda d: hello(z_dev(z_peer(d + 1))))
    each(31, lambda d: hello(plane_dev(pid_peer(d + 1))))
    pl.semaphore_wait(barrier, 38)

    def a_send(t):
        return copy(gp.at[rows(t * 8, 8)], rg.at[pid], ga_s.at[t], ga_r.at[pid], plane_dev(t))

    def a_recv(t):
        return copy(gp.at[rows(t * 8, 8)], rg.at[t], ga_s.at[t], ga_r.at[t], plane_dev(t))

    def v_send(t):
        return copy(v.at[rows(t * 48, 48)], rv.at[z], va_s.at[t], va_r.at[z], z_dev(t))

    def v_recv(t):
        return copy(v.at[rows(t * 48, 48)], rv.at[t], va_s.at[t], va_r.at[t], z_dev(t))

    each(31, lambda d: a_send(pid_peer(d + 1)).start())
    each(7, lambda d: v_send(z_peer(d + 1)).start())
    rg[pid] = gp[rows(pid * 8, 8)]
    rv[z] = v[rows(z * 48, 48)]
    each(31, lambda d: a_recv(pid_peer(d + 1)).wait_recv())
    s8[...] = jnp.sum(rg[...], axis=0)
    rz[z] = s8[...]

    def z_send(t):
        return copy(s8, rz.at[z], gz_s.at[t], gz_r.at[z], z_dev(t))

    def z_recv(t):
        return copy(s8, rz.at[t], gz_s.at[t], gz_r.at[t], z_dev(t))

    each(7, lambda d: z_send(z_peer(d + 1)).start())
    each(7, lambda d: z_recv(z_peer(d + 1)).wait_recv())
    gram[rows(pid * 8, 8)] = jnp.sum(rz[...], axis=0)

    def g_send(t):
        mine = gram.at[rows(pid * 8, 8)]
        return copy(mine, mine, gg_s.at[t], gg_r.at[pid], plane_dev(t))

    def g_recv(t):
        theirs = gram.at[rows(t * 8, 8)]
        return copy(theirs, theirs, gg_s.at[t], gg_r.at[t], plane_dev(t))

    each(31, lambda d: g_send(pid_peer(d + 1)).start())
    each(7, lambda d: v_recv(z_peer(d + 1)).wait_recv())
    vs[...] = -jnp.sum(rv[...], axis=0)
    each(31, lambda d: g_recv(pid_peer(d + 1)).wait_recv())
    each(31, lambda d: a_send(pid_peer(d + 1)).wait_send())
    each(7, lambda d: v_send(z_peer(d + 1)).wait_send())
    each(7, lambda d: z_send(z_peer(d + 1)).wait_send())
    each(31, lambda d: g_send(pid_peer(d + 1)).wait_send())


def factor_kernel(gram, vs, dv, dq, work, left):
    a = gram[...]
    work[...] = (a + a.T) * 0.5
    sub = lax.broadcasted_iota(jnp.int32, (8, 128), 0)
    lane = lax.broadcasted_iota(jnp.int32, (8, 128), 1)
    wide = lambda col: jnp.broadcast_to(col, (8, 128))
    for k in range(8):
        base = 32 * k
        tile, off = base // 128, base % 128
        wk = [
            [work[base + 8 * g : base + 8 * g + 8, 128 * t : 128 * t + 128] for t in range(2)]
            for g in range(4)
        ]
        col = [
            [wide(wk[g][tile][:, off + j : off + j + 1]) if g >= j // 8 else None for g in range(4)]
            for j in range(32)
        ]
        inside = (lane >= off) & (lane < off + 32)
        for g in range(4):
            unit = jnp.where(lane - off == sub + 8 * g, 1.0, 0.0)
            wk[g][tile] = jnp.where(inside, unit, wk[g][tile])
        pivots = [jnp.ones((8, 128), F32) for _ in range(4)]
        for j in range(32):
            gj, sj = j // 8, j % 8
            d = wide(col[j][gj][sj : sj + 1, :])
            pivots[gj] = jnp.where(sub == sj, d, pivots[gj])
            r = 1.0 / d
            m = [None] * 4
            for g in range(gj, 4):
                m[g] = col[j][g] * r
                if g == gj:
                    m[g] = jnp.where(sub > sj, m[g], 0.0)
            for i in range(j + 1, 32):
                f = wide(col[j][i // 8][i % 8 : i % 8 + 1, :])
                for g in range(i // 8, 4):
                    col[i][g] = col[i][g] - m[g] * f
            for t in range(2):
                line = wide(wk[gj][t][sj : sj + 1, :])
                for g in range(gj, 4):
                    wk[g][t] = wk[g][t] - m[g] * line
        for g in range(4):
            scale = lax.rsqrt(pivots[g])
            for t in range(2):
                wk[g][t] = wk[g][t] * scale
        u = jnp.concatenate([jnp.concatenate(wk[g], axis=1) for g in range(4)], axis=0)
        lanes = lax.broadcasted_iota(jnp.int32, (32, 256), 1)
        work[base : base + 32, :] = jnp.where(lanes < base + 32, u, 0.0)
        if k < 7:
            u_high, u_low = split2(u)
            one = jnp.concatenate([u_high, u_low, u_high], axis=0)
            two = jnp.concatenate([u_high, u_high, u_low], axis=0)
            edge = base + 32
            start = edge // 128 * 128
            change = dot(one[:, start:].T, two)[edge - start :]
            rest = work[edge:, :]
            lanes = lax.broadcasted_iota(jnp.int32, rest.shape, 1)
            rest = jnp.where((lanes >= base) & (lanes < edge), 0.0, rest)
            work[edge:, :] = rest - change

    slab = vs[...]
    gap = jnp.zeros((16, NORB), F32)
    both = jnp.concatenate([slab, gap, slab, gap], axis=0)
    lane8 = lane < 64

    def deal(out):
        for p in range(16):
            base = (p // 8) * 128 + (p % 8) * 2
            even = left[pl.ds(base, 8, stride=16), :]
            odd = left[pl.ds(base + 1, 8, stride=16), :]
            out[p] = jnp.where(lane8, even, odd)

    left[...] = both.T
    deal(dv)
    l_high, l_low = split2(work[...])
    b_high, b_low = split2(both)
    left[...] = (
        dot(l_high, b_high, (1, 1)) + dot(l_low, b_high, (1, 1)) + dot(l_high, b_low, (1, 1))
    )
    deal(dq)


def return_kernel(dv, dq, ov, oq, rp, sz, rz, pa_s, pa_r, za_s, za_r):
    xl, z, y, c, h = me()
    p = xl * 8 + y * 2 + c
    z_dev = lambda t: (xl, t, y, c, h)
    half_dev = lambda t: of_plane(h * 16 + t, z)
    z_peer = lambda d: (z + d) % 8
    p_peer = lambda d: (p + d) % 16
    barrier = pltpu.get_barrier_semaphore()

    def hello(dev):
        pl.semaphore_signal(barrier, inc=1, device_id=dev, device_id_type=MESH)

    each(7, lambda d: hello(z_dev(z_peer(d + 1))))
    each(15, lambda d: hello(half_dev(p_peer(d + 1))))
    pl.semaphore_wait(barrier, 22)

    def p_send(n, t):
        src = (dv, dq)[n]
        return copy(src.at[t], rp.at[n, rows(p * 8, 8)], pa_s.at[n, t], pa_r.at[n, p], half_dev(t))

    def p_recv(n, t):
        src = (dv, dq)[n]
        return copy(src.at[t], rp.at[n, rows(t * 8, 8)], pa_s.at[n, t], pa_r.at[n, t], half_dev(t))

    def z_send(n, t):
        return copy(sz.at[n, t], rz.at[n, rows(z * 16, 16)], za_s.at[n, t], za_r.at[n, z], z_dev(t))

    def z_recv(n, t):
        return copy(sz.at[n, t], rz.at[n, rows(t * 16, 16)], za_s.at[n, t], za_r.at[n, t], z_dev(t))

    for n in range(2):
        each(15, lambda d: p_send(n, p_peer(d + 1)).start())
        rp[n, rows(p * 8, 8)] = (dv, dq)[n][p]
    for n in range(2):
        each(15, lambda d: p_recv(n, p_peer(d + 1)).wait_recv())
        for t in range(8):
            sz[n, t] = rp[n, pl.ds(t, 16, stride=8), :]
        each(7, lambda d: z_send(n, z_peer(d + 1)).start())
        rz[n, rows(z * 16, 16)] = sz[n, z]
    for n in range(2):
        each(7, lambda d: z_recv(n, z_peer(d + 1)).wait_recv())
        out = (ov, oq)[n]
        turned = rz[n].T
        for o in range(2):
            out[o] = turned[64 * o : 64 * o + 48]
    for n in range(2):
        each(15, lambda d: p_send(n, p_peer(d + 1)).wait_send())
        each(7, lambda d: z_send(n, z_peer(d + 1)).wait_send())


VM = pl.BlockSpec(memory_space=pltpu.VMEM)
SM = pl.BlockSpec(memory_space=pltpu.SMEM)
DMA = pltpu.SemaphoreType.DMA


def call(kernel, args, outs, scratch, number=None, name=None, specs=None):
    params = dict(vmem_limit_bytes=60 * 1024 * 1024)
    if number is not None:
        params.update(collective_id=number, has_side_effects=True)
    return pl.pallas_call(
        kernel,
        out_shape=[jax.ShapeDtypeStruct(s, d) for s, d in outs],
        in_specs=specs or [VM] * len(args),
        out_specs=[VM] * len(outs),
        scratch_shapes=scratch,
        compiler_params=pltpu.CompilerParams(**params),
        name=name,
    )(*args)


def on_device(orbitals, occupation):
    xl, z, y, c, h = me()
    own = orbitals.astype(F32)
    s1 = own.reshape(2, 10, 8, 3, NZ).transpose(2, 0, 3, 1, 4).reshape(8, 2, 3, 240)
    s1 = jnp.pad(s1, ((0, 0), (0, 0), (0, 1), (0, 16))).reshape(8, 16, 128)
    s2 = own.reshape(2, 45, 8, 16).transpose(3, 0, 2, 1)
    s2 = jnp.pad(s2, ((0, 0), (0, 0), (0, 0), (0, 3))).reshape(16, 2, ROWS)
    occ = jnp.broadcast_to(occupation.astype(F32)[None, :, None], (16, 2, 128))
    s2 = jnp.concatenate([s2, occ], axis=2).reshape(16, 8, 128)
    o1, o2 = call(
        gather_kernel, (s1, s2),
        (((2, NORB, 768), BF16), ((8, 32, 512), BF16)),
        [pltpu.VMEM((128, 128), F32), pltpu.VMEM((128, 128), F32),
         DMA((8,)), DMA((8,)), DMA((16,)), DMA((16,)), DMA((32,)), DMA((32,)), DMA((8,)), DMA((8,))],
        0, "gather",
    )
    where = jnp.stack([xl * 8 + y * 2 + c, h, z]).astype(jnp.int32)
    v, gp = call(
        potential_kernel,
        (where, o1, o2.reshape(NORB, 512), *permutations(), *tables()),
        (((ROWS, NORB), F32), ((NORB, NORB), F32)),
        [pltpu.VMEM((2, ROWS, 768), F32)],
        name="potential", specs=[SM] + [VM] * 11,
    )
    gram, vs = call(
        reduce_kernel, (gp, v),
        (((NORB, NORB), F32), ((48, NORB), F32)),
        [pltpu.VMEM((32, 8, NORB), F32), pltpu.VMEM((8, 48, NORB), F32), pltpu.VMEM((8, NORB), F32),
         pltpu.VMEM((8, 8, NORB), F32),
         DMA((32,)), DMA((32,)), DMA((8,)), DMA((8,)), DMA((8,)), DMA((8,)), DMA((32,)), DMA((32,))],
        1, "reduce",
    )
    dv, dq = call(
        factor_kernel, (gram, vs),
        (((16, 8, 128), F32), ((16, 8, 128), F32)),
        [pltpu.VMEM((NORB, NORB), F32), pltpu.VMEM((NORB, 128), F32)],
        name="factor",
    )
    ov, oq = call(
        return_kernel, (dv, dq),
        (((2, 48, 128), F32), ((2, 48, 128), F32)),
        [pltpu.VMEM((2, 128, 128), F32), pltpu.VMEM((2, 8, 16, 128), F32), pltpu.VMEM((2, 128, 128), F32),
         DMA((2, 16)), DMA((2, 16)), DMA((2, 8)), DMA((2, 8))],
        2, "give_back",
    )
    return tuple(a[:, :45].reshape(2, HALF) for a in (ov, oq))


def solution(mesh):
    torus = Mesh(mesh.devices.reshape(2, 8, 4, 2, mesh.shape["grid"]), AXES)
    return jax.shard_map(
        on_device,
        mesh=torus,
        in_specs=(P(ORB, "h"), P(ORB)),
        out_specs=(P(ORB, "h"), P(ORB, "h")),
        check_vma=False,
    )
```

```python
import functools
import math

import jax
import jax.numpy as jnp
import numpy as np
from jax import lax
from jax.experimental import pallas as pl
from jax.experimental.pallas import tpu as pltpu
from jax.sharding import Mesh
from jax.sharding import PartitionSpec as P

NX = 20
NY = 24
NZ = 24
NORB = 256
NPTS = 11520
HALF = NPTS // 2
MODES = 512
ROWS = 384
AXES = ("xl", "z", "y", "c", "h")
ORB = ("xl", "z", "y", "c")
MESH = pl.DeviceIdType.MESH
F32 = jnp.float32
BF16 = jnp.bfloat16


def rounded(a):
    return np.asarray(a, np.float32).astype(jnp.bfloat16).astype(np.float32)


def hartley_table(length):
    index = np.arange(length)
    angle = 2.0 * math.pi / length * (index[:, None] * index[None, :] % length)
    return rounded(np.cos(angle) + np.sin(angle))


def signed_square(length):
    index = np.arange(length)
    signed = np.where(index <= length // 2, index, index - length)
    return (2.0 * math.pi * signed / length) ** 2


def coulomb_kernel():
    total = (
        signed_square(NX)[:, None, None]
        + signed_square(NY)[None, :, None]
        + signed_square(NZ)[None, None, :]
    )
    return np.where(total > 0, 1.0 / np.where(total > 0, total, 1.0), 0.0) / NPTS


def two_parts(a):
    high = rounded(a)
    return high, rounded(a - high)


def tables():
    cx, cy, cz = hartley_table(NX), hartley_table(NY), hartley_table(NZ)
    kernel = coulomb_kernel()
    ac = NX * NZ
    tx = np.zeros((128, MODES), np.float32)
    tx[:NX, :ac] = np.repeat(cx, NZ, axis=1)
    tz = np.zeros((128, MODES), np.float32)
    tz[:NZ, :ac] = np.tile(cz, (1, NX))
    ty = np.zeros((128, 128), np.float32)
    tk = np.zeros((128, MODES), np.float32)
    k_high, k_low = two_parts(kernel.transpose(1, 0, 2).reshape(NY, ac))
    for at, part in ((0, k_high), (32, k_high), (64, k_low)):
        ty[:NY, at : at + NY] = cy
        tk[at : at + NY, :ac] = part
    phi = np.einsum("ax,cz->acxz", cx, cz).reshape(ac, NX, NZ)
    right = np.zeros((MODES, 2, 256), np.float32)
    for h in range(2):
        right[:ac, h, :240] = phi[:, 10 * h : 10 * h + 10].reshape(ac, 240)
    r_high, r_low = two_parts(right.reshape(MODES, 512))
    bf = lambda a: jnp.asarray(a, BF16)
    return bf(tx), bf(tz), bf(ty), bf(tk), bf(r_high), bf(r_low), jnp.asarray(ty[:32], F32)


def permutations():
    true = np.arange(NORB).reshape(2, 8, 8, 2)
    order_a = true.transpose(0, 2, 1, 3).reshape(-1)
    order_b = true.transpose(1, 0, 2, 3).reshape(-1)
    eye = np.eye(NORB, dtype=np.float32)
    return tuple(jnp.asarray(eye[:, o], BF16) for o in (order_a, order_b))


def split2(a):
    high = a.astype(BF16)
    return high, (a - high.astype(F32)).astype(BF16)


def dot(a, b, dims=(1, 0)):
    return lax.dot_general(
        a, b, (((dims[0],), (dims[1],)), ((), ())), preferred_element_type=F32
    )


def me():
    return tuple(lax.axis_index(a) for a in AXES)


def of_plane(pid, z):
    return ((pid // 8) % 2, z, (pid // 2) % 4, pid % 2, pid // 16)


def copy(src, dst, send_sem, recv_sem, device):
    return pltpu.make_async_remote_copy(
        src_ref=src, dst_ref=dst, send_sem=send_sem, recv_sem=recv_sem,
        device_id=device, device_id_type=MESH,
    )


def rows(start, size):
    return pl.ds(pl.multiple_of(start, size), size)


def each(count, body):
    lax.fori_loop(0, count, lambda i, carry: (body(i), carry)[1], 0)


def swap(n, i, body):
    each(n - 1, lambda d: body((i + d + 1) % n))


def greet(barrier, n, i, device):
    swap(n, i, lambda t: pl.semaphore_signal(barrier, inc=1, device_id=device(t), device_id_type=MESH))
    return n - 1


def shifted(a, factor, shift):
    return lax.shift_right_logical(a * factor, shift)


def main_kernel(
    s1, s2, perm_a, perm_b, tx, tz, ty, tk, rh, rl, cy, ov, oq,
    o1, o2, r1, r2, green, left, y_rows, v_f, v_b, gp, gc, gh, rg, rv, s8, rz,
    gram, vall, tt, dd, rp,
    za_s, za_r, pa_s, pa_r, cg_s, cg_r, cf_s, cf_r, zg_s, zg_r,
    gc_s, gc_r, ga_s, ga_r, va_s, va_r, gz_s, gz_r, gg_s, gg_r, gf_s, gf_r,
    vg_s, vg_r, d_s, d_r,
):
    xl, z, y, c, h = me()
    p = xl * 8 + y * 2 + c
    q = h * 8 + xl * 4 + y
    z_dev = lambda t: (xl, t, y, c, h)
    half_dev = lambda t: of_plane(h * 16 + t, z)
    chip_dev = lambda t: ((t // 4) % 2, z, t % 4, c, t // 8)
    core_dev = (xl, z, y, 1 - c, h)

    barrier = pltpu.get_barrier_semaphore()
    greeted = greet(barrier, 8, z, z_dev) + greet(barrier, 16, p, half_dev)
    greeted += greet(barrier, 16, q, chip_dev)
    pl.semaphore_signal(barrier, inc=1, device_id=core_dev, device_id_type=MESH)

    row = lax.broadcasted_iota(jnp.int32, (ROWS, 128), 0)
    lane = lax.broadcasted_iota(jnp.int32, (ROWS, 128), 1)
    zz = shifted(row, 1366, 16)
    s = row - zz * 48
    cell = h * HALF + s * 128 + zz * 16 + p
    x = shifted(cell, 7282, 22)
    yz = cell - x * (NY * NZ)
    y_cell = shifted(yz, 2731, 16)
    z_cell = yz - y_cell * NZ
    hot = lambda a: jnp.where(a == lane, 1.0, 0.0).astype(BF16)
    left[...] = dot(hot(jnp.where(s < 45, x, 127)), tx[...]) * dot(hot(z_cell), tz[...])
    y_rows[...] = dot(hot(y_cell), ty[...])
    middle = (lane >= 32) & (lane < 64)

    def green_part(t):
        k_high, k_low = split2(y_rows[...] * cy[pl.ds(z * 3 + t, 1), :])
        mix = jnp.where(middle, k_low.astype(F32), k_high.astype(F32)).astype(BF16)
        l_high, l_low = split2(left[...] * dot(mix, tk[...]))
        g = dot(l_high, rh[...]) + dot(l_low, rh[...]) + dot(l_high, rl[...])
        for hh in range(2):
            green[hh, :, t * 256 : (t + 1) * 256] = g[:, hh * 256 : (hh + 1) * 256]

    pl.semaphore_wait(barrier, greeted + 1)

    def z_send(t):
        return copy(s1.at[t], r1.at[rows(z * 16, 16)], za_s.at[t], za_r.at[z], z_dev(t))

    def z_recv(t):
        return copy(s1.at[t], r1.at[rows(t * 16, 16)], za_s.at[t], za_r.at[t], z_dev(t))

    def p_send(t):
        return copy(s2.at[t], r2.at[rows(p * 8, 8)], pa_s.at[t], pa_r.at[p], half_dev(t))

    def p_recv(t):
        return copy(s2.at[t], r2.at[rows(t * 8, 8)], pa_s.at[t], pa_r.at[t], half_dev(t))

    swap(8, z, lambda t: z_send(t).start())
    swap(16, p, lambda t: p_send(t).start())
    r1[rows(z * 16, 16)] = s1[z]
    r2[rows(p * 8, 8)] = s2[p]
    green_part(0)
    swap(8, z, lambda t: z_recv(t).wait_recv())
    for t in range(3):
        o1[h, rows(p * 16, 16), t * 256 : (t + 1) * 256] = jnp.concatenate(
            [r1[pl.ds(2 * t + k, 16, stride=8), :] for k in range(2)], axis=1
        ).astype(BF16)

    def block(t, core):
        return o1.at[t // 8, rows(((t // 4) % 2 * 8 + t % 4 * 2 + core) * 16, 16)]

    def c_send(t):
        return copy(block(q, c), block(q, c), cg_s.at[t], cg_r.at[q], chip_dev(t))

    def c_recv(t):
        return copy(block(t, c), block(t, c), cg_s.at[t], cg_r.at[t], chip_dev(t))

    def f_send(t):
        return copy(block(t, c), block(t, c), cf_s.at[t], cf_r.at[t], core_dev)

    def f_recv(t):
        return copy(block(t, 1 - c), block(t, 1 - c), cf_s.at[t], cf_r.at[t], core_dev)

    swap(16, q, lambda t: c_send(t).start())
    f_send(q).start()
    swap(16, p, lambda t: p_recv(t).wait_recv())
    for k in range(3):
        o2[rows(z * 32, 32), k * 128 : (k + 1) * 128] = r2[pl.ds(k, 32, stride=4), :].astype(BF16)

    def zg_send(t):
        mine = o2.at[rows(z * 32, 32)]
        return copy(mine, mine, zg_s.at[t], zg_r.at[z], z_dev(t))

    def zg_recv(t):
        theirs = o2.at[rows(t * 32, 32)]
        return copy(theirs, theirs, zg_s.at[t], zg_r.at[t], z_dev(t))

    swap(8, z, lambda t: zg_send(t).start())
    green_part(1)
    green_part(2)

    def pass_on(t):
        c_recv(t).wait_recv()
        f_send(t).start()

    swap(16, q, pass_on)
    swap(8, z, lambda t: zg_recv(t).wait_recv())
    o_rows = dot(perm_b[...], o2[...])
    o_b = o_rows.astype(BF16)
    w = (o_rows * o_rows[:, 45:46]).astype(BF16).T
    each(16, lambda t: f_recv(t).wait_recv())

    v = jnp.zeros((NORB, ROWS), F32)
    for hh in range(2):
        orb = dot(perm_a[...], o1[hh]).astype(BF16)
        m_high, m_low = split2(green[hh] * dot(w, orb))
        v = v + dot(orb, m_high, (1, 1)) + dot(orb, m_low, (1, 1))
    v_high, v_low = split2(v)
    gp[...] = (dot(o_b, v_high, (1, 1)) + dot(o_b, v_low, (1, 1))) * (1.0 / NPTS)

    def half_send():
        other = gp.at[rows((1 - c) * 128, 128)]
        return copy(other, gc, gc_s, gc_r, core_dev)

    def v_part(part, t):
        return v_b.at[part, :, rows(t * 16, 16), :]

    def v_send(part, t):
        return copy(v_part(part, t), rv.at[part, z], va_s.at[part, t], va_r.at[part, z], z_dev(t))

    def v_recv(part, t):
        return copy(v_part(part, t), rv.at[part, t], va_s.at[part, t], va_r.at[part, t], z_dev(t))

    half_send().start()
    for part, value in ((0, v_high), (1, v_low)):
        v_b[part] = value.reshape(2, 128, ROWS)
    v_f[...] = v.reshape(2, 128, ROWS)
    swap(8, z, lambda t: v_send(0, t).start())
    half_send().wait_recv()
    gh[...] = gp[rows(c * 128, 128)] + gc[...]

    def a_send(t):
        return copy(gh.at[rows(t * 8, 8)], rg.at[q], ga_s.at[t], ga_r.at[q], chip_dev(t))

    def a_recv(t):
        return copy(gh.at[rows(t * 8, 8)], rg.at[t], ga_s.at[t], ga_r.at[t], chip_dev(t))

    swap(16, q, lambda t: a_send(t).start())
    rg[q] = gh[rows(q * 8, 8)]
    for part in range(2):
        rv[part, z] = jnp.zeros((2, 16, ROWS), BF16)
    swap(16, q, lambda t: a_recv(t).wait_recv())
    s8[...] = jnp.sum(rg[...], axis=0)

    def gz_send(t):
        return copy(s8, rz.at[z], gz_s.at[t], gz_r.at[z], z_dev(t))

    def gz_recv(t):
        return copy(s8, rz.at[t], gz_s.at[t], gz_r.at[t], z_dev(t))

    swap(8, z, lambda t: gz_send(t).start())
    swap(8, z, lambda t: v_send(1, t).start())
    rz[z] = s8[...]
    swap(8, z, lambda t: gz_recv(t).wait_recv())

    def line(t, core):
        return gram.at[rows(core * 128 + t * 8, 8)]

    gram[rows(c * 128 + q * 8, 8)] = jnp.sum(rz[...], axis=0)

    def g_send(t):
        return copy(line(q, c), line(q, c), gg_s.at[t], gg_r.at[q], chip_dev(t))

    def g_recv(t):
        return copy(line(t, c), line(t, c), gg_s.at[t], gg_r.at[t], chip_dev(t))

    def gf_send(t):
        return copy(line(t, c), line(t, c), gf_s.at[t], gf_r.at[t], core_dev)

    def gf_recv(t):
        return copy(line(t, 1 - c), line(t, 1 - c), gf_s.at[t], gf_r.at[t], core_dev)

    swap(16, q, lambda t: g_send(t).start())
    gf_send(q).start()

    for part in range(2):
        swap(8, z, lambda t, part=part: v_recv(part, t).wait_recv())
    others = jnp.sum(rv[0].astype(F32) + rv[1].astype(F32), axis=0)
    mine = -(v_f[:, rows(z * 16, 16), :] + others)
    m_high, m_low = split2(mine)
    own = vall.at[:, rows(z * 16, 16), :]
    own[:, :, :ROWS] = m_high
    own[:, :, ROWS:] = m_low

    def vg_send(t):
        return copy(own, own, vg_s.at[t], vg_r.at[z], z_dev(t))

    def vg_recv(t):
        theirs = vall.at[:, rows(t * 16, 16), :]
        return copy(theirs, theirs, vg_s.at[t], vg_r.at[t], z_dev(t))

    swap(8, z, lambda t: vg_send(t).start())

    def g_pass_on(t):
        g_recv(t).wait_recv()
        gf_send(t).start()

    swap(16, q, g_pass_on)

    def d_send(n, t):
        return copy(dd.at[n, rows(t * 8, 8)], rp.at[n, rows(p * 8, 8)], d_s.at[n, t], d_r.at[n, p], half_dev(t))

    def d_recv(n, t):
        return copy(dd.at[n, rows(t * 8, 8)], rp.at[n, rows(t * 8, 8)], d_s.at[n, t], d_r.at[n, t], half_dev(t))

    def deal(n, value):
        for k in range(3):
            tt[n, k] = value[:, k * 128 : (k + 1) * 128]
        even, odd = (
            jnp.concatenate([tt[n, k, pl.ds(o, 16, stride=2), :] for k in range(3)], axis=1)
            for o in range(2)
        )
        gap = jnp.zeros((16, 16), F32)
        for k in range(8):
            cells = slice(48 * k, 48 * k + 48)
            dd[n, pl.ds(k, 16, stride=8), :] = jnp.concatenate(
                [even[:, cells], gap, odd[:, cells], gap], axis=1
            )
        swap(16, p, lambda t: d_send(n, t).start())
        rp[n, rows(p * 8, 8)] = dd[n, rows(p * 8, 8)]

    def land(n, out):
        swap(16, p, lambda t: d_recv(n, t).wait_recv())
        table = jnp.concatenate([rp[n, pl.ds(k, 16, stride=8), :] for k in range(8)], axis=0)
        turned = table.T
        for k in range(45):
            out[:, k * 128 : (k + 1) * 128] = jnp.concatenate(
                [turned[k : k + 1], turned[64 + k : 65 + k]], axis=0
            )

    deal(0, mine.reshape(32, ROWS))
    each(16, lambda t: gf_recv(t).wait_recv())
    half_send().wait_send()
    swap(16, q, lambda t: g_send(t).wait_send())
    each(16, lambda t: gf_send(t).wait_send())
    a = gram[...]
    gram[...] = (a + a.T) * 0.5
    eliminate(gram)
    l_rows = jnp.concatenate([gram[rows(k * 128 + z * 16, 16), :] for k in range(2)], axis=0)
    l_both = jnp.concatenate(split2(l_rows), axis=0)
    swap(8, z, lambda t: vg_recv(t).wait_recv())
    out = dot(l_both, vall[...].reshape(NORB, 2 * ROWS))
    deal(1, out[:32, :ROWS] + out[32:, :ROWS] + out[:32, ROWS:])
    land(0, ov)
    for group, i, sends in (
        (8, z, (z_send, zg_send, functools.partial(v_send, 0), functools.partial(v_send, 1), gz_send, vg_send)),
        (16, p, (p_send, functools.partial(d_send, 0))),
        (16, q, (c_send, a_send)),
    ):
        for send in sends:
            swap(group, i, lambda t, send=send: send(t).wait_send())
    each(16, lambda t: f_send(t).wait_send())
    land(1, oq)
    swap(16, p, lambda t: d_send(1, t).wait_send())


def eliminate(work):
    sub = lax.broadcasted_iota(jnp.int32, (8, 128), 0)
    lane = lax.broadcasted_iota(jnp.int32, (8, 128), 1)
    wide = lambda col: jnp.broadcast_to(col, (8, 128))
    for k in range(8):
        base = 32 * k
        tile, off = base // 128, base % 128
        wk = [
            [work[base + 8 * g : base + 8 * g + 8, 128 * t : 128 * t + 128] for t in range(2)]
            for g in range(4)
        ]
        col = [
            [wide(wk[g][tile][:, off + j : off + j + 1]) if g >= j // 8 else None for g in range(4)]
            for j in range(32)
        ]
        inside = (lane >= off) & (lane < off + 32)
        for g in range(4):
            unit = jnp.where(lane - off == sub + 8 * g, 1.0, 0.0)
            wk[g][tile] = jnp.where(inside, unit, wk[g][tile])
        pivots = [jnp.ones((8, 128), F32) for _ in range(4)]
        for j in range(0, 32, 2):
            gj, sj = j // 8, j % 8
            u, v = col[j], col[j + 1]
            p11 = wide(u[gj][sj : sj + 1, :])
            p21 = wide(u[gj][sj + 1 : sj + 2, :])
            p22 = wide(v[gj][sj + 1 : sj + 2, :])
            det = p11 * p22 - p21 * p21
            r = 1.0 / det
            r11 = 1.0 / p11
            pivots[gj] = jnp.where(sub == sj, p11, jnp.where(sub == sj + 1, det * r11, pivots[gj]))
            q11, q21, q22 = p22 * r, p21 * r, p11 * r
            al, be = [None] * 4, [None] * 4
            for g in range(gj, 4):
                al[g] = u[g] * q11 - v[g] * q21
                be[g] = v[g] * q22 - u[g] * q21
            below = sub > sj + 1
            be[gj] = jnp.where(below, be[gj], 0.0)
            al[gj] = jnp.where(below, al[gj], jnp.where(sub == sj + 1, p21 * r11, 0.0))
            for i in range(j + 2, 32):
                fu = wide(u[i // 8][i % 8 : i % 8 + 1, :])
                fv = wide(v[i // 8][i % 8 : i % 8 + 1, :])
                for g in range(i // 8, 4):
                    col[i][g] = col[i][g] - (al[g] * fu + be[g] * fv)
            for t in range(2):
                one = wide(wk[gj][t][sj : sj + 1, :])
                two = wide(wk[gj][t][sj + 1 : sj + 2, :])
                for g in range(gj, 4):
                    wk[g][t] = wk[g][t] - (al[g] * one + be[g] * two)
        for g in range(4):
            scale = lax.rsqrt(pivots[g])
            for t in range(2):
                wk[g][t] = wk[g][t] * scale
        u = jnp.concatenate([jnp.concatenate(wk[g], axis=1) for g in range(4)], axis=0)
        lanes = lax.broadcasted_iota(jnp.int32, (32, 256), 1)
        work[base : base + 32, :] = jnp.where(lanes < base + 32, u, 0.0)
        if k < 7:
            u_high, u_low = split2(u)
            one = jnp.concatenate([u_high, u_low, u_high], axis=0)
            two = jnp.concatenate([u_high, u_high, u_low], axis=0)
            edge = base + 32
            start = edge // 128 * 128
            change = dot(one[:, start:].T, two)[edge - start :]
            rest = work[edge:, :]
            lanes = lax.broadcasted_iota(jnp.int32, rest.shape, 1)
            rest = jnp.where((lanes >= base) & (lanes < edge), 0.0, rest)
            work[edge:, :] = rest - change


VM = pl.BlockSpec(memory_space=pltpu.VMEM)
SM = pl.BlockSpec(memory_space=pltpu.SMEM)
DMA = pltpu.SemaphoreType.DMA


def call(kernel, args, outs, scratch, number=None, name=None, specs=None):
    params = dict(vmem_limit_bytes=60 * 1024 * 1024)
    if number is not None:
        params.update(collective_id=number, has_side_effects=True)
    return pl.pallas_call(
        kernel,
        out_shape=[jax.ShapeDtypeStruct(s, d) for s, d in outs],
        in_specs=specs or [VM] * len(args),
        out_specs=[VM] * len(outs),
        scratch_shapes=scratch,
        compiler_params=pltpu.CompilerParams(**params),
        name=name,
    )(*args)


def on_device(orbitals, occupation):
    xl, z, y, c, h = me()
    own = orbitals.astype(F32)
    s1 = own.reshape(2, 10, 8, 3, NZ).transpose(2, 0, 3, 1, 4).reshape(8, 2, 3, 240)
    s1 = jnp.pad(s1, ((0, 0), (0, 0), (0, 1), (0, 16))).reshape(8, 16, 128)
    s2 = own.reshape(2, 45, 8, 16).transpose(3, 0, 2, 1)
    occ = jnp.broadcast_to(occupation.astype(F32)[None, :, None, None], (16, 2, 8, 1))
    s2 = jnp.concatenate([s2, occ], axis=3)
    s2 = jnp.pad(s2, ((0, 0), (0, 0), (0, 0), (0, 2))).reshape(16, 2, ROWS)
    s2 = jnp.pad(s2, ((0, 0), (0, 0), (0, 128))).reshape(16, 8, 128)
    vm = pltpu.VMEM
    return tuple(call(
        main_kernel, (s1, s2, *permutations(), *tables()),
        (((2, HALF), F32), ((2, HALF), F32)),
        [vm((2, NORB, 768), BF16), vm((NORB, ROWS), BF16), vm((128, 128), F32), vm((128, 128), F32),
         vm((2, ROWS, 768), F32), vm((ROWS, MODES), F32), vm((ROWS, 128), F32),
         vm((2, 128, ROWS), F32), vm((2, 2, 128, ROWS), BF16), vm((NORB, NORB), F32),
         vm((128, NORB), F32), vm((128, NORB), F32), vm((16, 8, NORB), F32),
         vm((2, 8, 2, 16, ROWS), BF16), vm((8, NORB), F32), vm((8, 8, NORB), F32),
         vm((NORB, NORB), F32), vm((2, 128, 2 * ROWS), BF16), vm((2, 3, 32, 128), F32),
         vm((2, 128, 128), F32), vm((2, 128, 128), F32),
         DMA((8,)), DMA((8,)), DMA((16,)), DMA((16,)), DMA((16,)), DMA((16,)), DMA((16,)), DMA((16,)),
         DMA((8,)), DMA((8,)), DMA, DMA, DMA((16,)), DMA((16,)), DMA((2, 8)), DMA((2, 8)),
         DMA((8,)), DMA((8,)), DMA((16,)), DMA((16,)), DMA((16,)), DMA((16,)),
         DMA((8,)), DMA((8,)), DMA((2, 16)), DMA((2, 16))],
        0, "exchange",
    ))


def solution(mesh):
    torus = Mesh(mesh.devices.reshape(2, 8, 4, 2, mesh.shape["grid"]), AXES)
    return jax.shard_map(
        on_device,
        mesh=torus,
        in_specs=(P(ORB, "h"), P(ORB)),
        out_specs=(P(ORB, "h"), P(ORB, "h")),
        check_vma=False,
    )
```

```python
import functools
import math

import jax
import jax.numpy as jnp
import numpy as np
from jax import lax
from jax.experimental import pallas as pl
from jax.experimental.pallas import tpu as pltpu
from jax.sharding import Mesh
from jax.sharding import PartitionSpec as P

NX = 20
NY = 24
NZ = 24
NORB = 256
NPTS = 11520
HALF = NPTS // 2
MODES = 512
ROWS = 384
AXES = ("xl", "z", "y", "c", "h")
ORB = ("xl", "z", "y", "c")
MESH = pl.DeviceIdType.MESH
F32 = jnp.float32
BF16 = jnp.bfloat16


def rounded(a):
    return np.asarray(a, np.float32).astype(jnp.bfloat16).astype(np.float32)


def hartley_table(length):
    index = np.arange(length)
    angle = 2.0 * math.pi / length * (index[:, None] * index[None, :] % length)
    return rounded(np.cos(angle) + np.sin(angle))


def signed_square(length):
    index = np.arange(length)
    signed = np.where(index <= length // 2, index, index - length)
    return (2.0 * math.pi * signed / length) ** 2


def coulomb_kernel():
    total = (
        signed_square(NX)[:, None, None]
        + signed_square(NY)[None, :, None]
        + signed_square(NZ)[None, None, :]
    )
    return np.where(total > 0, 1.0 / np.where(total > 0, total, 1.0), 0.0) / NPTS


def two_parts(a):
    high = rounded(a)
    return high, rounded(a - high)


def tables():
    cx, cy, cz = hartley_table(NX), hartley_table(NY), hartley_table(NZ)
    kernel = coulomb_kernel()
    ac = NX * NZ
    tx = np.zeros((128, MODES), np.float32)
    tx[:NX, :ac] = np.repeat(cx, NZ, axis=1)
    tz = np.zeros((128, MODES), np.float32)
    tz[:NZ, :ac] = np.tile(cz, (1, NX))
    ty = np.zeros((128, 128), np.float32)
    tk = np.zeros((128, MODES), np.float32)
    k_high, k_low = two_parts(kernel.transpose(1, 0, 2).reshape(NY, ac))
    for at, part in ((0, k_high), (32, k_high), (64, k_low)):
        ty[:NY, at : at + NY] = cy
        tk[at : at + NY, :ac] = part
    phi = np.einsum("ax,cz->acxz", cx, cz).reshape(ac, NX, NZ)
    right = np.zeros((MODES, 2, 256), np.float32)
    for h in range(2):
        right[:ac, h, :240] = phi[:, 10 * h : 10 * h + 10].reshape(ac, 240)
    r_high, r_low = two_parts(right.reshape(MODES, 512))
    bf = lambda a: jnp.asarray(a, BF16)
    three = np.concatenate([tx, tz, tk], axis=1)
    return bf(three), bf(ty), bf(np.concatenate([r_high, r_low], axis=1)), jnp.asarray(ty[:32], F32)


def permutations():
    true = np.arange(NORB).reshape(2, 8, 8, 2)
    order_a = true.transpose(0, 2, 1, 3).reshape(-1)
    order_b = true.transpose(1, 0, 2, 3).reshape(-1)
    eye = np.eye(NORB, dtype=np.float32)
    return jnp.asarray(np.concatenate([eye[:, order_a], eye[:, order_b]], axis=1), BF16)


def split2(a):
    high = a.astype(BF16)
    return high, (a - high.astype(F32)).astype(BF16)


def dot(a, b, dims=(1, 0)):
    return lax.dot_general(
        a, b, (((dims[0],), (dims[1],)), ((), ())), preferred_element_type=F32
    )


def me():
    return tuple(lax.axis_index(a) for a in AXES)


def of_plane(pid, z):
    return ((pid // 8) % 2, z, (pid // 2) % 4, pid % 2, pid // 16)


def copy(src, dst, send_sem, recv_sem, device):
    return pltpu.make_async_remote_copy(
        src_ref=src, dst_ref=dst, send_sem=send_sem, recv_sem=recv_sem,
        device_id=device, device_id_type=MESH,
    )


def rows(start, size):
    return pl.ds(pl.multiple_of(start, size), size)


def each(count, body):
    lax.fori_loop(0, count, lambda i, carry: (body(i), carry)[1], 0)


def swap(n, i, body):
    each(n - 1, lambda d: body((i + d + 1) % n))


Z_ORDER = (4, 3, 5, 2, 6, 1, 7)
CHIP_ORDER = (
    (2, 2), (2, 1), (2, 3), (1, 2), (3, 2), (1, 1), (1, 3), (3, 1), (3, 3),
    (2, 0), (0, 2), (1, 0), (3, 0), (0, 1), (0, 3),
)
HALF_ORDER = tuple((a, b, k) for a, b in ((1, 2), (1, 1), (1, 3), (0, 2), (1, 0), (0, 1), (0, 3)) for k in range(2)) + ((0, 0, 1),)


def greet(barrier, n, i, device):
    swap(n, i, lambda t: pl.semaphore_signal(barrier, inc=1, device_id=device(t), device_id_type=MESH))
    return n - 1


def shifted(a, factor, shift):
    return lax.shift_right_logical(a * factor, shift)


def main_kernel(
    s1_any, s2_any, perm_any, t_any, ty_any, right_any, cy_any, ov, oq,
    s1, s2, perm, t3, ty, right, cy, in_s,
    o1, o2, r1, r2, green, left, y_rows, v_f, v_b, gp, gc, gh, rg, rv, s8, rz,
    gram, vall, tt, dd, rp,
    za_s, za_r, pa_s, pa_r, cg_s, cg_r, cf_s, cf_r, zg_s, zg_r,
    gc_s, gc_r, ga_s, ga_r, va_s, va_r, gz_s, gz_r, gg_s, gg_r, gf_s, gf_r,
    vg_s, vg_r, d_s, d_r,
):
    xl, z, y, c, h = me()
    p = xl * 8 + y * 2 + c
    q = h * 8 + xl * 4 + y
    z_dev = lambda t: (xl, t, y, c, h)
    half_dev = lambda t: of_plane(h * 16 + t, z)
    chip_dev = lambda t: ((t // 4) % 2, z, t % 4, c, t // 8)
    core_dev = (xl, z, y, 1 - c, h)

    def z_line(body):
        for d in Z_ORDER:
            body((z + d) % 8)

    def chips(body):
        for dx, dy in CHIP_ORDER:
            body((q // 4 + dx) % 4 * 4 + (y + dy) % 4)

    def half(body):
        for dx, dy, dc in HALF_ORDER:
            body((xl + dx) % 2 * 8 + (y + dy) % 4 * 2 + (c + dc) % 2)

    barrier = pltpu.get_barrier_semaphore()
    greeted = greet(barrier, 8, z, z_dev) + greet(barrier, 16, p, half_dev)
    greeted += greet(barrier, 16, q, chip_dev)
    pl.semaphore_signal(barrier, inc=1, device_id=core_dev, device_id_type=MESH)

    held = (
        (s1_any, s1), (s2_any, s2), (t_any, t3), (ty_any, ty), (cy_any, cy),
        (right_any, right), (perm_any, perm),
    )
    held = [pltpu.make_async_copy(a, b, in_s.at[k]) for k, (a, b) in enumerate(held)]
    for one in held:
        one.start()
    perm_a, perm_b = perm.at[:, :NORB], perm.at[:, NORB:]
    tx, tz, tk = (t3.at[:, k * MODES : (k + 1) * MODES] for k in range(3))
    rh, rl = right.at[:, :512], right.at[:, 512:]
    for one in held[2:5]:
        one.wait()

    row = lax.broadcasted_iota(jnp.int32, (ROWS, 128), 0)
    lane = lax.broadcasted_iota(jnp.int32, (ROWS, 128), 1)
    zz = shifted(row, 1366, 16)
    s = row - zz * 48
    cell = h * HALF + s * 128 + zz * 16 + p
    x = shifted(cell, 7282, 22)
    yz = cell - x * (NY * NZ)
    y_cell = shifted(yz, 2731, 16)
    z_cell = yz - y_cell * NZ
    hot = lambda a: jnp.where(a == lane, 1.0, 0.0).astype(BF16)
    left[...] = dot(hot(jnp.where(s < 45, x, 127)), tx[...]) * dot(hot(z_cell), tz[...])
    y_rows[...] = dot(hot(y_cell), ty[...])
    middle = (lane >= 32) & (lane < 64)

    def green_part(t):
        k_high, k_low = split2(y_rows[...] * cy[pl.ds(z * 3 + t, 1), :])
        mix = jnp.where(middle, k_low.astype(F32), k_high.astype(F32)).astype(BF16)
        l_high, l_low = split2(left[...] * dot(mix, tk[...]))
        g = dot(l_high, rh[...]) + dot(l_low, rh[...]) + dot(l_high, rl[...])
        for hh in range(2):
            green[hh, :, t * 256 : (t + 1) * 256] = g[:, hh * 256 : (hh + 1) * 256]

    for one in held[:2]:
        one.wait()
    pl.semaphore_wait(barrier, greeted + 1)

    def z_send(t):
        return copy(s1.at[t], r1.at[rows(z * 16, 16)], za_s.at[t], za_r.at[z], z_dev(t))

    def z_recv(t):
        return copy(s1.at[t], r1.at[rows(t * 16, 16)], za_s.at[t], za_r.at[t], z_dev(t))

    def p_send(t):
        return copy(s2.at[t], r2.at[rows(p * 8, 8)], pa_s.at[t], pa_r.at[p], half_dev(t))

    def p_recv(t):
        return copy(s2.at[t], r2.at[rows(t * 8, 8)], pa_s.at[t], pa_r.at[t], half_dev(t))

    half(lambda t: p_send(t).start())
    z_line(lambda t: z_send(t).start())
    r1[rows(z * 16, 16)] = s1[z]
    r2[rows(p * 8, 8)] = s2[p]
    for one in held[5:]:
        one.wait()
    green_part(0)
    swap(16, p, lambda t: p_recv(t).wait_recv())
    for k in range(3):
        o2[rows(z * 32, 32), k * 128 : (k + 1) * 128] = r2[pl.ds(k, 32, stride=4), :].astype(BF16)

    def zg_send(t):
        mine = o2.at[rows(z * 32, 32)]
        return copy(mine, mine, zg_s.at[t], zg_r.at[z], z_dev(t))

    def zg_recv(t):
        theirs = o2.at[rows(t * 32, 32)]
        return copy(theirs, theirs, zg_s.at[t], zg_r.at[t], z_dev(t))

    z_line(lambda t: zg_send(t).start())
    swap(8, z, lambda t: z_recv(t).wait_recv())
    for t in range(3):
        o1[h, rows(p * 16, 16), t * 256 : (t + 1) * 256] = jnp.concatenate(
            [r1[pl.ds(2 * t + k, 16, stride=8), :] for k in range(2)], axis=1
        ).astype(BF16)

    def block(t, core):
        return o1.at[t // 8, rows(((t // 4) % 2 * 8 + t % 4 * 2 + core) * 16, 16)]

    def c_send(t):
        return copy(block(q, c), block(q, c), cg_s.at[t], cg_r.at[q], chip_dev(t))

    def c_recv(t):
        return copy(block(t, c), block(t, c), cg_s.at[t], cg_r.at[t], chip_dev(t))

    def f_send(t):
        return copy(block(t, c), block(t, c), cf_s.at[t], cf_r.at[t], core_dev)

    def f_recv(t):
        return copy(block(t, 1 - c), block(t, 1 - c), cf_s.at[t], cf_r.at[t], core_dev)

    chips(lambda t: c_send(t).start())
    f_send(q).start()
    green_part(1)
    green_part(2)

    def pass_on(t):
        c_recv(t).wait_recv()
        f_send(t).start()

    chips(pass_on)
    swap(8, z, lambda t: zg_recv(t).wait_recv())
    o_rows = dot(perm_b[...], o2[...])
    o_b = o_rows.astype(BF16)
    w = (o_rows * o_rows[:, 45:46]).astype(BF16).T
    each(16, lambda t: f_recv(t).wait_recv())

    v = jnp.zeros((NORB, ROWS), F32)
    for hh in range(2):
        orb = dot(perm_a[...], o1[hh]).astype(BF16)
        m_high, m_low = split2(green[hh] * dot(w, orb))
        v = v + dot(orb, m_high, (1, 1)) + dot(orb, m_low, (1, 1))
    v_high, v_low = split2(v)
    gp[...] = (dot(o_b, v_high, (1, 1)) + dot(o_b, v_low, (1, 1))) * (1.0 / NPTS)

    def half_send():
        other = gp.at[rows((1 - c) * 128, 128)]
        return copy(other, gc, gc_s, gc_r, core_dev)

    def v_send(part, t):
        if part == 0:
            src, dst = v_b.at[0, :, rows(t * 16, 16), :], rv.at[0, z]
        else:
            src, dst = v_b.at[1, part - 1, rows(t * 16, 16), :], rv.at[1, z, part - 1]
        return copy(src, dst, va_s.at[part, t], va_r.at[part, z], z_dev(t))

    def v_recv(part, t):
        if part == 0:
            src, dst = v_b.at[0, :, rows(t * 16, 16), :], rv.at[0, t]
        else:
            src, dst = v_b.at[1, part - 1, rows(t * 16, 16), :], rv.at[1, t, part - 1]
        return copy(src, dst, va_s.at[part, t], va_r.at[part, t], z_dev(t))

    half_send().start()
    for part, value in ((0, v_high), (1, v_low)):
        v_b[part] = value.reshape(2, 128, ROWS)
    v_f[...] = v.reshape(2, 128, ROWS)
    z_line(lambda t: v_send(0, t).start())
    z_line(lambda t: v_send(1, t).start())
    half_send().wait_recv()
    gh[...] = gp[rows(c * 128, 128)] + gc[...]

    def a_send(t):
        return copy(gh.at[rows(t * 8, 8)], rg.at[q], ga_s.at[t], ga_r.at[q], chip_dev(t))

    def a_recv(t):
        return copy(gh.at[rows(t * 8, 8)], rg.at[t], ga_s.at[t], ga_r.at[t], chip_dev(t))

    chips(lambda t: a_send(t).start())
    rg[q] = gh[rows(q * 8, 8)]
    for part in range(2):
        rv[part, z] = jnp.zeros((2, 16, ROWS), BF16)
    swap(16, q, lambda t: a_recv(t).wait_recv())
    s8[...] = jnp.sum(rg[...], axis=0)

    def gz_send(t):
        return copy(s8, rz.at[z], gz_s.at[t], gz_r.at[z], z_dev(t))

    def gz_recv(t):
        return copy(s8, rz.at[t], gz_s.at[t], gz_r.at[t], z_dev(t))

    z_line(lambda t: gz_send(t).start())
    z_line(lambda t: v_send(2, t).start())
    rz[z] = s8[...]
    swap(8, z, lambda t: gz_recv(t).wait_recv())

    def line(t, core):
        return gram.at[rows(core * 128 + t * 8, 8)]

    gram[rows(c * 128 + q * 8, 8)] = jnp.sum(rz[...], axis=0)

    def g_send(t):
        return copy(line(q, c), line(q, c), gg_s.at[t], gg_r.at[q], chip_dev(t))

    def g_recv(t):
        return copy(line(t, c), line(t, c), gg_s.at[t], gg_r.at[t], chip_dev(t))

    def gf_send(t):
        return copy(line(t, c), line(t, c), gf_s.at[t], gf_r.at[t], core_dev)

    def gf_recv(t):
        return copy(line(t, 1 - c), line(t, 1 - c), gf_s.at[t], gf_r.at[t], core_dev)

    chips(lambda t: g_send(t).start())
    gf_send(q).start()

    for part in range(3):
        swap(8, z, lambda t, part=part: v_recv(part, t).wait_recv())
    others = jnp.sum(rv[0].astype(F32) + rv[1].astype(F32), axis=0)
    mine = -(v_f[:, rows(z * 16, 16), :] + others)
    m_high, m_low = split2(mine)
    own = vall.at[:, rows(z * 16, 16), :]
    own[:, :, :ROWS] = m_high
    own[:, :, ROWS:] = m_low

    def vg_send(t):
        return copy(own, own, vg_s.at[t], vg_r.at[z], z_dev(t))

    def vg_recv(t):
        theirs = vall.at[:, rows(t * 16, 16), :]
        return copy(theirs, theirs, vg_s.at[t], vg_r.at[t], z_dev(t))

    z_line(lambda t: vg_send(t).start())

    def g_pass_on(t):
        g_recv(t).wait_recv()
        gf_send(t).start()

    chips(g_pass_on)

    def d_send(n, t):
        return copy(dd.at[n, rows(t * 8, 8)], rp.at[n, rows(p * 8, 8)], d_s.at[n, t], d_r.at[n, p], half_dev(t))

    def d_recv(n, t):
        return copy(dd.at[n, rows(t * 8, 8)], rp.at[n, rows(t * 8, 8)], d_s.at[n, t], d_r.at[n, t], half_dev(t))

    def deal(n, value):
        for k in range(3):
            tt[n, k] = value[:, k * 128 : (k + 1) * 128]
        even, odd = (
            jnp.concatenate([tt[n, k, pl.ds(o, 16, stride=2), :] for k in range(3)], axis=1)
            for o in range(2)
        )
        gap = jnp.zeros((16, 16), F32)
        for k in range(8):
            cells = slice(48 * k, 48 * k + 48)
            dd[n, pl.ds(k, 16, stride=8), :] = jnp.concatenate(
                [even[:, cells], gap, odd[:, cells], gap], axis=1
            )
        half(lambda t: d_send(n, t).start())
        rp[n, rows(p * 8, 8)] = dd[n, rows(p * 8, 8)]

    def land(n, out):
        swap(16, p, lambda t: d_recv(n, t).wait_recv())
        table = jnp.concatenate([rp[n, pl.ds(k, 16, stride=8), :] for k in range(8)], axis=0)
        turned = table.T
        for k in range(45):
            out[:, k * 128 : (k + 1) * 128] = jnp.concatenate(
                [turned[k : k + 1], turned[64 + k : 65 + k]], axis=0
            )

    deal(0, mine.reshape(32, ROWS))
    each(16, lambda t: gf_recv(t).wait_recv())
    half_send().wait_send()
    swap(16, q, lambda t: g_send(t).wait_send())
    each(16, lambda t: gf_send(t).wait_send())
    a = gram[...]
    gram[...] = (a + a.T) * 0.5
    eliminate(gram)
    l_rows = jnp.concatenate([gram[rows(k * 128 + z * 16, 16), :] for k in range(2)], axis=0)
    l_both = jnp.concatenate(split2(l_rows), axis=0)
    swap(8, z, lambda t: vg_recv(t).wait_recv())
    out = dot(l_both, vall[...].reshape(NORB, 2 * ROWS))
    deal(1, out[:32, :ROWS] + out[32:, :ROWS] + out[:32, ROWS:])
    land(0, ov)
    for group, i, sends in (
        (8, z, (z_send, zg_send, *(functools.partial(v_send, k) for k in range(3)), gz_send, vg_send)),
        (16, p, (p_send, functools.partial(d_send, 0))),
        (16, q, (c_send, a_send)),
    ):
        for send in sends:
            swap(group, i, lambda t, send=send: send(t).wait_send())
    each(16, lambda t: f_send(t).wait_send())
    land(1, oq)
    swap(16, p, lambda t: d_send(1, t).wait_send())


def eliminate(work):
    sub = lax.broadcasted_iota(jnp.int32, (8, 128), 0)
    lane = lax.broadcasted_iota(jnp.int32, (8, 128), 1)
    wide = lambda col: jnp.broadcast_to(col, (8, 128))
    for k in range(8):
        base = 32 * k
        tile, off = base // 128, base % 128
        wk = [
            [work[base + 8 * g : base + 8 * g + 8, 128 * t : 128 * t + 128] for t in range(2)]
            for g in range(4)
        ]
        col = [
            [wide(wk[g][tile][:, off + j : off + j + 1]) if g >= j // 8 else None for g in range(4)]
            for j in range(32)
        ]
        inside = (lane >= off) & (lane < off + 32)
        for g in range(4):
            unit = jnp.where(lane - off == sub + 8 * g, 1.0, 0.0)
            wk[g][tile] = jnp.where(inside, unit, wk[g][tile])
        pivots = [jnp.ones((8, 128), F32) for _ in range(4)]
        for j in range(0, 32, 2):
            gj, sj = j // 8, j % 8
            u, v = col[j], col[j + 1]
            p11 = wide(u[gj][sj : sj + 1, :])
            p21 = wide(u[gj][sj + 1 : sj + 2, :])
            p22 = wide(v[gj][sj + 1 : sj + 2, :])
            det = p11 * p22 - p21 * p21
            r = 1.0 / det
            r11 = 1.0 / p11
            pivots[gj] = jnp.where(sub == sj, p11, jnp.where(sub == sj + 1, det * r11, pivots[gj]))
            q11, q21, q22 = p22 * r, p21 * r, p11 * r
            al, be = [None] * 4, [None] * 4
            for g in range(gj, 4):
                al[g] = u[g] * q11 - v[g] * q21
                be[g] = v[g] * q22 - u[g] * q21
            below = sub > sj + 1
            be[gj] = jnp.where(below, be[gj], 0.0)
            al[gj] = jnp.where(below, al[gj], jnp.where(sub == sj + 1, p21 * r11, 0.0))
            for i in range(j + 2, 32):
                fu = wide(u[i // 8][i % 8 : i % 8 + 1, :])
                fv = wide(v[i // 8][i % 8 : i % 8 + 1, :])
                for g in range(i // 8, 4):
                    col[i][g] = col[i][g] - (al[g] * fu + be[g] * fv)
            for t in range(2):
                one = wide(wk[gj][t][sj : sj + 1, :])
                two = wide(wk[gj][t][sj + 1 : sj + 2, :])
                for g in range(gj, 4):
                    wk[g][t] = wk[g][t] - (al[g] * one + be[g] * two)
        for g in range(4):
            scale = lax.rsqrt(pivots[g])
            for t in range(2):
                wk[g][t] = wk[g][t] * scale
        u = jnp.concatenate([jnp.concatenate(wk[g], axis=1) for g in range(4)], axis=0)
        lanes = lax.broadcasted_iota(jnp.int32, (32, 256), 1)
        work[base : base + 32, :] = jnp.where(lanes < base + 32, u, 0.0)
        if k < 7:
            u_high, u_low = split2(u)
            one = jnp.concatenate([u_high, u_low, u_high], axis=0)
            two = jnp.concatenate([u_high, u_high, u_low], axis=0)
            edge = base + 32
            start = edge // 128 * 128
            change = dot(one[:, start:].T, two)[edge - start :]
            rest = work[edge:, :]
            lanes = lax.broadcasted_iota(jnp.int32, rest.shape, 1)
            rest = jnp.where((lanes >= base) & (lanes < edge), 0.0, rest)
            work[edge:, :] = rest - change


VM = pl.BlockSpec(memory_space=pltpu.VMEM)
ANY = pl.BlockSpec(memory_space=pl.ANY)
DMA = pltpu.SemaphoreType.DMA


def call(kernel, args, outs, scratch, number, name):
    return pl.pallas_call(
        kernel,
        out_shape=[jax.ShapeDtypeStruct(s, d) for s, d in outs],
        in_specs=[ANY] * len(args),
        out_specs=[VM] * len(outs),
        scratch_shapes=scratch,
        compiler_params=pltpu.CompilerParams(
            vmem_limit_bytes=60 * 1024 * 1024, collective_id=number, has_side_effects=True
        ),
        name=name,
    )(*args)


def on_device(orbitals, occupation):
    xl, z, y, c, h = me()
    own = orbitals.astype(F32)
    s1 = own.reshape(2, 10, 8, 3, NZ).transpose(2, 0, 3, 1, 4).reshape(8, 2, 3, 240)
    s1 = jnp.pad(s1, ((0, 0), (0, 0), (0, 1), (0, 16))).reshape(8, 16, 128)
    s2 = own.reshape(2, 45, 8, 16).transpose(3, 0, 2, 1)
    occ = jnp.broadcast_to(occupation.astype(F32)[None, :, None, None], (16, 2, 8, 1))
    s2 = jnp.concatenate([s2, occ], axis=3)
    s2 = jnp.pad(s2, ((0, 0), (0, 0), (0, 0), (0, 2))).reshape(16, 2, ROWS)
    s2 = jnp.pad(s2, ((0, 0), (0, 0), (0, 128))).reshape(16, 8, 128)
    vm = pltpu.VMEM
    return tuple(call(
        main_kernel, (s1, s2, permutations(), *tables()),
        (((2, HALF), F32), ((2, HALF), F32)),
        [vm((8, 16, 128), F32), vm((16, 8, 128), F32), vm((NORB, 512), BF16), vm((128, 3 * MODES), BF16),
         vm((128, 128), BF16), vm((MODES, 1024), BF16), vm((32, 128), F32), DMA((7,)),
         vm((2, NORB, 768), BF16), vm((NORB, ROWS), BF16), vm((128, 128), F32), vm((128, 128), F32),
         vm((2, ROWS, 768), F32), vm((ROWS, MODES), F32), vm((ROWS, 128), F32),
         vm((2, 128, ROWS), F32), vm((2, 2, 128, ROWS), BF16), vm((NORB, NORB), F32),
         vm((128, NORB), F32), vm((128, NORB), F32), vm((16, 8, NORB), F32),
         vm((2, 8, 2, 16, ROWS), BF16), vm((8, NORB), F32), vm((8, 8, NORB), F32),
         vm((NORB, NORB), F32), vm((2, 128, 2 * ROWS), BF16), vm((2, 3, 32, 128), F32),
         vm((2, 128, 128), F32), vm((2, 128, 128), F32),
         DMA((8,)), DMA((8,)), DMA((16,)), DMA((16,)), DMA((16,)), DMA((16,)), DMA((16,)), DMA((16,)),
         DMA((8,)), DMA((8,)), DMA, DMA, DMA((16,)), DMA((16,)), DMA((3, 8)), DMA((3, 8)),
         DMA((8,)), DMA((8,)), DMA((16,)), DMA((16,)), DMA((16,)), DMA((16,)),
         DMA((8,)), DMA((8,)), DMA((2, 16)), DMA((2, 16))],
        0, "exchange",
    ))


def solution(mesh):
    torus = Mesh(mesh.devices.reshape(2, 8, 4, 2, mesh.shape["grid"]), AXES)
    return jax.shard_map(
        on_device,
        mesh=torus,
        in_specs=(P(ORB, "h"), P(ORB)),
        out_specs=(P(ORB, "h"), P(ORB, "h")),
        check_vma=False,
    )
```

```python
import functools
import math

import jax
import jax.numpy as jnp
import numpy as np
from jax import lax
from jax.experimental import pallas as pl
from jax.experimental.pallas import tpu as pltpu
from jax.sharding import Mesh
from jax.sharding import PartitionSpec as P

NX = 20
NY = 24
NZ = 24
NORB = 256
NPTS = 11520
HALF = NPTS // 2
MODES = 512
ROWS = 384
AXES = ("xl", "z", "y", "c", "h")
ORB = ("xl", "z", "y", "c")
MESH = pl.DeviceIdType.MESH
F32 = jnp.float32
BF16 = jnp.bfloat16


def rounded(a):
    return np.asarray(a, np.float32).astype(jnp.bfloat16).astype(np.float32)


def hartley_table(length):
    index = np.arange(length)
    angle = 2.0 * math.pi / length * (index[:, None] * index[None, :] % length)
    return rounded(np.cos(angle) + np.sin(angle))


def signed_square(length):
    index = np.arange(length)
    signed = np.where(index <= length // 2, index, index - length)
    return (2.0 * math.pi * signed / length) ** 2


def coulomb_kernel():
    total = (
        signed_square(NX)[:, None, None]
        + signed_square(NY)[None, :, None]
        + signed_square(NZ)[None, None, :]
    )
    return np.where(total > 0, 1.0 / np.where(total > 0, total, 1.0), 0.0) / NPTS


def two_parts(a):
    high = rounded(a)
    return high, rounded(a - high)


def tables():
    cx, cy, cz = hartley_table(NX), hartley_table(NY), hartley_table(NZ)
    kernel = coulomb_kernel()
    ac = NX * NZ
    tx = np.zeros((128, MODES), np.float32)
    tx[:NX, :ac] = np.repeat(cx, NZ, axis=1)
    tz = np.zeros((128, MODES), np.float32)
    tz[:NZ, :ac] = np.tile(cz, (1, NX))
    ty = np.zeros((128, 128), np.float32)
    tk = np.zeros((128, MODES), np.float32)
    k_high, k_low = two_parts(kernel.transpose(1, 0, 2).reshape(NY, ac))
    for at, part in ((0, k_high), (32, k_high), (64, k_low)):
        ty[:NY, at : at + NY] = cy
        tk[at : at + NY, :ac] = part
    phi = np.einsum("ax,cz->acxz", cx, cz).reshape(ac, NX, NZ)
    right = np.zeros((MODES, 2, 256), np.float32)
    for h in range(2):
        right[:ac, h, :240] = phi[:, 10 * h : 10 * h + 10].reshape(ac, 240)
    r_high, r_low = two_parts(right.reshape(MODES, 512))
    bf = lambda a: jnp.asarray(a, BF16)
    three = np.concatenate([tx, tz, tk], axis=1)
    return bf(three), bf(ty), bf(np.concatenate([r_high, r_low], axis=1)), jnp.asarray(ty[:32], F32)


def permutations():
    true = np.arange(NORB).reshape(2, 8, 8, 2)
    order_a = true.transpose(0, 2, 1, 3).reshape(-1)
    order_b = true.transpose(1, 3, 0, 2).reshape(-1)
    eye = np.eye(NORB, dtype=np.float32)
    return jnp.asarray(np.concatenate([eye[:, order_a], eye[:, order_b]], axis=1), BF16)


def split2(a):
    high = a.astype(BF16)
    return high, (a - high.astype(F32)).astype(BF16)


def dot(a, b, dims=(1, 0)):
    return lax.dot_general(
        a, b, (((dims[0],), (dims[1],)), ((), ())), preferred_element_type=F32
    )


def me():
    return tuple(lax.axis_index(a) for a in AXES)


def of_plane(pid, z):
    return ((pid // 8) % 2, z, (pid // 2) % 4, pid % 2, pid // 16)


def copy(src, dst, send_sem, recv_sem, device):
    return pltpu.make_async_remote_copy(
        src_ref=src, dst_ref=dst, send_sem=send_sem, recv_sem=recv_sem,
        device_id=device, device_id_type=MESH,
    )


def rows(start, size):
    return pl.ds(pl.multiple_of(start, size), size)


def each(count, body):
    lax.fori_loop(0, count, lambda i, carry: (body(i), carry)[1], 0)


def swap(n, i, body):
    each(n - 1, lambda d: body((i + d + 1) % n))


Z_ORDER = (4, 3, 5, 2, 6, 1, 7)
CHIP_ORDER = (
    (2, 2), (2, 1), (2, 3), (1, 2), (3, 2), (1, 1), (1, 3), (3, 1), (3, 3),
    (2, 0), (0, 2), (1, 0), (3, 0), (0, 1), (0, 3),
)
HALF_ORDER = tuple((a, b, k) for a, b in ((1, 2), (1, 1), (1, 3), (0, 2), (1, 0), (0, 1), (0, 3)) for k in range(2)) + ((0, 0, 1),)


def greet(barrier, n, i, device):
    swap(n, i, lambda t: pl.semaphore_signal(barrier, inc=1, device_id=device(t), device_id_type=MESH))
    return n - 1


def shifted(a, factor, shift):
    return lax.shift_right_logical(a * factor, shift)


def main_kernel(
    st_any, raw_any, oc_any, perm_any, t_any, ty_any, right_any, cy_any, ov, oq,
    st, raw, oc, s1, s2, cells, turned_cells, perm, t3, ty, right, cy, in_s,
    o1, o2, r1, r2, green, left, y_rows, v_f, v_b, gp, gc, gh, rg, rv, s8, rz,
    gram, vall, tt, dd, rp,
    za_s, za_r, pa_s, pa_r, cg_s, cg_r, cf_s, cf_r, zg_s, zg_r,
    gc_s, gc_r, ga_s, ga_r, va_s, va_r, gz_s, gz_r, gg_s, gg_r, gf_s, gf_r,
    vg_s, vg_r, d_s, d_r,
):
    xl, z, y, c, h = me()
    p = xl * 8 + y * 2 + c
    q = h * 8 + xl * 4 + y
    z_dev = lambda t: (xl, t, y, c, h)
    half_dev = lambda t: of_plane(h * 16 + t, z)
    chip_dev = lambda t: ((t // 4) % 2, z, t % 4, c, t // 8)
    core_dev = (xl, z, y, 1 - c, h)

    def z_line(body):
        for d in Z_ORDER:
            body((z + d) % 8)

    def chips(body):
        for dx, dy in CHIP_ORDER:
            body((q // 4 + dx) % 4 * 4 + (y + dy) % 4)

    def half(body):
        for dx, dy, dc in HALF_ORDER:
            body((xl + dx) % 2 * 8 + (y + dy) % 4 * 2 + (c + dc) % 2)

    barrier = pltpu.get_barrier_semaphore()
    greeted = greet(barrier, 8, z, z_dev) + greet(barrier, 16, p, half_dev)
    greeted += greet(barrier, 16, q, chip_dev)
    pl.semaphore_signal(barrier, inc=1, device_id=core_dev, device_id_type=MESH)

    held = (
        (raw_any, raw), (oc_any, oc), (st_any, st), (t_any, t3), (ty_any, ty), (cy_any, cy),
        (right_any, right), (perm_any, perm),
    )
    held = [pltpu.make_async_copy(a, b, in_s.at[k]) for k, (a, b) in enumerate(held)]
    for one in held:
        one.start()
    perm_a, perm_b = perm.at[:, :NORB], perm.at[:, NORB:]
    tx, tz, tk = (t3.at[:, k * MODES : (k + 1) * MODES] for k in range(3))
    rh, rl = right.at[:, :512], right.at[:, 512:]
    for one in held[:3]:
        one.wait()
    cells[...] = jnp.zeros_like(cells)
    for k in range(45):
        pair = raw[:, k * 128 : (k + 1) * 128].astype(F32)
        for o in range(2):
            cells[64 * o + k : 64 * o + k + 1, :] = pair[o : o + 1]
    for o in range(2):
        cells[64 * o + 45 : 64 * o + 46, :] = oc[o : o + 1, :]
    turned_cells[...] = cells[...].T
    for k in range(16):
        s2[k] = turned_cells[pl.ds(k, 8, stride=16), :]
    for k in range(8):
        for o in range(2):
            for part in range(2):
                s1[k, pl.ds(8 * o + part, 4, stride=2), :] = st[k, o, :4, 128 * part : 128 * part + 128]
    for one in held[3:6]:
        one.wait()

    row = lax.broadcasted_iota(jnp.int32, (ROWS, 128), 0)
    lane = lax.broadcasted_iota(jnp.int32, (ROWS, 128), 1)
    zz = shifted(row, 1366, 16)
    s = row - zz * 48
    cell = h * HALF + s * 128 + zz * 16 + p
    x = shifted(cell, 7282, 22)
    yz = cell - x * (NY * NZ)
    y_cell = shifted(yz, 2731, 16)
    z_cell = yz - y_cell * NZ
    hot = lambda a: jnp.where(a == lane, 1.0, 0.0).astype(BF16)
    left[...] = dot(hot(jnp.where(s < 45, x, 127)), tx[...]) * dot(hot(z_cell), tz[...])
    y_rows[...] = dot(hot(y_cell), ty[...])
    middle = (lane >= 32) & (lane < 64)

    def green_part(t):
        k_high, k_low = split2(y_rows[...] * cy[pl.ds(z * 3 + t, 1), :])
        mix = jnp.where(middle, k_low.astype(F32), k_high.astype(F32)).astype(BF16)
        l_high, l_low = split2(left[...] * dot(mix, tk[...]))
        g = dot(l_high, rh[...]) + dot(l_low, rh[...]) + dot(l_high, rl[...])
        for hh in range(2):
            green[hh, :, t * 256 : (t + 1) * 256] = g[:, hh * 256 : (hh + 1) * 256]

    pl.semaphore_wait(barrier, greeted + 1)

    def z_send(t):
        return copy(s1.at[t], r1.at[rows(z * 16, 16)], za_s.at[t], za_r.at[z], z_dev(t))

    def z_recv(t):
        return copy(s1.at[t], r1.at[rows(t * 16, 16)], za_s.at[t], za_r.at[t], z_dev(t))

    def p_send(t):
        return copy(s2.at[t], r2.at[rows(p * 8, 8)], pa_s.at[t], pa_r.at[p], half_dev(t))

    def p_recv(t):
        return copy(s2.at[t], r2.at[rows(t * 8, 8)], pa_s.at[t], pa_r.at[t], half_dev(t))

    half(lambda t: p_send(t).start())
    z_line(lambda t: z_send(t).start())
    r1[rows(z * 16, 16)] = s1[z]
    r2[rows(p * 8, 8)] = s2[p]
    for one in held[6:]:
        one.wait()
    green_part(0)
    swap(16, p, lambda t: p_recv(t).wait_recv())
    by_row = [r2[pl.ds(k, 16, stride=8), :] for k in range(8)]
    o2[rows(z * 32, 32), :] = jnp.concatenate(
        [jnp.concatenate([b[:, 64 * o : 64 * o + 48] for b in by_row], axis=1) for o in range(2)], axis=0
    ).astype(BF16)

    def zg_send(t):
        mine = o2.at[rows(z * 32, 32)]
        return copy(mine, mine, zg_s.at[t], zg_r.at[z], z_dev(t))

    def zg_recv(t):
        theirs = o2.at[rows(t * 32, 32)]
        return copy(theirs, theirs, zg_s.at[t], zg_r.at[t], z_dev(t))

    z_line(lambda t: zg_send(t).start())
    swap(8, z, lambda t: z_recv(t).wait_recv())
    for t in range(3):
        o1[h, rows(p * 16, 16), t * 256 : (t + 1) * 256] = jnp.concatenate(
            [r1[pl.ds(2 * t + k, 16, stride=8), :] for k in range(2)], axis=1
        ).astype(BF16)

    def block(t, core):
        return o1.at[t // 8, rows(((t // 4) % 2 * 8 + t % 4 * 2 + core) * 16, 16)]

    def c_send(t):
        return copy(block(q, c), block(q, c), cg_s.at[t], cg_r.at[q], chip_dev(t))

    def c_recv(t):
        return copy(block(t, c), block(t, c), cg_s.at[t], cg_r.at[t], chip_dev(t))

    def f_send(t):
        return copy(block(t, c), block(t, c), cf_s.at[t], cf_r.at[t], core_dev)

    def f_recv(t):
        return copy(block(t, 1 - c), block(t, 1 - c), cf_s.at[t], cf_r.at[t], core_dev)

    chips(lambda t: c_send(t).start())
    f_send(q).start()
    green_part(1)
    green_part(2)

    def pass_on(t):
        c_recv(t).wait_recv()
        f_send(t).start()

    chips(pass_on)
    swap(8, z, lambda t: zg_recv(t).wait_recv())
    o_rows = dot(perm_b[...], o2[...])
    o_b = o_rows.astype(BF16)
    w = (o_rows * o_rows[:, 45:46]).astype(BF16).T
    each(16, lambda t: f_recv(t).wait_recv())

    v = jnp.zeros((NORB, ROWS), F32)
    for hh in range(2):
        orb = dot(perm_a[...], o1[hh]).astype(BF16)
        m_high, m_low = split2(green[hh] * dot(w, orb))
        v = v + dot(orb, m_high, (1, 1)) + dot(orb, m_low, (1, 1))
    v_high, v_low = split2(v)
    gp[...] = (dot(o_b, v_high, (1, 1)) + dot(o_b, v_low, (1, 1))) * (1.0 / NPTS)

    def half_send():
        other = gp.at[rows((1 - c) * 128, 128)]
        return copy(other, gc, gc_s, gc_r, core_dev)

    def v_send(part, t):
        if part == 0:
            src, dst = v_b.at[0, :, rows(t * 16, 16), :], rv.at[0, z]
        else:
            src, dst = v_b.at[1, part - 1, rows(t * 16, 16), :], rv.at[1, z, part - 1]
        return copy(src, dst, va_s.at[part, t], va_r.at[part, z], z_dev(t))

    def v_recv(part, t):
        if part == 0:
            src, dst = v_b.at[0, :, rows(t * 16, 16), :], rv.at[0, t]
        else:
            src, dst = v_b.at[1, part - 1, rows(t * 16, 16), :], rv.at[1, t, part - 1]
        return copy(src, dst, va_s.at[part, t], va_r.at[part, t], z_dev(t))

    half_send().start()
    for part, value in ((0, v_high), (1, v_low)):
        v_b[part] = value.reshape(2, 128, ROWS)
    v_f[...] = v.reshape(2, 128, ROWS)
    z_line(lambda t: v_send(0, t).start())
    z_line(lambda t: v_send(1, t).start())
    half_send().wait_recv()
    gh[...] = gp[rows(c * 128, 128)] + gc[...]

    def a_send(t):
        return copy(gh.at[rows(t * 8, 8)], rg.at[q], ga_s.at[t], ga_r.at[q], chip_dev(t))

    def a_recv(t):
        return copy(gh.at[rows(t * 8, 8)], rg.at[t], ga_s.at[t], ga_r.at[t], chip_dev(t))

    chips(lambda t: a_send(t).start())
    rg[q] = gh[rows(q * 8, 8)]
    for part in range(2):
        rv[part, z] = jnp.zeros((2, 16, ROWS), BF16)
    swap(16, q, lambda t: a_recv(t).wait_recv())
    s8[...] = jnp.sum(rg[...], axis=0)

    def gz_send(t):
        return copy(s8, rz.at[z], gz_s.at[t], gz_r.at[z], z_dev(t))

    def gz_recv(t):
        return copy(s8, rz.at[t], gz_s.at[t], gz_r.at[t], z_dev(t))

    z_line(lambda t: gz_send(t).start())
    z_line(lambda t: v_send(2, t).start())
    rz[z] = s8[...]
    swap(8, z, lambda t: gz_recv(t).wait_recv())

    def line(t, core):
        return gram.at[rows(core * 128 + t * 8, 8)]

    gram[rows(c * 128 + q * 8, 8)] = jnp.sum(rz[...], axis=0)

    def g_send(t):
        return copy(line(q, c), line(q, c), gg_s.at[t], gg_r.at[q], chip_dev(t))

    def g_recv(t):
        return copy(line(t, c), line(t, c), gg_s.at[t], gg_r.at[t], chip_dev(t))

    def gf_send(t):
        return copy(line(t, c), line(t, c), gf_s.at[t], gf_r.at[t], core_dev)

    def gf_recv(t):
        return copy(line(t, 1 - c), line(t, 1 - c), gf_s.at[t], gf_r.at[t], core_dev)

    chips(lambda t: g_send(t).start())
    gf_send(q).start()

    for part in range(3):
        swap(8, z, lambda t, part=part: v_recv(part, t).wait_recv())
    others = jnp.sum(rv[0].astype(F32) + rv[1].astype(F32), axis=0)
    mine = -(v_f[:, rows(z * 16, 16), :] + others)
    m_high, m_low = split2(mine)
    own = vall.at[:, rows(z * 16, 16), :]
    own[:, :, :ROWS] = m_high
    own[:, :, ROWS:] = m_low

    def vg_send(t):
        return copy(own, own, vg_s.at[t], vg_r.at[z], z_dev(t))

    def vg_recv(t):
        theirs = vall.at[:, rows(t * 16, 16), :]
        return copy(theirs, theirs, vg_s.at[t], vg_r.at[t], z_dev(t))

    z_line(lambda t: vg_send(t).start())

    def g_pass_on(t):
        g_recv(t).wait_recv()
        gf_send(t).start()

    chips(g_pass_on)

    def d_send(n, t):
        return copy(dd.at[n, rows(t * 8, 8)], rp.at[n, rows(p * 8, 8)], d_s.at[n, t], d_r.at[n, p], half_dev(t))

    def d_recv(n, t):
        return copy(dd.at[n, rows(t * 8, 8)], rp.at[n, rows(t * 8, 8)], d_s.at[n, t], d_r.at[n, t], half_dev(t))

    def deal(n, value):
        for k in range(3):
            tt[n, k] = value[:, k * 128 : (k + 1) * 128]
        even, odd = (
            jnp.concatenate([tt[n, k, pl.ds(o, 16, stride=2), :] for k in range(3)], axis=1)
            for o in range(2)
        )
        gap = jnp.zeros((16, 16), F32)
        for k in range(8):
            cells = slice(48 * k, 48 * k + 48)
            dd[n, pl.ds(k, 16, stride=8), :] = jnp.concatenate(
                [even[:, cells], gap, odd[:, cells], gap], axis=1
            )
        half(lambda t: d_send(n, t).start())
        rp[n, rows(p * 8, 8)] = dd[n, rows(p * 8, 8)]

    def land(n, out):
        swap(16, p, lambda t: d_recv(n, t).wait_recv())
        table = jnp.concatenate([rp[n, pl.ds(k, 16, stride=8), :] for k in range(8)], axis=0)
        turned = table.T
        for k in range(45):
            out[:, k * 128 : (k + 1) * 128] = jnp.concatenate(
                [turned[k : k + 1], turned[64 + k : 65 + k]], axis=0
            )

    deal(0, mine.reshape(32, ROWS))
    each(16, lambda t: gf_recv(t).wait_recv())
    half_send().wait_send()
    swap(16, q, lambda t: g_send(t).wait_send())
    each(16, lambda t: gf_send(t).wait_send())
    a = gram[...]
    gram[...] = (a + a.T) * 0.5
    eliminate(gram)
    l_rows = jnp.concatenate([gram[rows(k * 128 + z * 16, 16), :] for k in range(2)], axis=0)
    l_both = jnp.concatenate(split2(l_rows), axis=0)
    swap(8, z, lambda t: vg_recv(t).wait_recv())
    out = dot(l_both, vall[...].reshape(NORB, 2 * ROWS))
    deal(1, out[:32, :ROWS] + out[32:, :ROWS] + out[:32, ROWS:])
    land(0, ov)
    for group, i, sends in (
        (8, z, (z_send, zg_send, *(functools.partial(v_send, k) for k in range(3)), gz_send, vg_send)),
        (16, p, (p_send, functools.partial(d_send, 0))),
        (16, q, (c_send, a_send)),
    ):
        for send in sends:
            swap(group, i, lambda t, send=send: send(t).wait_send())
    each(16, lambda t: f_send(t).wait_send())
    land(1, oq)
    swap(16, p, lambda t: d_send(1, t).wait_send())


def eliminate(work):
    sub = lax.broadcasted_iota(jnp.int32, (8, 128), 0)
    lane = lax.broadcasted_iota(jnp.int32, (8, 128), 1)
    wide = lambda col: jnp.broadcast_to(col, (8, 128))
    for k in range(8):
        base = 32 * k
        tile, off = base // 128, base % 128
        wk = [
            [work[base + 8 * g : base + 8 * g + 8, 128 * t : 128 * t + 128] for t in range(2)]
            for g in range(4)
        ]
        col = [
            [wide(wk[g][tile][:, off + j : off + j + 1]) if g >= j // 8 else None for g in range(4)]
            for j in range(32)
        ]
        inside = (lane >= off) & (lane < off + 32)
        for g in range(4):
            unit = jnp.where(lane - off == sub + 8 * g, 1.0, 0.0)
            wk[g][tile] = jnp.where(inside, unit, wk[g][tile])
        pivots = [jnp.ones((8, 128), F32) for _ in range(4)]
        for j in range(0, 32, 2):
            gj, sj = j // 8, j % 8
            u, v = col[j], col[j + 1]
            p11 = wide(u[gj][sj : sj + 1, :])
            p21 = wide(u[gj][sj + 1 : sj + 2, :])
            p22 = wide(v[gj][sj + 1 : sj + 2, :])
            det = p11 * p22 - p21 * p21
            r = 1.0 / det
            r11 = 1.0 / p11
            pivots[gj] = jnp.where(sub == sj, p11, jnp.where(sub == sj + 1, det * r11, pivots[gj]))
            q11, q21, q22 = p22 * r, p21 * r, p11 * r
            al, be = [None] * 4, [None] * 4
            for g in range(gj, 4):
                al[g] = u[g] * q11 - v[g] * q21
                be[g] = v[g] * q22 - u[g] * q21
            below = sub > sj + 1
            be[gj] = jnp.where(below, be[gj], 0.0)
            al[gj] = jnp.where(below, al[gj], jnp.where(sub == sj + 1, p21 * r11, 0.0))
            for i in range(j + 2, 32):
                fu = wide(u[i // 8][i % 8 : i % 8 + 1, :])
                fv = wide(v[i // 8][i % 8 : i % 8 + 1, :])
                for g in range(i // 8, 4):
                    col[i][g] = col[i][g] - (al[g] * fu + be[g] * fv)
            for t in range(2):
                one = wide(wk[gj][t][sj : sj + 1, :])
                two = wide(wk[gj][t][sj + 1 : sj + 2, :])
                for g in range(gj, 4):
                    wk[g][t] = wk[g][t] - (al[g] * one + be[g] * two)
        for g in range(4):
            scale = lax.rsqrt(pivots[g])
            for t in range(2):
                wk[g][t] = wk[g][t] * scale
        u = jnp.concatenate([jnp.concatenate(wk[g], axis=1) for g in range(4)], axis=0)
        lanes = lax.broadcasted_iota(jnp.int32, (32, 256), 1)
        work[base : base + 32, :] = jnp.where(lanes < base + 32, u, 0.0)
        if k < 7:
            u_high, u_low = split2(u)
            one = jnp.concatenate([u_high, u_low, u_high], axis=0)
            two = jnp.concatenate([u_high, u_high, u_low], axis=0)
            edge = base + 32
            start = edge // 128 * 128
            change = dot(one[:, start:].T, two)[edge - start :]
            rest = work[edge:, :]
            lanes = lax.broadcasted_iota(jnp.int32, rest.shape, 1)
            rest = jnp.where((lanes >= base) & (lanes < edge), 0.0, rest)
            work[edge:, :] = rest - change


VM = pl.BlockSpec(memory_space=pltpu.VMEM)
ANY = pl.BlockSpec(memory_space=pl.ANY)
DMA = pltpu.SemaphoreType.DMA


def call(kernel, args, outs, scratch, number, name):
    return pl.pallas_call(
        kernel,
        out_shape=[jax.ShapeDtypeStruct(s, d) for s, d in outs],
        in_specs=[ANY] * len(args),
        out_specs=[VM] * len(outs),
        scratch_shapes=scratch,
        compiler_params=pltpu.CompilerParams(
            vmem_limit_bytes=60 * 1024 * 1024, collective_id=number, has_side_effects=True
        ),
        name=name,
    )(*args)


def on_device(orbitals, occupation):
    st = orbitals.astype(F32).reshape(2, 10, 8, 3, NZ).transpose(2, 0, 3, 1, 4).reshape(8, 2, 3, 240)
    st = jnp.pad(st, ((0, 0), (0, 0), (0, 5), (0, 16)))
    occ = jnp.broadcast_to(occupation.astype(F32)[:, None], (2, 128))
    vm = pltpu.VMEM
    return tuple(call(
        main_kernel, (st, orbitals, occ, permutations(), *tables()),
        (((2, HALF), F32), ((2, HALF), F32)),
        [vm((8, 2, 8, 256), F32), vm((2, HALF), BF16), vm((2, 128), F32),
         vm((8, 16, 128), F32), vm((16, 8, 128), F32), vm((128, 128), F32), vm((128, 128), F32), vm((NORB, 512), BF16), vm((128, 3 * MODES), BF16),
         vm((128, 128), BF16), vm((MODES, 1024), BF16), vm((32, 128), F32), DMA((8,)),
         vm((2, NORB, 768), BF16), vm((NORB, ROWS), BF16), vm((128, 128), F32), vm((128, 128), F32),
         vm((2, ROWS, 768), F32), vm((ROWS, MODES), F32), vm((ROWS, 128), F32),
         vm((2, 128, ROWS), F32), vm((2, 2, 128, ROWS), BF16), vm((NORB, NORB), F32),
         vm((128, NORB), F32), vm((128, NORB), F32), vm((16, 8, NORB), F32),
         vm((2, 8, 2, 16, ROWS), BF16), vm((8, NORB), F32), vm((8, 8, NORB), F32),
         vm((NORB, NORB), F32), vm((2, 128, 2 * ROWS), BF16), vm((2, 3, 32, 128), F32),
         vm((2, 128, 128), F32), vm((2, 128, 128), F32),
         DMA((8,)), DMA((8,)), DMA((16,)), DMA((16,)), DMA((16,)), DMA((16,)), DMA((16,)), DMA((16,)),
         DMA((8,)), DMA((8,)), DMA, DMA, DMA((16,)), DMA((16,)), DMA((3, 8)), DMA((3, 8)),
         DMA((8,)), DMA((8,)), DMA((16,)), DMA((16,)), DMA((16,)), DMA((16,)),
         DMA((8,)), DMA((8,)), DMA((2, 16)), DMA((2, 16))],
        0, "exchange",
    ))


def solution(mesh):
    torus = Mesh(mesh.devices.reshape(2, 8, 4, 2, mesh.shape["grid"]), AXES)
    return jax.shard_map(
        on_device,
        mesh=torus,
        in_specs=(P(ORB, "h"), P(ORB)),
        out_specs=(P(ORB, "h"), P(ORB, "h")),
        check_vma=False,
    )
```

```python
import functools
import math

import jax
import jax.numpy as jnp
import numpy as np
from jax import lax
from jax.experimental import pallas as pl
from jax.experimental.pallas import tpu as pltpu
from jax.sharding import Mesh
from jax.sharding import PartitionSpec as P

NX = 20
NY = 24
NZ = 24
NORB = 256
NPTS = 11520
HALF = NPTS // 2
MODES = 512
ROWS = 384
AXES = ("xl", "z", "y", "c", "h")
ORB = ("xl", "z", "y", "c")
MESH = pl.DeviceIdType.MESH
F32 = jnp.float32
BF16 = jnp.bfloat16


def rounded(a):
    return np.asarray(a, np.float32).astype(jnp.bfloat16).astype(np.float32)


def hartley_table(length):
    index = np.arange(length)
    angle = 2.0 * math.pi / length * (index[:, None] * index[None, :] % length)
    return rounded(np.cos(angle) + np.sin(angle))


def signed_square(length):
    index = np.arange(length)
    signed = np.where(index <= length // 2, index, index - length)
    return (2.0 * math.pi * signed / length) ** 2


def coulomb_kernel():
    total = (
        signed_square(NX)[:, None, None]
        + signed_square(NY)[None, :, None]
        + signed_square(NZ)[None, None, :]
    )
    return np.where(total > 0, 1.0 / np.where(total > 0, total, 1.0), 0.0) / NPTS


def two_parts(a):
    high = rounded(a)
    return high, rounded(a - high)


def tables():
    cx, cy, cz = hartley_table(NX), hartley_table(NY), hartley_table(NZ)
    kernel = coulomb_kernel()
    ac = NX * NZ
    tx = np.zeros((128, MODES), np.float32)
    tx[:NX, :ac] = np.repeat(cx, NZ, axis=1)
    tz = np.zeros((128, MODES), np.float32)
    tz[:NZ, :ac] = np.tile(cz, (1, NX))
    ty = np.zeros((128, 128), np.float32)
    tk = np.zeros((128, MODES), np.float32)
    k_high, k_low = two_parts(kernel.transpose(1, 0, 2).reshape(NY, ac))
    for at, part in ((0, k_high), (32, k_high), (64, k_low)):
        ty[:NY, at : at + NY] = cy
        tk[at : at + NY, :ac] = part
    phi = np.einsum("ax,cz->acxz", cx, cz).reshape(ac, NX, NZ)
    right = np.zeros((MODES, 2, 256), np.float32)
    for h in range(2):
        right[:ac, h, :240] = phi[:, 10 * h : 10 * h + 10].reshape(ac, 240)
    r_high, r_low = two_parts(right.reshape(MODES, 512))
    bf = lambda a: jnp.asarray(a, BF16)
    three = np.concatenate([tx, tz, tk], axis=1)
    return bf(three), bf(ty), bf(np.concatenate([r_high, r_low], axis=1)), jnp.asarray(ty[:32], F32)


def permutations():
    true = np.arange(NORB).reshape(2, 8, 8, 2)
    order_a = true.transpose(0, 2, 1, 3).reshape(-1)
    order_b = true.transpose(1, 3, 0, 2).reshape(-1)
    eye = np.eye(NORB, dtype=np.float32)
    return jnp.asarray(np.concatenate([eye[:, order_a], eye[:, order_b]], axis=1), BF16)


def split2(a):
    high = a.astype(BF16)
    return high, (a - high.astype(F32)).astype(BF16)


def dot(a, b, dims=(1, 0)):
    return lax.dot_general(
        a, b, (((dims[0],), (dims[1],)), ((), ())), preferred_element_type=F32
    )


def me():
    return tuple(lax.axis_index(a) for a in AXES)


def of_plane(pid, z):
    return ((pid // 8) % 2, z, (pid // 2) % 4, pid % 2, pid // 16)


def copy(src, dst, send_sem, recv_sem, device):
    return pltpu.make_async_remote_copy(
        src_ref=src, dst_ref=dst, send_sem=send_sem, recv_sem=recv_sem,
        device_id=device, device_id_type=MESH,
    )


def rows(start, size):
    return pl.ds(pl.multiple_of(start, size), size)


def each(count, body):
    lax.fori_loop(0, count, lambda i, carry: (body(i), carry)[1], 0)


def swap(n, i, body):
    each(n - 1, lambda d: body((i + d + 1) % n))


Z_ORDER = (4, 3, 5, 2, 6, 1, 7)
CHIP_ORDER = (
    (2, 2), (2, 1), (2, 3), (1, 2), (3, 2), (1, 1), (1, 3), (3, 1), (3, 3),
    (2, 0), (0, 2), (1, 0), (3, 0), (0, 1), (0, 3),
)
HALF_ORDER = tuple((a, b, k) for a, b in ((1, 2), (1, 1), (1, 3), (0, 2), (1, 0), (0, 1), (0, 3)) for k in range(2)) + ((0, 0, 1),)


def greet(barrier, n, i, device):
    swap(n, i, lambda t: pl.semaphore_signal(barrier, inc=1, device_id=device(t), device_id_type=MESH))
    return n - 1


def shifted(a, factor, shift):
    return lax.shift_right_logical(a * factor, shift)


def main_kernel(
    st_any, raw_any, perm_any, t_any, ty_any, right_any, cy_any, results,
    st, raw, s1, s2, cells, turned_cells, perm, t3, ty, right, cy, in_s,
    o1, o2, r1, r2, green, left, y_rows, v_f, v_b, gp, gc, gh, rg, rv, s8, rz,
    gram, vall, tt, dd, rp,
    za_s, za_r, pa_s, pa_r, cg_s, cg_r, cf_s, cf_r, zg_s, zg_r,
    gc_s, gc_r, ga_s, ga_r, va_s, va_r, gz_s, gz_r, gg_s, gg_r, gf_s, gf_r,
    vg_s, vg_r, d_s, d_r,
):
    xl, z, y, c, h = me()
    p = xl * 8 + y * 2 + c
    q = h * 8 + xl * 4 + y
    z_dev = lambda t: (xl, t, y, c, h)
    half_dev = lambda t: of_plane(h * 16 + t, z)
    chip_dev = lambda t: ((t // 4) % 2, z, t % 4, c, t // 8)
    core_dev = (xl, z, y, 1 - c, h)

    def z_line(body):
        for d in Z_ORDER:
            body((z + d) % 8)

    def chips(body):
        for dx, dy in CHIP_ORDER:
            body((q // 4 + dx) % 4 * 4 + (y + dy) % 4)

    def half(body):
        for dx, dy, dc in HALF_ORDER:
            body((xl + dx) % 2 * 8 + (y + dy) % 4 * 2 + (c + dc) % 2)

    barrier = pltpu.get_barrier_semaphore()
    greeted = greet(barrier, 8, z, z_dev) + greet(barrier, 16, p, half_dev)
    greeted += greet(barrier, 16, q, chip_dev)
    pl.semaphore_signal(barrier, inc=1, device_id=core_dev, device_id_type=MESH)

    held = (
        (raw_any, raw), (st_any, st), (t_any, t3), (ty_any, ty), (cy_any, cy),
        (right_any, right), (perm_any, perm),
    )
    held = [pltpu.make_async_copy(a, b, in_s.at[k]) for k, (a, b) in enumerate(held)]
    for one in held:
        one.start()
    perm_a, perm_b = perm.at[:, :NORB], perm.at[:, NORB:]
    tx, tz, tk = (t3.at[:, k * MODES : (k + 1) * MODES] for k in range(3))
    rh, rl = right.at[:, :512], right.at[:, 512:]
    for one in held[:2]:
        one.wait()
    cells[...] = jnp.zeros_like(cells)
    for k in range(45):
        pair = raw[:, k * 128 : (k + 1) * 128].astype(F32)
        for o in range(2):
            cells[64 * o + k : 64 * o + k + 1, :] = pair[o : o + 1]
    for o in range(2):
        cells[64 * o + 45 : 64 * o + 46, :] = st[0, o, 3:4, :128]
    turned_cells[...] = cells[...].T
    for k in range(16):
        s2[k] = turned_cells[pl.ds(k, 8, stride=16), :]
    for k in range(8):
        for o in range(2):
            for part in range(2):
                s1[k, pl.ds(8 * o + part, 4, stride=2), :] = st[k, o, :4, 128 * part : 128 * part + 128]
    for one in held[2:5]:
        one.wait()

    row = lax.broadcasted_iota(jnp.int32, (ROWS, 128), 0)
    lane = lax.broadcasted_iota(jnp.int32, (ROWS, 128), 1)
    zz = shifted(row, 1366, 16)
    s = row - zz * 48
    cell = h * HALF + s * 128 + zz * 16 + p
    x = shifted(cell, 7282, 22)
    yz = cell - x * (NY * NZ)
    y_cell = shifted(yz, 2731, 16)
    z_cell = yz - y_cell * NZ
    hot = lambda a: jnp.where(a == lane, 1.0, 0.0).astype(BF16)
    left[...] = dot(hot(jnp.where(s < 45, x, 127)), tx[...]) * dot(hot(z_cell), tz[...])
    y_rows[...] = dot(hot(y_cell), ty[...])
    middle = (lane >= 32) & (lane < 64)

    def green_part(t):
        k_high, k_low = split2(y_rows[...] * cy[pl.ds(z * 3 + t, 1), :])
        mix = jnp.where(middle, k_low.astype(F32), k_high.astype(F32)).astype(BF16)
        l_high, l_low = split2(left[...] * dot(mix, tk[...]))
        g = dot(l_high, rh[...]) + dot(l_low, rh[...]) + dot(l_high, rl[...])
        for hh in range(2):
            green[hh, :, t * 256 : (t + 1) * 256] = g[:, hh * 256 : (hh + 1) * 256]

    pl.semaphore_wait(barrier, greeted + 1)

    def z_send(t):
        return copy(s1.at[t], r1.at[rows(z * 16, 16)], za_s.at[t], za_r.at[z], z_dev(t))

    def z_recv(t):
        return copy(s1.at[t], r1.at[rows(t * 16, 16)], za_s.at[t], za_r.at[t], z_dev(t))

    def p_send(t):
        return copy(s2.at[t], r2.at[rows(p * 8, 8)], pa_s.at[t], pa_r.at[p], half_dev(t))

    def p_recv(t):
        return copy(s2.at[t], r2.at[rows(t * 8, 8)], pa_s.at[t], pa_r.at[t], half_dev(t))

    half(lambda t: p_send(t).start())
    z_line(lambda t: z_send(t).start())
    r1[rows(z * 16, 16)] = s1[z]
    r2[rows(p * 8, 8)] = s2[p]
    for one in held[5:]:
        one.wait()
    green_part(0)
    swap(16, p, lambda t: p_recv(t).wait_recv())
    by_row = [r2[pl.ds(k, 16, stride=8), :] for k in range(8)]
    o2[rows(z * 32, 32), :] = jnp.concatenate(
        [jnp.concatenate([b[:, 64 * o : 64 * o + 48] for b in by_row], axis=1) for o in range(2)], axis=0
    ).astype(BF16)

    def zg_send(t):
        mine = o2.at[rows(z * 32, 32)]
        return copy(mine, mine, zg_s.at[t], zg_r.at[z], z_dev(t))

    def zg_recv(t):
        theirs = o2.at[rows(t * 32, 32)]
        return copy(theirs, theirs, zg_s.at[t], zg_r.at[t], z_dev(t))

    z_line(lambda t: zg_send(t).start())
    swap(8, z, lambda t: z_recv(t).wait_recv())
    for t in range(3):
        o1[h, rows(p * 16, 16), t * 256 : (t + 1) * 256] = jnp.concatenate(
            [r1[pl.ds(2 * t + k, 16, stride=8), :] for k in range(2)], axis=1
        ).astype(BF16)

    def block(t, core):
        return o1.at[t // 8, rows(((t // 4) % 2 * 8 + t % 4 * 2 + core) * 16, 16)]

    def c_send(t):
        return copy(block(q, c), block(q, c), cg_s.at[t], cg_r.at[q], chip_dev(t))

    def c_recv(t):
        return copy(block(t, c), block(t, c), cg_s.at[t], cg_r.at[t], chip_dev(t))

    def f_send(t):
        return copy(block(t, c), block(t, c), cf_s.at[t], cf_r.at[t], core_dev)

    def f_recv(t):
        return copy(block(t, 1 - c), block(t, 1 - c), cf_s.at[t], cf_r.at[t], core_dev)

    chips(lambda t: c_send(t).start())
    f_send(q).start()
    green_part(1)
    green_part(2)

    def pass_on(t):
        c_recv(t).wait_recv()
        f_send(t).start()

    chips(pass_on)
    swap(8, z, lambda t: zg_recv(t).wait_recv())
    o_rows = dot(perm_b[...], o2[...])
    o_b = o_rows.astype(BF16)
    w = (o_rows * o_rows[:, 45:46]).astype(BF16).T
    each(16, lambda t: f_recv(t).wait_recv())

    v = jnp.zeros((NORB, ROWS), F32)
    for hh in range(2):
        orb = dot(perm_a[...], o1[hh]).astype(BF16)
        m_high, m_low = split2(green[hh] * dot(w, orb))
        v = v + dot(orb, m_high, (1, 1)) + dot(orb, m_low, (1, 1))
    v_high, v_low = split2(v)
    gp[...] = (dot(o_b, v_high, (1, 1)) + dot(o_b, v_low, (1, 1))) * (1.0 / NPTS)

    def half_send():
        other = gp.at[rows((1 - c) * 128, 128)]
        return copy(other, gc, gc_s, gc_r, core_dev)

    def v_send(part, t):
        if part == 0:
            src, dst = v_b.at[0, :, rows(t * 16, 16), :], rv.at[0, z]
        else:
            src, dst = v_b.at[1, part - 1, rows(t * 16, 16), :], rv.at[1, z, part - 1]
        return copy(src, dst, va_s.at[part, t], va_r.at[part, z], z_dev(t))

    def v_recv(part, t):
        if part == 0:
            src, dst = v_b.at[0, :, rows(t * 16, 16), :], rv.at[0, t]
        else:
            src, dst = v_b.at[1, part - 1, rows(t * 16, 16), :], rv.at[1, t, part - 1]
        return copy(src, dst, va_s.at[part, t], va_r.at[part, t], z_dev(t))

    half_send().start()
    for part, value in ((0, v_high), (1, v_low)):
        v_b[part] = value.reshape(2, 128, ROWS)
    v_f[...] = v.reshape(2, 128, ROWS)
    z_line(lambda t: v_send(0, t).start())
    z_line(lambda t: v_send(1, t).start())
    half_send().wait_recv()
    gh[...] = gp[rows(c * 128, 128)] + gc[...]

    def a_send(t):
        return copy(gh.at[rows(t * 8, 8)], rg.at[q], ga_s.at[t], ga_r.at[q], chip_dev(t))

    def a_recv(t):
        return copy(gh.at[rows(t * 8, 8)], rg.at[t], ga_s.at[t], ga_r.at[t], chip_dev(t))

    chips(lambda t: a_send(t).start())
    rg[q] = gh[rows(q * 8, 8)]
    for part in range(2):
        rv[part, z] = jnp.zeros((2, 16, ROWS), BF16)
    swap(16, q, lambda t: a_recv(t).wait_recv())
    s8[...] = jnp.sum(rg[...], axis=0)

    def gz_send(t):
        return copy(s8, rz.at[z], gz_s.at[t], gz_r.at[z], z_dev(t))

    def gz_recv(t):
        return copy(s8, rz.at[t], gz_s.at[t], gz_r.at[t], z_dev(t))

    z_line(lambda t: gz_send(t).start())
    z_line(lambda t: v_send(2, t).start())
    rz[z] = s8[...]
    swap(8, z, lambda t: gz_recv(t).wait_recv())

    def line(t, core):
        return gram.at[rows(core * 128 + t * 8, 8)]

    gram[rows(c * 128 + q * 8, 8)] = jnp.sum(rz[...], axis=0)

    def g_send(t):
        return copy(line(q, c), line(q, c), gg_s.at[t], gg_r.at[q], chip_dev(t))

    def g_recv(t):
        return copy(line(t, c), line(t, c), gg_s.at[t], gg_r.at[t], chip_dev(t))

    def gf_send(t):
        return copy(line(t, c), line(t, c), gf_s.at[t], gf_r.at[t], core_dev)

    def gf_recv(t):
        return copy(line(t, 1 - c), line(t, 1 - c), gf_s.at[t], gf_r.at[t], core_dev)

    chips(lambda t: g_send(t).start())
    gf_send(q).start()

    for part in range(3):
        swap(8, z, lambda t, part=part: v_recv(part, t).wait_recv())
    others = jnp.sum(rv[0].astype(F32) + rv[1].astype(F32), axis=0)
    mine = v_f[:, rows(z * 16, 16), :] + others
    m_high, m_low = split2(mine)
    own = vall.at[:, rows(z * 16, 16), :]
    own[:, :, :ROWS] = m_high
    own[:, :, ROWS:] = m_low

    def vg_send(t):
        return copy(own, own, vg_s.at[t], vg_r.at[z], z_dev(t))

    def vg_recv(t):
        theirs = vall.at[:, rows(t * 16, 16), :]
        return copy(theirs, theirs, vg_s.at[t], vg_r.at[t], z_dev(t))

    z_line(lambda t: vg_send(t).start())

    def g_pass_on(t):
        g_recv(t).wait_recv()
        gf_send(t).start()

    chips(g_pass_on)

    def d_send(n, t):
        return copy(dd.at[n, rows(t * 8, 8)], rp.at[n, rows(p * 8, 8)], d_s.at[n, t], d_r.at[n, p], half_dev(t))

    def d_recv(n, t):
        return copy(dd.at[n, rows(t * 8, 8)], rp.at[n, rows(t * 8, 8)], d_s.at[n, t], d_r.at[n, t], half_dev(t))

    def deal(n, value):
        for k in range(3):
            tt[n, k] = value[:, k * 128 : (k + 1) * 128]
        even, odd = (
            jnp.concatenate([tt[n, k, pl.ds(o, 16, stride=2), :] for k in range(3)], axis=1)
            for o in range(2)
        )
        gap = jnp.zeros((16, 16), F32)
        for k in range(8):
            cells = slice(48 * k, 48 * k + 48)
            dd[n, pl.ds(k, 16, stride=8), :] = jnp.concatenate(
                [even[:, cells], gap, odd[:, cells], gap], axis=1
            )
        half(lambda t: d_send(n, t).start())
        rp[n, rows(p * 8, 8)] = dd[n, rows(p * 8, 8)]

    def land(n):
        swap(16, p, lambda t: d_recv(n, t).wait_recv())
        table = jnp.concatenate([rp[n, pl.ds(k, 16, stride=8), :] for k in range(8)], axis=0)
        turned = table.T
        for k in range(45):
            results[n, :, k * 128 : (k + 1) * 128] = jnp.concatenate(
                [turned[k : k + 1], turned[64 + k : 65 + k]], axis=0
            )

    deal(0, mine.reshape(32, ROWS))
    each(16, lambda t: gf_recv(t).wait_recv())
    half_send().wait_send()
    swap(16, q, lambda t: g_send(t).wait_send())
    each(16, lambda t: gf_send(t).wait_send())
    a = gram[...]
    gram[...] = (a + a.T) * 0.5
    eliminate(gram)
    l_rows = jnp.concatenate([gram[rows(k * 128 + z * 16, 16), :] for k in range(2)], axis=0)
    l_both = jnp.concatenate(split2(l_rows), axis=0)
    swap(8, z, lambda t: vg_recv(t).wait_recv())
    out = dot(l_both, vall[...].reshape(NORB, 2 * ROWS))
    deal(1, out[:32, :ROWS] + out[32:, :ROWS] + out[:32, ROWS:])
    land(0)
    for group, i, sends in (
        (8, z, (z_send, zg_send, *(functools.partial(v_send, k) for k in range(3)), gz_send, vg_send)),
        (16, p, (p_send, functools.partial(d_send, 0))),
        (16, q, (c_send, a_send)),
    ):
        for send in sends:
            swap(group, i, lambda t, send=send: send(t).wait_send())
    each(16, lambda t: f_send(t).wait_send())
    land(1)
    swap(16, p, lambda t: d_send(1, t).wait_send())


def eliminate(work):
    sub = lax.broadcasted_iota(jnp.int32, (8, 128), 0)
    lane = lax.broadcasted_iota(jnp.int32, (8, 128), 1)
    wide = lambda col: jnp.broadcast_to(col, (8, 128))
    for k in range(8):
        base = 32 * k
        tile, off = base // 128, base % 128
        wk = [
            [work[base + 8 * g : base + 8 * g + 8, 128 * t : 128 * t + 128] for t in range(2)]
            for g in range(4)
        ]
        col = [
            [wide(wk[g][tile][:, off + j : off + j + 1]) if g >= j // 8 else None for g in range(4)]
            for j in range(32)
        ]
        inside = (lane >= off) & (lane < off + 32)
        for g in range(4):
            unit = jnp.where(lane - off == sub + 8 * g, 1.0, 0.0)
            wk[g][tile] = jnp.where(inside, unit, wk[g][tile])
        pivots = [jnp.ones((8, 128), F32) for _ in range(4)]
        for j in range(0, 32, 2):
            gj, sj = j // 8, j % 8
            u, v = col[j], col[j + 1]
            p11 = wide(u[gj][sj : sj + 1, :])
            p21 = wide(u[gj][sj + 1 : sj + 2, :])
            p22 = wide(v[gj][sj + 1 : sj + 2, :])
            det = p11 * p22 - p21 * p21
            r = 1.0 / det
            r11 = 1.0 / p11
            pivots[gj] = jnp.where(sub == sj, p11, jnp.where(sub == sj + 1, det * r11, pivots[gj]))
            q11, q21, q22 = p22 * r, p21 * r, p11 * r
            al, be = [None] * 4, [None] * 4
            for g in range(gj, 4):
                al[g] = u[g] * q11 - v[g] * q21
                be[g] = v[g] * q22 - u[g] * q21
            below = sub > sj + 1
            be[gj] = jnp.where(below, be[gj], 0.0)
            al[gj] = jnp.where(below, al[gj], jnp.where(sub == sj + 1, p21 * r11, 0.0))
            for i in range(j + 2, 32):
                fu = wide(u[i // 8][i % 8 : i % 8 + 1, :])
                fv = wide(v[i // 8][i % 8 : i % 8 + 1, :])
                for g in range(i // 8, 4):
                    col[i][g] = col[i][g] - (al[g] * fu + be[g] * fv)
            for t in range(2):
                one = wide(wk[gj][t][sj : sj + 1, :])
                two = wide(wk[gj][t][sj + 1 : sj + 2, :])
                for g in range(gj, 4):
                    wk[g][t] = wk[g][t] - (al[g] * one + be[g] * two)
        for g in range(4):
            scale = lax.rsqrt(pivots[g])
            for t in range(2):
                wk[g][t] = wk[g][t] * scale
        u = jnp.concatenate([jnp.concatenate(wk[g], axis=1) for g in range(4)], axis=0)
        lanes = lax.broadcasted_iota(jnp.int32, (32, 256), 1)
        work[base : base + 32, :] = jnp.where(lanes < base + 32, u, 0.0)
        if k < 7:
            u_high, u_low = split2(u)
            one = jnp.concatenate([u_high, u_low, u_high], axis=0)
            two = jnp.concatenate([u_high, u_high, u_low], axis=0)
            edge = base + 32
            start = edge // 128 * 128
            change = dot(one[:, start:].T, two)[edge - start :]
            rest = work[edge:, :]
            lanes = lax.broadcasted_iota(jnp.int32, rest.shape, 1)
            rest = jnp.where((lanes >= base) & (lanes < edge), 0.0, rest)
            work[edge:, :] = rest - change


VM = pl.BlockSpec(memory_space=pltpu.VMEM)
ANY = pl.BlockSpec(memory_space=pl.ANY)
DMA = pltpu.SemaphoreType.DMA


def call(kernel, args, outs, scratch, number, name):
    return pl.pallas_call(
        kernel,
        out_shape=[jax.ShapeDtypeStruct(s, d) for s, d in outs],
        in_specs=[ANY] * len(args),
        out_specs=[VM] * len(outs),
        scratch_shapes=scratch,
        compiler_params=pltpu.CompilerParams(
            vmem_limit_bytes=60 * 1024 * 1024, collective_id=number, has_side_effects=True
        ),
        name=name,
    )(*args)


def on_device(orbitals, occupation):
    st = orbitals.astype(F32).reshape(2, 10, 8, 3, NZ).transpose(2, 0, 3, 1, 4).reshape(8, 2, 3, 240)
    st = jnp.pad(st, ((0, 0), (0, 0), (0, 5), (0, 16)))
    spare = lax.broadcasted_iota(jnp.int32, st.shape, 2) == 3
    st = jnp.where(spare, occupation.astype(F32)[None, :, None, None], st)
    vm = pltpu.VMEM
    both = call(
        main_kernel, (st, orbitals, permutations(), *tables()),
        (((2, 2, HALF), F32),),
        [vm((8, 2, 8, 256), F32), vm((2, HALF), BF16),
         vm((8, 16, 128), F32), vm((16, 8, 128), F32), vm((128, 128), F32), vm((128, 128), F32), vm((NORB, 512), BF16), vm((128, 3 * MODES), BF16),
         vm((128, 128), BF16), vm((MODES, 1024), BF16), vm((32, 128), F32), DMA((8,)),
         vm((2, NORB, 768), BF16), vm((NORB, ROWS), BF16), vm((128, 128), F32), vm((128, 128), F32),
         vm((2, ROWS, 768), F32), vm((ROWS, MODES), F32), vm((ROWS, 128), F32),
         vm((2, 128, ROWS), F32), vm((2, 2, 128, ROWS), BF16), vm((NORB, NORB), F32),
         vm((128, NORB), F32), vm((128, NORB), F32), vm((16, 8, NORB), F32),
         vm((2, 8, 2, 16, ROWS), BF16), vm((8, NORB), F32), vm((8, 8, NORB), F32),
         vm((NORB, NORB), F32), vm((2, 128, 2 * ROWS), BF16), vm((2, 3, 32, 128), F32),
         vm((2, 128, 128), F32), vm((2, 128, 128), F32),
         DMA((8,)), DMA((8,)), DMA((16,)), DMA((16,)), DMA((16,)), DMA((16,)), DMA((16,)), DMA((16,)),
         DMA((8,)), DMA((8,)), DMA, DMA, DMA((16,)), DMA((16,)), DMA((3, 8)), DMA((3, 8)),
         DMA((8,)), DMA((8,)), DMA((16,)), DMA((16,)), DMA((16,)), DMA((16,)),
         DMA((8,)), DMA((8,)), DMA((2, 16)), DMA((2, 16))],
        0, "exchange",
    )[0]
    return -both[0], -both[1]


def solution(mesh):
    torus = Mesh(mesh.devices.reshape(2, 8, 4, 2, mesh.shape["grid"]), AXES)
    return jax.shard_map(
        on_device,
        mesh=torus,
        in_specs=(P(ORB, "h"), P(ORB)),
        out_specs=(P(ORB, "h"), P(ORB, "h")),
        check_vma=False,
    )
```

```python
import functools
import math

import jax
import jax.numpy as jnp
import numpy as np
from jax import lax
from jax.experimental import pallas as pl
from jax.experimental.pallas import tpu as pltpu
from jax.sharding import Mesh
from jax.sharding import PartitionSpec as P

NX = 20
NY = 24
NZ = 24
NORB = 256
NPTS = 11520
HALF = NPTS // 2
MODES = 512
ROWS = 384
AXES = ("xl", "z", "y", "c", "h")
ORB = ("xl", "z", "y", "c")
MESH = pl.DeviceIdType.MESH
F32 = jnp.float32
BF16 = jnp.bfloat16


def rounded(a):
    return np.asarray(a, np.float32).astype(jnp.bfloat16).astype(np.float32)


def hartley_table(length):
    index = np.arange(length)
    angle = 2.0 * math.pi / length * (index[:, None] * index[None, :] % length)
    return rounded(np.cos(angle) + np.sin(angle))


def signed_square(length):
    index = np.arange(length)
    signed = np.where(index <= length // 2, index, index - length)
    return (2.0 * math.pi * signed / length) ** 2


def coulomb_kernel():
    total = (
        signed_square(NX)[:, None, None]
        + signed_square(NY)[None, :, None]
        + signed_square(NZ)[None, None, :]
    )
    return np.where(total > 0, 1.0 / np.where(total > 0, total, 1.0), 0.0) / NPTS


def two_parts(a):
    high = rounded(a)
    return high, rounded(a - high)


def tables():
    cx, cy, cz = hartley_table(NX), hartley_table(NY), hartley_table(NZ)
    kernel = coulomb_kernel()
    ac = NX * NZ
    tx = np.zeros((128, MODES), np.float32)
    tx[:NX, :ac] = np.repeat(cx, NZ, axis=1)
    tz = np.zeros((128, MODES), np.float32)
    tz[:NZ, :ac] = np.tile(cz, (1, NX))
    ty = np.zeros((128, 128), np.float32)
    tk = np.zeros((128, MODES), np.float32)
    k_high, k_low = two_parts(kernel.transpose(1, 0, 2).reshape(NY, ac))
    for at, part in ((0, k_high), (32, k_high), (64, k_low)):
        ty[:NY, at : at + NY] = cy
        tk[at : at + NY, :ac] = part
    phi = np.einsum("ax,cz->acxz", cx, cz).reshape(ac, NX, NZ)
    right = np.zeros((MODES, 2, 256), np.float32)
    for h in range(2):
        right[:ac, h, :240] = phi[:, 10 * h : 10 * h + 10].reshape(ac, 240)
    r_high, r_low = two_parts(right.reshape(MODES, 512))
    bf = lambda a: jnp.asarray(a, BF16)
    three = np.concatenate([tx, tz, tk], axis=1)
    return bf(three), bf(ty), bf(np.concatenate([r_high, r_low], axis=1)), jnp.asarray(ty[:32], F32)


def permutations():
    true = np.arange(NORB).reshape(2, 8, 8, 2)
    order_a = true.transpose(0, 2, 1, 3).reshape(-1)
    order_b = true.transpose(1, 3, 0, 2).reshape(-1)
    eye = np.eye(NORB, dtype=np.float32)
    return jnp.asarray(np.concatenate([eye[:, order_a], eye[:, order_b]], axis=1), BF16)


def split2(a):
    high = a.astype(BF16)
    return high, (a - high.astype(F32)).astype(BF16)


def dot(a, b, dims=(1, 0)):
    return lax.dot_general(
        a, b, (((dims[0],), (dims[1],)), ((), ())), preferred_element_type=F32
    )


def me():
    return tuple(lax.axis_index(a) for a in AXES)


def of_plane(pid, z):
    return ((pid // 8) % 2, z, (pid // 2) % 4, pid % 2, pid // 16)


def copy(src, dst, send_sem, recv_sem, device):
    return pltpu.make_async_remote_copy(
        src_ref=src, dst_ref=dst, send_sem=send_sem, recv_sem=recv_sem,
        device_id=device, device_id_type=MESH,
    )


def rows(start, size):
    return pl.ds(pl.multiple_of(start, size), size)


def each(count, body):
    lax.fori_loop(0, count, lambda i, carry: (body(i), carry)[1], 0)


def swap(n, i, body):
    each(n - 1, lambda d: body((i + d + 1) % n))


Z_ORDER = (4, 3, 5, 2, 6, 1, 7)
CHIP_ORDER = (
    (2, 2), (2, 1), (2, 3), (1, 2), (3, 2), (1, 1), (1, 3), (3, 1), (3, 3),
    (2, 0), (0, 2), (1, 0), (3, 0), (0, 1), (0, 3),
)
HALF_ORDER = tuple((a, b, k) for a, b in ((1, 2), (1, 1), (1, 3), (0, 2), (1, 0), (0, 1), (0, 3)) for k in range(2)) + ((0, 0, 1),)


def greet(barrier, n, i, device):
    swap(n, i, lambda t: pl.semaphore_signal(barrier, inc=1, device_id=device(t), device_id_type=MESH))
    return n - 1


def shifted(a, factor, shift):
    return lax.shift_right_logical(a * factor, shift)


def main_kernel(
    st_any, raw_any, oc_any, perm_any, t_any, ty_any, right_any, cy_any, results,
    st, raw, oc, s1, by_y, s2, cells, turned_cells, perm, t3, ty, right, cy, in_s,
    o1, o2, r1, r2, green, left, y_rows, v_f, v_b, gp, gc, gh, rg, rv, s8, rz,
    gram, vall, tt, dd, rp,
    za_s, za_r, pa_s, pa_r, cg_s, cg_r, cf_s, cf_r, zg_s, zg_r,
    gc_s, gc_r, ga_s, ga_r, va_s, va_r, gz_s, gz_r, gg_s, gg_r, gf_s, gf_r,
    vg_s, vg_r, d_s, d_r,
):
    xl, z, y, c, h = me()
    p = xl * 8 + y * 2 + c
    q = h * 8 + xl * 4 + y
    z_dev = lambda t: (xl, t, y, c, h)
    half_dev = lambda t: of_plane(h * 16 + t, z)
    chip_dev = lambda t: ((t // 4) % 2, z, t % 4, c, t // 8)
    core_dev = (xl, z, y, 1 - c, h)

    def z_line(body):
        for d in Z_ORDER:
            body((z + d) % 8)

    def chips(body):
        for dx, dy in CHIP_ORDER:
            body((q // 4 + dx) % 4 * 4 + (y + dy) % 4)

    def half(body):
        for dx, dy, dc in HALF_ORDER:
            body((xl + dx) % 2 * 8 + (y + dy) % 4 * 2 + (c + dc) % 2)

    barrier = pltpu.get_barrier_semaphore()
    greeted = greet(barrier, 8, z, z_dev) + greet(barrier, 16, p, half_dev)
    greeted += greet(barrier, 16, q, chip_dev)
    pl.semaphore_signal(barrier, inc=1, device_id=core_dev, device_id_type=MESH)

    held = (
        (raw_any, raw), (oc_any, oc), (st_any, st), (t_any, t3), (ty_any, ty), (cy_any, cy),
        (right_any, right), (perm_any, perm),
    )
    held = [pltpu.make_async_copy(a, b, in_s.at[k]) for k, (a, b) in enumerate(held)]
    for one in held:
        one.start()
    perm_a, perm_b = perm.at[:, :NORB], perm.at[:, NORB:]
    tx, tz, tk = (t3.at[:, k * MODES : (k + 1) * MODES] for k in range(3))
    rh, rl = right.at[:, :512], right.at[:, 512:]
    for one in held[:3]:
        one.wait()
    cells[...] = jnp.zeros_like(cells)
    for k in range(45):
        pair = raw[:, k * 128 : (k + 1) * 128].astype(F32)
        for o in range(2):
            cells[64 * o + k : 64 * o + k + 1, :] = pair[o : o + 1]
    for o in range(2):
        cells[64 * o + 45 : 64 * o + 46, :] = jnp.broadcast_to(oc[...].astype(F32)[None, o : o + 1], (1, 128))
    turned_cells[...] = cells[...].T
    for k in range(16):
        s2[k] = turned_cells[pl.ds(k, 8, stride=16), :]
    s1[...] = jnp.zeros_like(s1)
    for o in range(2):
        wide_rows = jnp.concatenate(
            [st[o, k].astype(F32) for k in range(10)] + [jnp.zeros((NY, 16), F32)], axis=1
        )
        for part in range(2):
            by_y[o, part] = wide_rows[:, 128 * part : 128 * part + 128]
            for t in range(3):
                s1[pl.ds(8 * o + 2 * t + part, 8, stride=16), :] = by_y[o, part, pl.ds(t, 8, stride=3), :]
    for one in held[3:6]:
        one.wait()

    row = lax.broadcasted_iota(jnp.int32, (ROWS, 128), 0)
    lane = lax.broadcasted_iota(jnp.int32, (ROWS, 128), 1)
    zz = shifted(row, 1366, 16)
    s = row - zz * 48
    cell = h * HALF + s * 128 + zz * 16 + p
    x = shifted(cell, 7282, 22)
    yz = cell - x * (NY * NZ)
    y_cell = shifted(yz, 2731, 16)
    z_cell = yz - y_cell * NZ
    hot = lambda a: jnp.where(a == lane, 1.0, 0.0).astype(BF16)
    left[...] = dot(hot(jnp.where(s < 45, x, 127)), tx[...]) * dot(hot(z_cell), tz[...])
    y_rows[...] = dot(hot(y_cell), ty[...])
    middle = (lane >= 32) & (lane < 64)

    def green_part(t):
        k_high, k_low = split2(y_rows[...] * cy[pl.ds(z * 3 + t, 1), :])
        mix = jnp.where(middle, k_low.astype(F32), k_high.astype(F32)).astype(BF16)
        l_high, l_low = split2(left[...] * dot(mix, tk[...]))
        g = dot(l_high, rh[...]) + dot(l_low, rh[...]) + dot(l_high, rl[...])
        for hh in range(2):
            green[hh, :, t * 256 : (t + 1) * 256] = g[:, hh * 256 : (hh + 1) * 256]

    pl.semaphore_wait(barrier, greeted + 1)

    def z_send(t):
        return copy(s1.at[rows(t * 16, 16)], r1.at[rows(z * 16, 16)], za_s.at[t], za_r.at[z], z_dev(t))

    def z_recv(t):
        return copy(s1.at[rows(t * 16, 16)], r1.at[rows(t * 16, 16)], za_s.at[t], za_r.at[t], z_dev(t))

    def p_send(t):
        return copy(s2.at[t], r2.at[rows(p * 8, 8)], pa_s.at[t], pa_r.at[p], half_dev(t))

    def p_recv(t):
        return copy(s2.at[t], r2.at[rows(t * 8, 8)], pa_s.at[t], pa_r.at[t], half_dev(t))

    half(lambda t: p_send(t).start())
    z_line(lambda t: z_send(t).start())
    r1[rows(z * 16, 16)] = s1[rows(z * 16, 16)]
    r2[rows(p * 8, 8)] = s2[p]
    for one in held[6:]:
        one.wait()
    green_part(0)
    swap(16, p, lambda t: p_recv(t).wait_recv())
    by_row = [r2[pl.ds(k, 16, stride=8), :] for k in range(8)]
    o2[rows(z * 32, 32), :] = jnp.concatenate(
        [jnp.concatenate([b[:, 64 * o : 64 * o + 48] for b in by_row], axis=1) for o in range(2)], axis=0
    ).astype(BF16)

    def zg_send(t):
        mine = o2.at[rows(z * 32, 32)]
        return copy(mine, mine, zg_s.at[t], zg_r.at[z], z_dev(t))

    def zg_recv(t):
        theirs = o2.at[rows(t * 32, 32)]
        return copy(theirs, theirs, zg_s.at[t], zg_r.at[t], z_dev(t))

    z_line(lambda t: zg_send(t).start())
    swap(8, z, lambda t: z_recv(t).wait_recv())
    for t in range(3):
        o1[h, rows(p * 16, 16), t * 256 : (t + 1) * 256] = jnp.concatenate(
            [r1[pl.ds(2 * t + k, 16, stride=8), :] for k in range(2)], axis=1
        ).astype(BF16)

    def block(t, core):
        return o1.at[t // 8, rows(((t // 4) % 2 * 8 + t % 4 * 2 + core) * 16, 16)]

    def c_send(t):
        return copy(block(q, c), block(q, c), cg_s.at[t], cg_r.at[q], chip_dev(t))

    def c_recv(t):
        return copy(block(t, c), block(t, c), cg_s.at[t], cg_r.at[t], chip_dev(t))

    def f_send(t):
        return copy(block(t, c), block(t, c), cf_s.at[t], cf_r.at[t], core_dev)

    def f_recv(t):
        return copy(block(t, 1 - c), block(t, 1 - c), cf_s.at[t], cf_r.at[t], core_dev)

    chips(lambda t: c_send(t).start())
    f_send(q).start()
    green_part(1)
    green_part(2)

    def pass_on(t):
        c_recv(t).wait_recv()
        f_send(t).start()

    chips(pass_on)
    swap(8, z, lambda t: zg_recv(t).wait_recv())
    o_rows = dot(perm_b[...], o2[...])
    o_b = o_rows.astype(BF16)
    w = (o_rows * o_rows[:, 45:46]).astype(BF16).T
    each(16, lambda t: f_recv(t).wait_recv())

    v = jnp.zeros((NORB, ROWS), F32)
    for hh in range(2):
        orb = dot(perm_a[...], o1[hh]).astype(BF16)
        m_high, m_low = split2(green[hh] * dot(w, orb))
        v = v + dot(orb, m_high, (1, 1)) + dot(orb, m_low, (1, 1))
    v_high, v_low = split2(v)
    gp[...] = (dot(o_b, v_high, (1, 1)) + dot(o_b, v_low, (1, 1))) * (1.0 / NPTS)

    def half_send():
        other = gp.at[rows((1 - c) * 128, 128)]
        return copy(other, gc, gc_s, gc_r, core_dev)

    def v_send(part, t):
        if part == 0:
            src, dst = v_b.at[0, :, rows(t * 16, 16), :], rv.at[0, z]
        else:
            src, dst = v_b.at[1, part - 1, rows(t * 16, 16), :], rv.at[1, z, part - 1]
        return copy(src, dst, va_s.at[part, t], va_r.at[part, z], z_dev(t))

    def v_recv(part, t):
        if part == 0:
            src, dst = v_b.at[0, :, rows(t * 16, 16), :], rv.at[0, t]
        else:
            src, dst = v_b.at[1, part - 1, rows(t * 16, 16), :], rv.at[1, t, part - 1]
        return copy(src, dst, va_s.at[part, t], va_r.at[part, t], z_dev(t))

    half_send().start()
    for part, value in ((0, v_high), (1, v_low)):
        v_b[part] = value.reshape(2, 128, ROWS)
    v_f[...] = v.reshape(2, 128, ROWS)
    z_line(lambda t: v_send(0, t).start())
    z_line(lambda t: v_send(1, t).start())
    half_send().wait_recv()
    gh[...] = gp[rows(c * 128, 128)] + gc[...]

    def a_send(t):
        return copy(gh.at[rows(t * 8, 8)], rg.at[q], ga_s.at[t], ga_r.at[q], chip_dev(t))

    def a_recv(t):
        return copy(gh.at[rows(t * 8, 8)], rg.at[t], ga_s.at[t], ga_r.at[t], chip_dev(t))

    chips(lambda t: a_send(t).start())
    rg[q] = gh[rows(q * 8, 8)]
    for part in range(2):
        rv[part, z] = jnp.zeros((2, 16, ROWS), BF16)
    swap(16, q, lambda t: a_recv(t).wait_recv())
    s8[...] = jnp.sum(rg[...], axis=0)

    def gz_send(t):
        return copy(s8, rz.at[z], gz_s.at[t], gz_r.at[z], z_dev(t))

    def gz_recv(t):
        return copy(s8, rz.at[t], gz_s.at[t], gz_r.at[t], z_dev(t))

    z_line(lambda t: gz_send(t).start())
    z_line(lambda t: v_send(2, t).start())
    rz[z] = s8[...]
    swap(8, z, lambda t: gz_recv(t).wait_recv())

    def line(t, core):
        return gram.at[rows(core * 128 + t * 8, 8)]

    gram[rows(c * 128 + q * 8, 8)] = jnp.sum(rz[...], axis=0)

    def g_send(t):
        return copy(line(q, c), line(q, c), gg_s.at[t], gg_r.at[q], chip_dev(t))

    def g_recv(t):
        return copy(line(t, c), line(t, c), gg_s.at[t], gg_r.at[t], chip_dev(t))

    def gf_send(t):
        return copy(line(t, c), line(t, c), gf_s.at[t], gf_r.at[t], core_dev)

    def gf_recv(t):
        return copy(line(t, 1 - c), line(t, 1 - c), gf_s.at[t], gf_r.at[t], core_dev)

    chips(lambda t: g_send(t).start())
    gf_send(q).start()

    for part in range(3):
        swap(8, z, lambda t, part=part: v_recv(part, t).wait_recv())
    others = jnp.sum(rv[0].astype(F32) + rv[1].astype(F32), axis=0)
    mine = v_f[:, rows(z * 16, 16), :] + others
    m_high, m_low = split2(mine)
    own = vall.at[:, rows(z * 16, 16), :]
    own[:, :, :ROWS] = m_high
    own[:, :, ROWS:] = m_low

    def vg_send(t):
        return copy(own, own, vg_s.at[t], vg_r.at[z], z_dev(t))

    def vg_recv(t):
        theirs = vall.at[:, rows(t * 16, 16), :]
        return copy(theirs, theirs, vg_s.at[t], vg_r.at[t], z_dev(t))

    z_line(lambda t: vg_send(t).start())

    def g_pass_on(t):
        g_recv(t).wait_recv()
        gf_send(t).start()

    chips(g_pass_on)

    def d_send(n, t):
        return copy(dd.at[n, rows(t * 8, 8)], rp.at[n, rows(p * 8, 8)], d_s.at[n, t], d_r.at[n, p], half_dev(t))

    def d_recv(n, t):
        return copy(dd.at[n, rows(t * 8, 8)], rp.at[n, rows(t * 8, 8)], d_s.at[n, t], d_r.at[n, t], half_dev(t))

    def deal(n, value):
        for k in range(3):
            tt[n, k] = value[:, k * 128 : (k + 1) * 128]
        even, odd = (
            jnp.concatenate([tt[n, k, pl.ds(o, 16, stride=2), :] for k in range(3)], axis=1)
            for o in range(2)
        )
        gap = jnp.zeros((16, 16), F32)
        for k in range(8):
            cells = slice(48 * k, 48 * k + 48)
            dd[n, pl.ds(k, 16, stride=8), :] = jnp.concatenate(
                [even[:, cells], gap, odd[:, cells], gap], axis=1
            )
        half(lambda t: d_send(n, t).start())
        rp[n, rows(p * 8, 8)] = dd[n, rows(p * 8, 8)]

    def land(n):
        swap(16, p, lambda t: d_recv(n, t).wait_recv())
        table = jnp.concatenate([rp[n, pl.ds(k, 16, stride=8), :] for k in range(8)], axis=0)
        turned = table.T
        for k in range(45):
            results[n, :, k * 128 : (k + 1) * 128] = jnp.concatenate(
                [turned[k : k + 1], turned[64 + k : 65 + k]], axis=0
            )

    deal(0, mine.reshape(32, ROWS))
    each(16, lambda t: gf_recv(t).wait_recv())
    half_send().wait_send()
    swap(16, q, lambda t: g_send(t).wait_send())
    each(16, lambda t: gf_send(t).wait_send())
    a = gram[...]
    gram[...] = (a + a.T) * 0.5
    eliminate(gram)
    l_rows = jnp.concatenate([gram[rows(k * 128 + z * 16, 16), :] for k in range(2)], axis=0)
    l_both = jnp.concatenate(split2(l_rows), axis=0)
    swap(8, z, lambda t: vg_recv(t).wait_recv())
    out = dot(l_both, vall[...].reshape(NORB, 2 * ROWS))
    deal(1, out[:32, :ROWS] + out[32:, :ROWS] + out[:32, ROWS:])
    land(0)
    for group, i, sends in (
        (8, z, (z_send, zg_send, *(functools.partial(v_send, k) for k in range(3)), gz_send, vg_send)),
        (16, p, (p_send, functools.partial(d_send, 0))),
        (16, q, (c_send, a_send)),
    ):
        for send in sends:
            swap(group, i, lambda t, send=send: send(t).wait_send())
    each(16, lambda t: f_send(t).wait_send())
    land(1)
    swap(16, p, lambda t: d_send(1, t).wait_send())


def eliminate(work):
    sub = lax.broadcasted_iota(jnp.int32, (8, 128), 0)
    lane = lax.broadcasted_iota(jnp.int32, (8, 128), 1)
    wide = lambda col: jnp.broadcast_to(col, (8, 128))
    for k in range(8):
        base = 32 * k
        tile, off = base // 128, base % 128
        wk = [
            [work[base + 8 * g : base + 8 * g + 8, 128 * t : 128 * t + 128] for t in range(2)]
            for g in range(4)
        ]
        col = [
            [wide(wk[g][tile][:, off + j : off + j + 1]) if g >= j // 8 else None for g in range(4)]
            for j in range(32)
        ]
        inside = (lane >= off) & (lane < off + 32)
        for g in range(4):
            unit = jnp.where(lane - off == sub + 8 * g, 1.0, 0.0)
            wk[g][tile] = jnp.where(inside, unit, wk[g][tile])
        pivots = [jnp.ones((8, 128), F32) for _ in range(4)]
        for j in range(0, 32, 2):
            gj, sj = j // 8, j % 8
            u, v = col[j], col[j + 1]
            p11 = wide(u[gj][sj : sj + 1, :])
            p21 = wide(u[gj][sj + 1 : sj + 2, :])
            p22 = wide(v[gj][sj + 1 : sj + 2, :])
            det = p11 * p22 - p21 * p21
            r = 1.0 / det
            r11 = 1.0 / p11
            pivots[gj] = jnp.where(sub == sj, p11, jnp.where(sub == sj + 1, det * r11, pivots[gj]))
            q11, q21, q22 = p22 * r, p21 * r, p11 * r
            al, be = [None] * 4, [None] * 4
            for g in range(gj, 4):
                al[g] = u[g] * q11 - v[g] * q21
                be[g] = v[g] * q22 - u[g] * q21
            below = sub > sj + 1
            be[gj] = jnp.where(below, be[gj], 0.0)
            al[gj] = jnp.where(below, al[gj], jnp.where(sub == sj + 1, p21 * r11, 0.0))
            for i in range(j + 2, 32):
                fu = wide(u[i // 8][i % 8 : i % 8 + 1, :])
                fv = wide(v[i // 8][i % 8 : i % 8 + 1, :])
                for g in range(i // 8, 4):
                    col[i][g] = col[i][g] - (al[g] * fu + be[g] * fv)
            for t in range(2):
                one = wide(wk[gj][t][sj : sj + 1, :])
                two = wide(wk[gj][t][sj + 1 : sj + 2, :])
                for g in range(gj, 4):
                    wk[g][t] = wk[g][t] - (al[g] * one + be[g] * two)
        for g in range(4):
            scale = lax.rsqrt(pivots[g])
            for t in range(2):
                wk[g][t] = wk[g][t] * scale
        u = jnp.concatenate([jnp.concatenate(wk[g], axis=1) for g in range(4)], axis=0)
        lanes = lax.broadcasted_iota(jnp.int32, (32, 256), 1)
        work[base : base + 32, :] = jnp.where(lanes < base + 32, u, 0.0)
        if k < 7:
            u_high, u_low = split2(u)
            one = jnp.concatenate([u_high, u_low, u_high], axis=0)
            two = jnp.concatenate([u_high, u_high, u_low], axis=0)
            edge = base + 32
            start = edge // 128 * 128
            change = dot(one[:, start:].T, two)[edge - start :]
            rest = work[edge:, :]
            lanes = lax.broadcasted_iota(jnp.int32, rest.shape, 1)
            rest = jnp.where((lanes >= base) & (lanes < edge), 0.0, rest)
            work[edge:, :] = rest - change


VM = pl.BlockSpec(memory_space=pltpu.VMEM)
ANY = pl.BlockSpec(memory_space=pl.ANY)
DMA = pltpu.SemaphoreType.DMA


def call(kernel, args, outs, scratch, number, name):
    return pl.pallas_call(
        kernel,
        out_shape=[jax.ShapeDtypeStruct(s, d) for s, d in outs],
        in_specs=[ANY] * len(args),
        out_specs=[VM] * len(outs),
        scratch_shapes=scratch,
        compiler_params=pltpu.CompilerParams(
            vmem_limit_bytes=60 * 1024 * 1024, collective_id=number, has_side_effects=True
        ),
        name=name,
    )(*args)


def on_device(orbitals, occupation):
    planes = orbitals.reshape(2, 10, NY, NZ)
    vm = pltpu.VMEM
    both = call(
        main_kernel, (planes, orbitals, occupation, permutations(), *tables()),
        (((2, 2, HALF), F32),),
        [vm((2, 10, NY, NZ), BF16), vm((2, HALF), BF16), vm((2,), BF16),
         vm((128, 128), F32), vm((2, 2, NY, 128), F32), vm((16, 8, 128), F32), vm((128, 128), F32), vm((128, 128), F32), vm((NORB, 512), BF16), vm((128, 3 * MODES), BF16),
         vm((128, 128), BF16), vm((MODES, 1024), BF16), vm((32, 128), F32), DMA((8,)),
         vm((2, NORB, 768), BF16), vm((NORB, ROWS), BF16), vm((128, 128), F32), vm((128, 128), F32),
         vm((2, ROWS, 768), F32), vm((ROWS, MODES), F32), vm((ROWS, 128), F32),
         vm((2, 128, ROWS), F32), vm((2, 2, 128, ROWS), BF16), vm((NORB, NORB), F32),
         vm((128, NORB), F32), vm((128, NORB), F32), vm((16, 8, NORB), F32),
         vm((2, 8, 2, 16, ROWS), BF16), vm((8, NORB), F32), vm((8, 8, NORB), F32),
         vm((NORB, NORB), F32), vm((2, 128, 2 * ROWS), BF16), vm((2, 3, 32, 128), F32),
         vm((2, 128, 128), F32), vm((2, 128, 128), F32),
         DMA((8,)), DMA((8,)), DMA((16,)), DMA((16,)), DMA((16,)), DMA((16,)), DMA((16,)), DMA((16,)),
         DMA((8,)), DMA((8,)), DMA, DMA, DMA((16,)), DMA((16,)), DMA((3, 8)), DMA((3, 8)),
         DMA((8,)), DMA((8,)), DMA((16,)), DMA((16,)), DMA((16,)), DMA((16,)),
         DMA((8,)), DMA((8,)), DMA((2, 16)), DMA((2, 16))],
        0, "exchange",
    )[0]
    return -both[0], -both[1]


def solution(mesh):
    torus = Mesh(mesh.devices.reshape(2, 8, 4, 2, mesh.shape["grid"]), AXES)
    return jax.shard_map(
        on_device,
        mesh=torus,
        in_specs=(P(ORB, "h"), P(ORB)),
        out_specs=(P(ORB, "h"), P(ORB, "h")),
        check_vma=False,
    )
```

```python
import functools
import math

import jax
import jax.numpy as jnp
import numpy as np
from jax import lax
from jax.experimental import pallas as pl
from jax.experimental.pallas import tpu as pltpu
from jax.sharding import Mesh
from jax.sharding import PartitionSpec as P

NX = 20
NY = 24
NZ = 24
NORB = 256
NPTS = 11520
HALF = NPTS // 2
MODES = 512
ROWS = 384
AXES = ("xl", "z", "y", "c", "h")
ORB = ("xl", "z", "y", "c")
MESH = pl.DeviceIdType.MESH
F32 = jnp.float32
BF16 = jnp.bfloat16


def rounded(a):
    return np.asarray(a, np.float32).astype(jnp.bfloat16).astype(np.float32)


def hartley_table(length):
    index = np.arange(length)
    angle = 2.0 * math.pi / length * (index[:, None] * index[None, :] % length)
    return rounded(np.cos(angle) + np.sin(angle))


def signed_square(length):
    index = np.arange(length)
    signed = np.where(index <= length // 2, index, index - length)
    return (2.0 * math.pi * signed / length) ** 2


def coulomb_kernel():
    total = (
        signed_square(NX)[:, None, None]
        + signed_square(NY)[None, :, None]
        + signed_square(NZ)[None, None, :]
    )
    return np.where(total > 0, 1.0 / np.where(total > 0, total, 1.0), 0.0) / NPTS


def two_parts(a):
    high = rounded(a)
    return high, rounded(a - high)


def tables():
    cx, cy, cz = hartley_table(NX), hartley_table(NY), hartley_table(NZ)
    kernel = coulomb_kernel()
    ac = NX * NZ
    tx = np.zeros((128, MODES), np.float32)
    tx[:NX, :ac] = np.repeat(cx, NZ, axis=1)
    tz = np.zeros((128, MODES), np.float32)
    tz[:NZ, :ac] = np.tile(cz, (1, NX))
    ty = np.zeros((128, 128), np.float32)
    tk = np.zeros((128, MODES), np.float32)
    k_high, k_low = two_parts(kernel.transpose(1, 0, 2).reshape(NY, ac))
    for at, part in ((0, k_high), (32, k_high), (64, k_low)):
        ty[:NY, at : at + NY] = cy
        tk[at : at + NY, :ac] = part
    phi = np.einsum("ax,cz->acxz", cx, cz).reshape(ac, NX, NZ)
    right = np.zeros((MODES, 2, 256), np.float32)
    for h in range(2):
        right[:ac, h, :240] = phi[:, 10 * h : 10 * h + 10].reshape(ac, 240)
    r_high, r_low = two_parts(right.reshape(MODES, 512))
    bf = lambda a: jnp.asarray(a, BF16)
    three = np.concatenate([tx, tz, tk], axis=1)
    return bf(three), bf(ty), bf(np.concatenate([r_high, r_low], axis=1)), jnp.asarray(ty[:32], F32)


def permutations():
    true = np.arange(NORB).reshape(2, 8, 8, 2)
    order_a = true.transpose(0, 2, 1, 3).reshape(-1)
    order_b = true.transpose(1, 3, 0, 2).reshape(-1)
    eye = np.eye(NORB, dtype=np.float32)
    return jnp.asarray(np.concatenate([eye[:, order_a], eye[:, order_b]], axis=1), BF16)


def split2(a):
    high = a.astype(BF16)
    return high, (a - high.astype(F32)).astype(BF16)


def dot(a, b, dims=(1, 0)):
    return lax.dot_general(
        a, b, (((dims[0],), (dims[1],)), ((), ())), preferred_element_type=F32
    )


def me():
    return tuple(lax.axis_index(a) for a in AXES)


def of_plane(pid, z):
    return ((pid // 8) % 2, z, (pid // 2) % 4, pid % 2, pid // 16)


def copy(src, dst, send_sem, recv_sem, device):
    return pltpu.make_async_remote_copy(
        src_ref=src, dst_ref=dst, send_sem=send_sem, recv_sem=recv_sem,
        device_id=device, device_id_type=MESH,
    )


def rows(start, size):
    return pl.ds(pl.multiple_of(start, size), size)


def each(count, body):
    lax.fori_loop(0, count, lambda i, carry: (body(i), carry)[1], 0)


def swap(n, i, body):
    each(n - 1, lambda d: body((i + d + 1) % n))


Z_ORDER = (4, 3, 5, 2, 6, 1, 7)
CHIP_ORDER = (
    (2, 2), (2, 1), (2, 3), (1, 2), (3, 2), (1, 1), (1, 3), (3, 1), (3, 3),
    (2, 0), (0, 2), (1, 0), (3, 0), (0, 1), (0, 3),
)
HALF_ORDER = tuple((a, b, k) for a, b in ((1, 2), (1, 1), (1, 3), (0, 2), (1, 0), (0, 1), (0, 3)) for k in range(2)) + ((0, 0, 1),)


def greet(barrier, n, i, device):
    swap(n, i, lambda t: pl.semaphore_signal(barrier, inc=1, device_id=device(t), device_id_type=MESH))
    return n - 1


def shifted(a, factor, shift):
    return lax.shift_right_logical(a * factor, shift)


def main_kernel(
    st_any, raw_any, oc_any, perm_any, t_any, ty_any, right_any, cy_any, results,
    st, raw, oc, s1, by_y, s2, cells, turned_cells, perm, t3, ty, right, cy, in_s,
    o1, o2, r1, r2, green, left, y_rows, v_f, v_b, gp, gc, gh, rg, rv, s8, rz,
    gram, vall, tt, dd, rp,
    za_s, za_r, pa_s, pa_r, cg_s, cg_r, cf_s, cf_r, zg_s, zg_r,
    gc_s, gc_r, ga_s, ga_r, va_s, va_r, gz_s, gz_r, gg_s, gg_r, gf_s, gf_r,
    vg_s, vg_r, d_s, d_r,
):
    xl, z, y, c, h = me()
    p = xl * 8 + y * 2 + c
    q = h * 8 + xl * 4 + y
    z_dev = lambda t: (xl, t, y, c, h)
    half_dev = lambda t: of_plane(h * 16 + t, z)
    chip_dev = lambda t: ((t // 4) % 2, z, t % 4, c, t // 8)
    core_dev = (xl, z, y, 1 - c, h)

    def z_line(body):
        for d in Z_ORDER:
            body((z + d) % 8)

    def chips(body):
        for dx, dy in CHIP_ORDER:
            body((q // 4 + dx) % 4 * 4 + (y + dy) % 4)

    def half(body):
        for dx, dy, dc in HALF_ORDER:
            body((xl + dx) % 2 * 8 + (y + dy) % 4 * 2 + (c + dc) % 2)

    barrier = pltpu.get_barrier_semaphore()
    greeted = greet(barrier, 8, z, z_dev) + greet(barrier, 16, p, half_dev)
    greeted += greet(barrier, 16, q, chip_dev)
    pl.semaphore_signal(barrier, inc=1, device_id=core_dev, device_id_type=MESH)

    held = (
        (raw_any, raw), (oc_any, oc), (st_any, st), (t_any, t3), (ty_any, ty), (cy_any, cy),
        (right_any, right), (perm_any, perm),
    )
    held = [pltpu.make_async_copy(a, b, in_s.at[k]) for k, (a, b) in enumerate(held)]
    for one in held:
        one.start()
    perm_a, perm_b = perm.at[:, :NORB], perm.at[:, NORB:]
    tx, tz, tk = (t3.at[:, k * MODES : (k + 1) * MODES] for k in range(3))
    rh, rl = right.at[:, :512], right.at[:, 512:]
    for one in held[:3]:
        one.wait()
    cells[...] = jnp.zeros_like(cells)
    for k in range(45):
        pair = raw[:, k * 128 : (k + 1) * 128].astype(F32)
        for o in range(2):
            cells[64 * o + k : 64 * o + k + 1, :] = pair[o : o + 1]
    for o in range(2):
        cells[64 * o + 45 : 64 * o + 46, :] = jnp.broadcast_to(oc[...].astype(F32)[None, o : o + 1], (1, 128))
    turned_cells[...] = cells[...].T
    for k in range(16):
        s2[k] = turned_cells[pl.ds(k, 8, stride=16), :]
    s1[...] = jnp.zeros_like(s1)
    for o in range(2):
        wide_rows = jnp.concatenate(
            [st[o, k].astype(F32) for k in range(10)] + [jnp.zeros((NY, 16), F32)], axis=1
        )
        for part in range(2):
            by_y[o, part] = wide_rows[:, 128 * part : 128 * part + 128]
            for t in range(3):
                s1[pl.ds(8 * o + 2 * t + part, 8, stride=16), :] = by_y[o, part, pl.ds(t, 8, stride=3), :]

    row = lax.broadcasted_iota(jnp.int32, (ROWS, 128), 0)
    lane = lax.broadcasted_iota(jnp.int32, (ROWS, 128), 1)
    zz = shifted(row, 1366, 16)
    s = row - zz * 48
    cell = h * HALF + s * 128 + zz * 16 + p
    x = shifted(cell, 7282, 22)
    yz = cell - x * (NY * NZ)
    y_cell = shifted(yz, 2731, 16)
    z_cell = yz - y_cell * NZ
    hot = lambda a: jnp.where(a == lane, 1.0, 0.0).astype(BF16)
    middle = (lane >= 32) & (lane < 64)

    def green_part(t):
        k_high, k_low = split2(y_rows[...] * cy[pl.ds(z * 3 + t, 1), :])
        mix = jnp.where(middle, k_low.astype(F32), k_high.astype(F32)).astype(BF16)
        l_high, l_low = split2(left[...] * dot(mix, tk[...]))
        g = dot(l_high, rh[...]) + dot(l_low, rh[...]) + dot(l_high, rl[...])
        for hh in range(2):
            green[hh, :, t * 256 : (t + 1) * 256] = g[:, hh * 256 : (hh + 1) * 256]

    pl.semaphore_wait(barrier, greeted + 1)

    def z_send(t):
        return copy(s1.at[rows(t * 16, 16)], r1.at[rows(z * 16, 16)], za_s.at[t], za_r.at[z], z_dev(t))

    def z_recv(t):
        return copy(s1.at[rows(t * 16, 16)], r1.at[rows(t * 16, 16)], za_s.at[t], za_r.at[t], z_dev(t))

    def p_send(t):
        return copy(s2.at[t], r2.at[rows(p * 8, 8)], pa_s.at[t], pa_r.at[p], half_dev(t))

    def p_recv(t):
        return copy(s2.at[t], r2.at[rows(t * 8, 8)], pa_s.at[t], pa_r.at[t], half_dev(t))

    half(lambda t: p_send(t).start())
    z_line(lambda t: z_send(t).start())
    r1[rows(z * 16, 16)] = s1[rows(z * 16, 16)]
    r2[rows(p * 8, 8)] = s2[p]
    for one in held[3:]:
        one.wait()
    left[...] = dot(hot(jnp.where(s < 45, x, 127)), tx[...]) * dot(hot(z_cell), tz[...])
    y_rows[...] = dot(hot(y_cell), ty[...])
    green_part(0)
    swap(16, p, lambda t: p_recv(t).wait_recv())
    by_row = [r2[pl.ds(k, 16, stride=8), :] for k in range(8)]
    o2[rows(z * 32, 32), :] = jnp.concatenate(
        [jnp.concatenate([b[:, 64 * o : 64 * o + 48] for b in by_row], axis=1) for o in range(2)], axis=0
    ).astype(BF16)

    def zg_send(t):
        mine = o2.at[rows(z * 32, 32)]
        return copy(mine, mine, zg_s.at[t], zg_r.at[z], z_dev(t))

    def zg_recv(t):
        theirs = o2.at[rows(t * 32, 32)]
        return copy(theirs, theirs, zg_s.at[t], zg_r.at[t], z_dev(t))

    z_line(lambda t: zg_send(t).start())
    swap(8, z, lambda t: z_recv(t).wait_recv())
    for t in range(3):
        o1[h, rows(p * 16, 16), t * 256 : (t + 1) * 256] = jnp.concatenate(
            [r1[pl.ds(2 * t + k, 16, stride=8), :] for k in range(2)], axis=1
        ).astype(BF16)

    def block(t, core):
        return o1.at[t // 8, rows(((t // 4) % 2 * 8 + t % 4 * 2 + core) * 16, 16)]

    def c_send(t):
        return copy(block(q, c), block(q, c), cg_s.at[t], cg_r.at[q], chip_dev(t))

    def c_recv(t):
        return copy(block(t, c), block(t, c), cg_s.at[t], cg_r.at[t], chip_dev(t))

    def f_send(t):
        return copy(block(t, c), block(t, c), cf_s.at[t], cf_r.at[t], core_dev)

    def f_recv(t):
        return copy(block(t, 1 - c), block(t, 1 - c), cf_s.at[t], cf_r.at[t], core_dev)

    chips(lambda t: c_send(t).start())
    f_send(q).start()
    green_part(1)
    green_part(2)

    def pass_on(t):
        c_recv(t).wait_recv()
        f_send(t).start()

    chips(pass_on)
    swap(8, z, lambda t: zg_recv(t).wait_recv())
    o_rows = dot(perm_b[...], o2[...])
    o_b = o_rows.astype(BF16)
    w = (o_rows * o_rows[:, 45:46]).astype(BF16).T
    each(16, lambda t: f_recv(t).wait_recv())

    v = jnp.zeros((NORB, ROWS), F32)
    for hh in range(2):
        orb = dot(perm_a[...], o1[hh]).astype(BF16)
        m_high, m_low = split2(green[hh] * dot(w, orb))
        v = v + dot(orb, m_high, (1, 1)) + dot(orb, m_low, (1, 1))
    v_high, v_low = split2(v)
    gp[...] = (dot(o_b, v_high, (1, 1)) + dot(o_b, v_low, (1, 1))) * (1.0 / NPTS)

    def half_send():
        other = gp.at[rows((1 - c) * 128, 128)]
        return copy(other, gc, gc_s, gc_r, core_dev)

    def v_send(part, t):
        if part == 0:
            src, dst = v_b.at[0, :, rows(t * 16, 16), :], rv.at[0, z]
        else:
            src, dst = v_b.at[1, part - 1, rows(t * 16, 16), :], rv.at[1, z, part - 1]
        return copy(src, dst, va_s.at[part, t], va_r.at[part, z], z_dev(t))

    def v_recv(part, t):
        if part == 0:
            src, dst = v_b.at[0, :, rows(t * 16, 16), :], rv.at[0, t]
        else:
            src, dst = v_b.at[1, part - 1, rows(t * 16, 16), :], rv.at[1, t, part - 1]
        return copy(src, dst, va_s.at[part, t], va_r.at[part, t], z_dev(t))

    half_send().start()
    for part, value in ((0, v_high), (1, v_low)):
        v_b[part] = value.reshape(2, 128, ROWS)
    v_f[...] = v.reshape(2, 128, ROWS)
    z_line(lambda t: v_send(0, t).start())
    z_line(lambda t: v_send(1, t).start())
    half_send().wait_recv()
    gh[...] = gp[rows(c * 128, 128)] + gc[...]

    def a_send(t):
        return copy(gh.at[rows(t * 8, 8)], rg.at[q], ga_s.at[t], ga_r.at[q], chip_dev(t))

    def a_recv(t):
        return copy(gh.at[rows(t * 8, 8)], rg.at[t], ga_s.at[t], ga_r.at[t], chip_dev(t))

    chips(lambda t: a_send(t).start())
    rg[q] = gh[rows(q * 8, 8)]
    for part in range(2):
        rv[part, z] = jnp.zeros((2, 16, ROWS), BF16)
    swap(16, q, lambda t: a_recv(t).wait_recv())
    s8[...] = jnp.sum(rg[...], axis=0)

    def gz_send(t):
        return copy(s8, rz.at[z], gz_s.at[t], gz_r.at[z], z_dev(t))

    def gz_recv(t):
        return copy(s8, rz.at[t], gz_s.at[t], gz_r.at[t], z_dev(t))

    z_line(lambda t: gz_send(t).start())
    z_line(lambda t: v_send(2, t).start())
    rz[z] = s8[...]
    swap(8, z, lambda t: gz_recv(t).wait_recv())

    def line(t, core):
        return gram.at[rows(core * 128 + t * 8, 8)]

    gram[rows(c * 128 + q * 8, 8)] = jnp.sum(rz[...], axis=0)

    def g_send(t):
        return copy(line(q, c), line(q, c), gg_s.at[t], gg_r.at[q], chip_dev(t))

    def g_recv(t):
        return copy(line(t, c), line(t, c), gg_s.at[t], gg_r.at[t], chip_dev(t))

    def gf_send(t):
        return copy(line(t, c), line(t, c), gf_s.at[t], gf_r.at[t], core_dev)

    def gf_recv(t):
        return copy(line(t, 1 - c), line(t, 1 - c), gf_s.at[t], gf_r.at[t], core_dev)

    chips(lambda t: g_send(t).start())
    gf_send(q).start()

    for part in range(3):
        swap(8, z, lambda t, part=part: v_recv(part, t).wait_recv())
    others = jnp.sum(rv[0].astype(F32) + rv[1].astype(F32), axis=0)
    mine = v_f[:, rows(z * 16, 16), :] + others
    m_high, m_low = split2(mine)
    own = vall.at[:, rows(z * 16, 16), :]
    own[:, :, :ROWS] = m_high
    own[:, :, ROWS:] = m_low

    def vg_send(t):
        return copy(own, own, vg_s.at[t], vg_r.at[z], z_dev(t))

    def vg_recv(t):
        theirs = vall.at[:, rows(t * 16, 16), :]
        return copy(theirs, theirs, vg_s.at[t], vg_r.at[t], z_dev(t))

    z_line(lambda t: vg_send(t).start())

    def g_pass_on(t):
        g_recv(t).wait_recv()
        gf_send(t).start()

    chips(g_pass_on)

    def d_send(n, t):
        return copy(dd.at[n, rows(t * 8, 8)], rp.at[n, rows(p * 8, 8)], d_s.at[n, t], d_r.at[n, p], half_dev(t))

    def d_recv(n, t):
        return copy(dd.at[n, rows(t * 8, 8)], rp.at[n, rows(t * 8, 8)], d_s.at[n, t], d_r.at[n, t], half_dev(t))

    def deal(n, value):
        for k in range(3):
            tt[n, k] = value[:, k * 128 : (k + 1) * 128]
        even, odd = (
            jnp.concatenate([tt[n, k, pl.ds(o, 16, stride=2), :] for k in range(3)], axis=1)
            for o in range(2)
        )
        gap = jnp.zeros((16, 16), F32)
        for k in range(8):
            cells = slice(48 * k, 48 * k + 48)
            dd[n, pl.ds(k, 16, stride=8), :] = jnp.concatenate(
                [even[:, cells], gap, odd[:, cells], gap], axis=1
            )
        half(lambda t: d_send(n, t).start())
        rp[n, rows(p * 8, 8)] = dd[n, rows(p * 8, 8)]

    def land(n):
        swap(16, p, lambda t: d_recv(n, t).wait_recv())
        table = jnp.concatenate([rp[n, pl.ds(k, 16, stride=8), :] for k in range(8)], axis=0)
        turned = table.T
        for k in range(45):
            results[n, :, k * 128 : (k + 1) * 128] = jnp.concatenate(
                [turned[k : k + 1], turned[64 + k : 65 + k]], axis=0
            )

    deal(0, mine.reshape(32, ROWS))
    each(16, lambda t: gf_recv(t).wait_recv())
    half_send().wait_send()
    swap(16, q, lambda t: g_send(t).wait_send())
    each(16, lambda t: gf_send(t).wait_send())
    a = gram[...]
    gram[...] = (a + a.T) * 0.5
    eliminate(gram)
    l_rows = jnp.concatenate([gram[rows(k * 128 + z * 16, 16), :] for k in range(2)], axis=0)
    l_both = jnp.concatenate(split2(l_rows), axis=0)
    swap(8, z, lambda t: vg_recv(t).wait_recv())
    out = dot(l_both, vall[...].reshape(NORB, 2 * ROWS))
    deal(1, out[:32, :ROWS] + out[32:, :ROWS] + out[:32, ROWS:])
    land(0)
    for group, i, sends in (
        (8, z, (z_send, zg_send, *(functools.partial(v_send, k) for k in range(3)), gz_send, vg_send)),
        (16, p, (p_send, functools.partial(d_send, 0))),
        (16, q, (c_send, a_send)),
    ):
        for send in sends:
            swap(group, i, lambda t, send=send: send(t).wait_send())
    each(16, lambda t: f_send(t).wait_send())
    land(1)
    swap(16, p, lambda t: d_send(1, t).wait_send())


def eliminate(work):
    sub = lax.broadcasted_iota(jnp.int32, (8, 128), 0)
    lane = lax.broadcasted_iota(jnp.int32, (8, 128), 1)
    wide = lambda col: jnp.broadcast_to(col, (8, 128))
    for k in range(8):
        base = 32 * k
        tile, off = base // 128, base % 128
        wk = [
            [work[base + 8 * g : base + 8 * g + 8, 128 * t : 128 * t + 128] for t in range(2)]
            for g in range(4)
        ]
        col = [
            [wide(wk[g][tile][:, off + j : off + j + 1]) if g >= j // 8 else None for g in range(4)]
            for j in range(32)
        ]
        inside = (lane >= off) & (lane < off + 32)
        for g in range(4):
            unit = jnp.where(lane - off == sub + 8 * g, 1.0, 0.0)
            wk[g][tile] = jnp.where(inside, unit, wk[g][tile])
        pivots = [jnp.ones((8, 128), F32) for _ in range(4)]
        for j in range(0, 32, 2):
            gj, sj = j // 8, j % 8
            u, v = col[j], col[j + 1]
            p11 = wide(u[gj][sj : sj + 1, :])
            p21 = wide(u[gj][sj + 1 : sj + 2, :])
            p22 = wide(v[gj][sj + 1 : sj + 2, :])
            det = p11 * p22 - p21 * p21
            r = 1.0 / det
            r11 = 1.0 / p11
            pivots[gj] = jnp.where(sub == sj, p11, jnp.where(sub == sj + 1, det * r11, pivots[gj]))
            q11, q21, q22 = p22 * r, p21 * r, p11 * r
            al, be = [None] * 4, [None] * 4
            for g in range(gj, 4):
                al[g] = u[g] * q11 - v[g] * q21
                be[g] = v[g] * q22 - u[g] * q21
            below = sub > sj + 1
            be[gj] = jnp.where(below, be[gj], 0.0)
            al[gj] = jnp.where(below, al[gj], jnp.where(sub == sj + 1, p21 * r11, 0.0))
            for i in range(j + 2, 32):
                fu = wide(u[i // 8][i % 8 : i % 8 + 1, :])
                fv = wide(v[i // 8][i % 8 : i % 8 + 1, :])
                for g in range(i // 8, 4):
                    col[i][g] = col[i][g] - (al[g] * fu + be[g] * fv)
            for t in range(2):
                one = wide(wk[gj][t][sj : sj + 1, :])
                two = wide(wk[gj][t][sj + 1 : sj + 2, :])
                for g in range(gj, 4):
                    wk[g][t] = wk[g][t] - (al[g] * one + be[g] * two)
        for g in range(4):
            scale = lax.rsqrt(pivots[g])
            for t in range(2):
                wk[g][t] = wk[g][t] * scale
        u = jnp.concatenate([jnp.concatenate(wk[g], axis=1) for g in range(4)], axis=0)
        lanes = lax.broadcasted_iota(jnp.int32, (32, 256), 1)
        work[base : base + 32, :] = jnp.where(lanes < base + 32, u, 0.0)
        if k < 7:
            u_high, u_low = split2(u)
            one = jnp.concatenate([u_high, u_low, u_high], axis=0)
            two = jnp.concatenate([u_high, u_high, u_low], axis=0)
            edge = base + 32
            start = edge // 128 * 128
            change = dot(one[:, start:].T, two)[edge - start :]
            rest = work[edge:, :]
            lanes = lax.broadcasted_iota(jnp.int32, rest.shape, 1)
            rest = jnp.where((lanes >= base) & (lanes < edge), 0.0, rest)
            work[edge:, :] = rest - change


VM = pl.BlockSpec(memory_space=pltpu.VMEM)
ANY = pl.BlockSpec(memory_space=pl.ANY)
DMA = pltpu.SemaphoreType.DMA


def call(kernel, args, outs, scratch, number, name):
    return pl.pallas_call(
        kernel,
        out_shape=[jax.ShapeDtypeStruct(s, d) for s, d in outs],
        in_specs=[ANY] * len(args),
        out_specs=[VM] * len(outs),
        scratch_shapes=scratch,
        compiler_params=pltpu.CompilerParams(
            vmem_limit_bytes=60 * 1024 * 1024, collective_id=number, has_side_effects=True
        ),
        name=name,
    )(*args)


def on_device(orbitals, occupation):
    planes = orbitals.reshape(2, 10, NY, NZ)
    vm = pltpu.VMEM
    both = call(
        main_kernel, (planes, orbitals, occupation, permutations(), *tables()),
        (((2, 2, HALF), F32),),
        [vm((2, 10, NY, NZ), BF16), vm((2, HALF), BF16), vm((2,), BF16),
         vm((128, 128), F32), vm((2, 2, NY, 128), F32), vm((16, 8, 128), F32), vm((128, 128), F32), vm((128, 128), F32), vm((NORB, 512), BF16), vm((128, 3 * MODES), BF16),
         vm((128, 128), BF16), vm((MODES, 1024), BF16), vm((32, 128), F32), DMA((8,)),
         vm((2, NORB, 768), BF16), vm((NORB, ROWS), BF16), vm((128, 128), F32), vm((128, 128), F32),
         vm((2, ROWS, 768), F32), vm((ROWS, MODES), F32), vm((ROWS, 128), F32),
         vm((2, 128, ROWS), F32), vm((2, 2, 128, ROWS), BF16), vm((NORB, NORB), F32),
         vm((128, NORB), F32), vm((128, NORB), F32), vm((16, 8, NORB), F32),
         vm((2, 8, 2, 16, ROWS), BF16), vm((8, NORB), F32), vm((8, 8, NORB), F32),
         vm((NORB, NORB), F32), vm((2, 128, 2 * ROWS), BF16), vm((2, 3, 32, 128), F32),
         vm((2, 128, 128), F32), vm((2, 128, 128), F32),
         DMA((8,)), DMA((8,)), DMA((16,)), DMA((16,)), DMA((16,)), DMA((16,)), DMA((16,)), DMA((16,)),
         DMA((8,)), DMA((8,)), DMA, DMA, DMA((16,)), DMA((16,)), DMA((3, 8)), DMA((3, 8)),
         DMA((8,)), DMA((8,)), DMA((16,)), DMA((16,)), DMA((16,)), DMA((16,)),
         DMA((8,)), DMA((8,)), DMA((2, 16)), DMA((2, 16))],
        0, "exchange",
    )[0]
    return -both[0], -both[1]


def solution(mesh):
    torus = Mesh(mesh.devices.reshape(2, 8, 4, 2, mesh.shape["grid"]), AXES)
    return jax.shard_map(
        on_device,
        mesh=torus,
        in_specs=(P(ORB, "h"), P(ORB)),
        out_specs=(P(ORB, "h"), P(ORB, "h")),
        check_vma=False,
    )
```

```python
import functools
import math

import jax
import jax.numpy as jnp
import numpy as np
from jax import lax
from jax.experimental import pallas as pl
from jax.experimental.pallas import tpu as pltpu
from jax.sharding import Mesh
from jax.sharding import PartitionSpec as P

NX = 20
NY = 24
NZ = 24
NORB = 256
NPTS = 11520
HALF = NPTS // 2
MODES = 512
ROWS = 384
AXES = ("xl", "z", "y", "c", "h")
ORB = ("xl", "z", "y", "c")
MESH = pl.DeviceIdType.MESH
F32 = jnp.float32
BF16 = jnp.bfloat16


def rounded(a):
    return np.asarray(a, np.float32).astype(jnp.bfloat16).astype(np.float32)


def hartley_table(length):
    index = np.arange(length)
    angle = 2.0 * math.pi / length * (index[:, None] * index[None, :] % length)
    return rounded(np.cos(angle) + np.sin(angle))


def signed_square(length):
    index = np.arange(length)
    signed = np.where(index <= length // 2, index, index - length)
    return (2.0 * math.pi * signed / length) ** 2


def coulomb_kernel():
    total = (
        signed_square(NX)[:, None, None]
        + signed_square(NY)[None, :, None]
        + signed_square(NZ)[None, None, :]
    )
    return np.where(total > 0, 1.0 / np.where(total > 0, total, 1.0), 0.0) / NPTS


def two_parts(a):
    high = rounded(a)
    return high, rounded(a - high)


def tables():
    cx, cy, cz = hartley_table(NX), hartley_table(NY), hartley_table(NZ)
    kernel = coulomb_kernel()
    ac = NX * NZ
    tx = np.zeros((128, MODES), np.float32)
    tx[:NX, :ac] = np.repeat(cx, NZ, axis=1)
    tz = np.zeros((128, MODES), np.float32)
    tz[:NZ, :ac] = np.tile(cz, (1, NX))
    ty = np.zeros((128, 128), np.float32)
    tk = np.zeros((128, MODES), np.float32)
    k_high, k_low = two_parts(kernel.transpose(1, 0, 2).reshape(NY, ac))
    for at, part in ((0, k_high), (32, k_high), (64, k_low)):
        ty[:NY, at : at + NY] = cy
        tk[at : at + NY, :ac] = part
    phi = np.einsum("ax,cz->acxz", cx, cz).reshape(ac, NX, NZ)
    right = np.zeros((MODES, 2, 256), np.float32)
    for h in range(2):
        right[:ac, h, :240] = phi[:, 10 * h : 10 * h + 10].reshape(ac, 240)
    r_high, r_low = two_parts(right.reshape(MODES, 512))
    bf = lambda a: jnp.asarray(a, BF16)
    three = np.concatenate([tx, tz, tk], axis=1)
    return bf(three), bf(ty), bf(np.concatenate([r_high, r_low], axis=1)), jnp.asarray(ty[:32], F32)


def permutations():
    true = np.arange(NORB).reshape(2, 8, 8, 2)
    order_a = true.transpose(0, 2, 1, 3).reshape(-1)
    order_b = true.transpose(1, 3, 0, 2).reshape(-1)
    eye = np.eye(NORB, dtype=np.float32)
    return jnp.asarray(np.concatenate([eye[:, order_a], eye[:, order_b]], axis=1), BF16)


def split2(a):
    high = a.astype(BF16)
    return high, (a - high.astype(F32)).astype(BF16)


def dot(a, b, dims=(1, 0)):
    return lax.dot_general(
        a, b, (((dims[0],), (dims[1],)), ((), ())), preferred_element_type=F32
    )


def me():
    return tuple(lax.axis_index(a) for a in AXES)


def of_plane(pid, z):
    return ((pid // 8) % 2, z, (pid // 2) % 4, pid % 2, pid // 16)


def copy(src, dst, send_sem, recv_sem, device):
    return pltpu.make_async_remote_copy(
        src_ref=src, dst_ref=dst, send_sem=send_sem, recv_sem=recv_sem,
        device_id=device, device_id_type=MESH,
    )


def rows(start, size):
    return pl.ds(pl.multiple_of(start, size), size)


def each(count, body):
    lax.fori_loop(0, count, lambda i, carry: (body(i), carry)[1], 0)


def swap(n, i, body):
    each(n - 1, lambda d: body((i + d + 1) % n))


Z_ORDER = (4, 3, 5, 2, 6, 1, 7)
CHIP_ORDER = (
    (2, 2), (2, 1), (2, 3), (1, 2), (3, 2), (1, 1), (1, 3), (3, 1), (3, 3),
    (2, 0), (0, 2), (1, 0), (3, 0), (0, 1), (0, 3),
)
HALF_ORDER = tuple((a, b, k) for a, b in ((1, 2), (1, 1), (1, 3), (0, 2), (1, 0), (0, 1), (0, 3)) for k in range(2)) + ((0, 0, 1),)


def greet(barrier, n, i, device):
    swap(n, i, lambda t: pl.semaphore_signal(barrier, inc=1, device_id=device(t), device_id_type=MESH))
    return n - 1


def shifted(a, factor, shift):
    return lax.shift_right_logical(a * factor, shift)


def main_kernel(
    st_any, raw_any, oc_any, perm_any, t_any, ty_any, right_any, cy_any, results,
    st, raw, oc, s1, by_y, s2, cells, turned_cells, perm, t3, ty, right, cy, in_s,
    o1, o2, r1, r2, green, left, y_rows, v_f, v_b, gp, gc, gh, rg, rv, s8, rz,
    gram, vall, tt, dd, rp,
    za_s, za_r, pa_s, pa_r, cg_s, cg_r, cf_s, cf_r, zg_s, zg_r,
    gc_s, gc_r, ga_s, ga_r, va_s, va_r, gz_s, gz_r, gg_s, gg_r, gf_s, gf_r,
    vg_s, vg_r, d_s, d_r,
):
    xl, z, y, c, h = me()
    p = xl * 8 + y * 2 + c
    q = h * 8 + xl * 4 + y
    z_dev = lambda t: (xl, t, y, c, h)
    half_dev = lambda t: of_plane(h * 16 + t, z)
    chip_dev = lambda t: ((t // 4) % 2, z, t % 4, c, t // 8)
    core_dev = (xl, z, y, 1 - c, h)

    def z_line(body):
        for d in Z_ORDER:
            body((z + d) % 8)

    def chips(body):
        for dx, dy in CHIP_ORDER:
            body((q // 4 + dx) % 4 * 4 + (y + dy) % 4)

    def half(body):
        for dx, dy, dc in HALF_ORDER:
            body((xl + dx) % 2 * 8 + (y + dy) % 4 * 2 + (c + dc) % 2)

    barrier = pltpu.get_barrier_semaphore()
    greeted = greet(barrier, 8, z, z_dev) + greet(barrier, 16, p, half_dev)
    greeted += greet(barrier, 16, q, chip_dev)
    pl.semaphore_signal(barrier, inc=1, device_id=core_dev, device_id_type=MESH)

    held = (
        (raw_any, raw), (oc_any, oc), (st_any, st), (t_any, t3), (ty_any, ty), (cy_any, cy),
        (right_any, right), (perm_any, perm),
    )
    held = [pltpu.make_async_copy(a, b, in_s.at[k]) for k, (a, b) in enumerate(held)]
    for one in held:
        one.start()
    perm_a, perm_b = perm.at[:, :NORB], perm.at[:, NORB:]
    tx, tz, tk = (t3.at[:, k * MODES : (k + 1) * MODES] for k in range(3))
    rh, rl = right.at[:, :512], right.at[:, 512:]
    for one in held[:3]:
        one.wait()
    cells[...] = jnp.zeros_like(cells)
    for k in range(45):
        pair = raw[:, k * 128 : (k + 1) * 128].astype(F32)
        for o in range(2):
            cells[64 * o + k : 64 * o + k + 1, :] = pair[o : o + 1]
    for o in range(2):
        cells[64 * o + 45 : 64 * o + 46, :] = jnp.broadcast_to(oc[...].astype(F32)[None, o : o + 1], (1, 128))
    turned_cells[...] = cells[...].T
    for k in range(16):
        s2[k] = turned_cells[pl.ds(k, 8, stride=16), :]
    s1[...] = jnp.zeros_like(s1)
    for o in range(2):
        wide_rows = jnp.concatenate(
            [st[o, k].astype(F32) for k in range(10)] + [jnp.zeros((NY, 16), F32)], axis=1
        )
        for part in range(2):
            by_y[o, part] = wide_rows[:, 128 * part : 128 * part + 128]
            for t in range(3):
                s1[pl.ds(8 * o + 2 * t + part, 8, stride=16), :] = by_y[o, part, pl.ds(t, 8, stride=3), :]

    row = lax.broadcasted_iota(jnp.int32, (ROWS, 128), 0)
    lane = lax.broadcasted_iota(jnp.int32, (ROWS, 128), 1)
    zz = shifted(row, 1366, 16)
    s = row - zz * 48
    cell = h * HALF + s * 128 + zz * 16 + p
    x = shifted(cell, 7282, 22)
    yz = cell - x * (NY * NZ)
    y_cell = shifted(yz, 2731, 16)
    z_cell = yz - y_cell * NZ
    hot = lambda a: jnp.where(a == lane, 1.0, 0.0).astype(BF16)
    middle = (lane >= 32) & (lane < 64)

    def green_part(t):
        k_high, k_low = split2(y_rows[...] * cy[pl.ds(z * 3 + t, 1), :])
        mix = jnp.where(middle, k_low.astype(F32), k_high.astype(F32)).astype(BF16)
        l_high, l_low = split2(left[...] * dot(mix, tk[...]))
        g = dot(l_high, rh[...]) + dot(l_low, rh[...]) + dot(l_high, rl[...])
        for hh in range(2):
            green[hh, :, t * 256 : (t + 1) * 256] = g[:, hh * 256 : (hh + 1) * 256]

    pl.semaphore_wait(barrier, greeted + 1)

    def z_send(t):
        return copy(s1.at[rows(t * 16, 16)], r1.at[rows(z * 16, 16)], za_s.at[t], za_r.at[z], z_dev(t))

    def z_recv(t):
        return copy(s1.at[rows(t * 16, 16)], r1.at[rows(t * 16, 16)], za_s.at[t], za_r.at[t], z_dev(t))

    def p_send(t):
        return copy(s2.at[t], r2.at[rows(p * 8, 8)], pa_s.at[t], pa_r.at[p], half_dev(t))

    def p_recv(t):
        return copy(s2.at[t], r2.at[rows(t * 8, 8)], pa_s.at[t], pa_r.at[t], half_dev(t))

    half(lambda t: p_send(t).start())
    z_line(lambda t: z_send(t).start())
    r1[rows(z * 16, 16)] = s1[rows(z * 16, 16)]
    r2[rows(p * 8, 8)] = s2[p]
    for one in held[3:]:
        one.wait()
    left[...] = dot(hot(jnp.where(s < 45, x, 127)), tx[...]) * dot(hot(z_cell), tz[...])
    y_rows[...] = dot(hot(y_cell), ty[...])
    green_part(0)
    swap(16, p, lambda t: p_recv(t).wait_recv())
    by_row = [r2[pl.ds(k, 16, stride=8), :] for k in range(8)]
    o2[rows(z * 32, 32), :] = jnp.concatenate(
        [jnp.concatenate([b[:, 64 * o : 64 * o + 48] for b in by_row], axis=1) for o in range(2)], axis=0
    ).astype(BF16)

    def zg_send(t):
        mine = o2.at[rows(z * 32, 32)]
        return copy(mine, mine, zg_s.at[t], zg_r.at[z], z_dev(t))

    def zg_recv(t):
        theirs = o2.at[rows(t * 32, 32)]
        return copy(theirs, theirs, zg_s.at[t], zg_r.at[t], z_dev(t))

    z_line(lambda t: zg_send(t).start())
    swap(8, z, lambda t: z_recv(t).wait_recv())
    for t in range(3):
        o1[h, rows(p * 16, 16), t * 256 : (t + 1) * 256] = jnp.concatenate(
            [r1[pl.ds(2 * t + k, 16, stride=8), :] for k in range(2)], axis=1
        ).astype(BF16)

    def block(t, core):
        return o1.at[t // 8, rows(((t // 4) % 2 * 8 + t % 4 * 2 + core) * 16, 16)]

    def c_send(t):
        return copy(block(q, c), block(q, c), cg_s.at[t], cg_r.at[q], chip_dev(t))

    def c_recv(t):
        return copy(block(t, c), block(t, c), cg_s.at[t], cg_r.at[t], chip_dev(t))

    def f_send(t):
        return copy(block(t, c), block(t, c), cf_s.at[t], cf_r.at[t], core_dev)

    def f_recv(t):
        return copy(block(t, 1 - c), block(t, 1 - c), cf_s.at[t], cf_r.at[t], core_dev)

    chips(lambda t: c_send(t).start())
    f_send(q).start()
    green_part(1)
    green_part(2)

    def pass_on(t):
        c_recv(t).wait_recv()
        f_send(t).start()

    chips(pass_on)
    swap(8, z, lambda t: zg_recv(t).wait_recv())
    o_rows = dot(perm_b[...], o2[...])
    o_b = o_rows.astype(BF16)
    w = (o_rows * o_rows[:, 45:46]).astype(BF16).T
    each(16, lambda t: f_recv(t).wait_recv())

    v = jnp.zeros((NORB, ROWS), F32)
    for hh in range(2):
        orb = dot(perm_a[...], o1[hh]).astype(BF16)
        m_high, m_low = split2(green[hh] * dot(w, orb))
        v = v + dot(orb, m_high, (1, 1)) + dot(orb, m_low, (1, 1))
    v_high, v_low = split2(v)
    gp[...] = (dot(o_b, v_high, (1, 1)) + dot(o_b, v_low, (1, 1))) * (1.0 / NPTS)

    def half_send():
        other = gp.at[rows((1 - c) * 128, 128)]
        return copy(other, gc, gc_s, gc_r, core_dev)

    def v_send(part, t):
        if part == 0:
            src, dst = v_b.at[0, :, rows(t * 16, 16), :], rv.at[0, z]
        else:
            src, dst = v_b.at[1, part - 1, rows(t * 16, 16), :], rv.at[1, z, part - 1]
        return copy(src, dst, va_s.at[part, t], va_r.at[part, z], z_dev(t))

    def v_recv(part, t):
        if part == 0:
            src, dst = v_b.at[0, :, rows(t * 16, 16), :], rv.at[0, t]
        else:
            src, dst = v_b.at[1, part - 1, rows(t * 16, 16), :], rv.at[1, t, part - 1]
        return copy(src, dst, va_s.at[part, t], va_r.at[part, t], z_dev(t))

    half_send().start()
    for part, value in ((0, v_high), (1, v_low)):
        v_b[part] = value.reshape(2, 128, ROWS)
    v_f[...] = v.reshape(2, 128, ROWS)
    z_line(lambda t: v_send(0, t).start())
    z_line(lambda t: v_send(1, t).start())
    half_send().wait_recv()
    gh[...] = gp[rows(c * 128, 128)] + gc[...]

    def a_send(t):
        return copy(gh.at[rows(t * 8, 8)], rg.at[q], ga_s.at[t], ga_r.at[q], chip_dev(t))

    def a_recv(t):
        return copy(gh.at[rows(t * 8, 8)], rg.at[t], ga_s.at[t], ga_r.at[t], chip_dev(t))

    chips(lambda t: a_send(t).start())
    rg[q] = gh[rows(q * 8, 8)]
    for part in range(2):
        rv[part, z] = jnp.zeros((2, 16, ROWS), BF16)
    swap(16, q, lambda t: a_recv(t).wait_recv())
    s8[...] = jnp.sum(rg[...], axis=0)

    def gz_send(t):
        return copy(s8, rz.at[z], gz_s.at[t], gz_r.at[z], z_dev(t))

    def gz_recv(t):
        return copy(s8, rz.at[t], gz_s.at[t], gz_r.at[t], z_dev(t))

    z_line(lambda t: gz_send(t).start())
    z_line(lambda t: v_send(2, t).start())
    rz[z] = s8[...]
    swap(8, z, lambda t: gz_recv(t).wait_recv())

    def line(t, core):
        return gram.at[rows(core * 128 + t * 8, 8)]

    gram[rows(c * 128 + q * 8, 8)] = jnp.sum(rz[...], axis=0)

    def g_send(t):
        return copy(line(q, c), line(q, c), gg_s.at[t], gg_r.at[q], chip_dev(t))

    def g_recv(t):
        return copy(line(t, c), line(t, c), gg_s.at[t], gg_r.at[t], chip_dev(t))

    def gf_send(t):
        return copy(line(t, c), line(t, c), gf_s.at[t], gf_r.at[t], core_dev)

    def gf_recv(t):
        return copy(line(t, 1 - c), line(t, 1 - c), gf_s.at[t], gf_r.at[t], core_dev)

    chips(lambda t: g_send(t).start())
    gf_send(q).start()

    for part in range(3):
        swap(8, z, lambda t, part=part: v_recv(part, t).wait_recv())
    others = jnp.sum(rv[0].astype(F32) + rv[1].astype(F32), axis=0)
    mine = v_f[:, rows(z * 16, 16), :] + others
    m_high, m_low = split2(mine)
    own = vall.at[:, rows(z * 16, 16), :]
    own[:, :, :ROWS] = m_high
    own[:, :, ROWS:] = m_low

    def vg_send(t):
        return copy(own, own, vg_s.at[t], vg_r.at[z], z_dev(t))

    def vg_recv(t):
        theirs = vall.at[:, rows(t * 16, 16), :]
        return copy(theirs, theirs, vg_s.at[t], vg_r.at[t], z_dev(t))

    z_line(lambda t: vg_send(t).start())

    def g_pass_on(t):
        g_recv(t).wait_recv()
        gf_send(t).start()


    def d_send(n, t):
        return copy(dd.at[n, rows(t * 8, 8)], rp.at[n, rows(p * 8, 8)], d_s.at[n, t], d_r.at[n, p], half_dev(t))

    def d_recv(n, t):
        return copy(dd.at[n, rows(t * 8, 8)], rp.at[n, rows(t * 8, 8)], d_s.at[n, t], d_r.at[n, t], half_dev(t))

    def deal(n, value):
        for k in range(3):
            tt[n, k] = value[:, k * 128 : (k + 1) * 128]
        even, odd = (
            jnp.concatenate([tt[n, k, pl.ds(o, 16, stride=2), :] for k in range(3)], axis=1)
            for o in range(2)
        )
        gap = jnp.zeros((16, 16), F32)
        for k in range(8):
            cells = slice(48 * k, 48 * k + 48)
            dd[n, pl.ds(k, 16, stride=8), :] = jnp.concatenate(
                [even[:, cells], gap, odd[:, cells], gap], axis=1
            )
        half(lambda t: d_send(n, t).start())
        rp[n, rows(p * 8, 8)] = dd[n, rows(p * 8, 8)]

    def land(n):
        swap(16, p, lambda t: d_recv(n, t).wait_recv())
        table = jnp.concatenate([rp[n, pl.ds(k, 16, stride=8), :] for k in range(8)], axis=0)
        turned = table.T
        for k in range(45):
            results[n, :, k * 128 : (k + 1) * 128] = jnp.concatenate(
                [turned[k : k + 1], turned[64 + k : 65 + k]], axis=0
            )

    deal(0, mine.reshape(32, ROWS))
    chips(g_pass_on)
    each(16, lambda t: gf_recv(t).wait_recv())
    half_send().wait_send()
    swap(16, q, lambda t: g_send(t).wait_send())
    each(16, lambda t: gf_send(t).wait_send())
    a = gram[...]
    gram[...] = (a + a.T) * 0.5
    eliminate(gram)
    l_rows = jnp.concatenate([gram[rows(k * 128 + z * 16, 16), :] for k in range(2)], axis=0)
    l_both = jnp.concatenate(split2(l_rows), axis=0)
    swap(8, z, lambda t: vg_recv(t).wait_recv())
    out = dot(l_both, vall[...].reshape(NORB, 2 * ROWS))
    deal(1, out[:32, :ROWS] + out[32:, :ROWS] + out[:32, ROWS:])
    land(0)
    for group, i, sends in (
        (8, z, (z_send, zg_send, *(functools.partial(v_send, k) for k in range(3)), gz_send, vg_send)),
        (16, p, (p_send, functools.partial(d_send, 0))),
        (16, q, (c_send, a_send)),
    ):
        for send in sends:
            swap(group, i, lambda t, send=send: send(t).wait_send())
    each(16, lambda t: f_send(t).wait_send())
    land(1)
    swap(16, p, lambda t: d_send(1, t).wait_send())


def eliminate(work):
    sub = lax.broadcasted_iota(jnp.int32, (8, 128), 0)
    lane = lax.broadcasted_iota(jnp.int32, (8, 128), 1)
    wide = lambda col: jnp.broadcast_to(col, (8, 128))
    for k in range(8):
        base = 32 * k
        tile, off = base // 128, base % 128
        wk = [
            [work[base + 8 * g : base + 8 * g + 8, 128 * t : 128 * t + 128] for t in range(2)]
            for g in range(4)
        ]
        col = [
            [wide(wk[g][tile][:, off + j : off + j + 1]) if g >= j // 8 else None for g in range(4)]
            for j in range(32)
        ]
        inside = (lane >= off) & (lane < off + 32)
        for g in range(4):
            unit = jnp.where(lane - off == sub + 8 * g, 1.0, 0.0)
            wk[g][tile] = jnp.where(inside, unit, wk[g][tile])
        pivots = [jnp.ones((8, 128), F32) for _ in range(4)]
        for j in range(0, 32, 2):
            gj, sj = j // 8, j % 8
            u, v = col[j], col[j + 1]
            p11 = wide(u[gj][sj : sj + 1, :])
            p21 = wide(u[gj][sj + 1 : sj + 2, :])
            p22 = wide(v[gj][sj + 1 : sj + 2, :])
            det = p11 * p22 - p21 * p21
            r = 1.0 / det
            r11 = 1.0 / p11
            pivots[gj] = jnp.where(sub == sj, p11, jnp.where(sub == sj + 1, det * r11, pivots[gj]))
            q11, q21, q22 = p22 * r, p21 * r, p11 * r
            al, be = [None] * 4, [None] * 4
            for g in range(gj, 4):
                al[g] = u[g] * q11 - v[g] * q21
                be[g] = v[g] * q22 - u[g] * q21
            below = sub > sj + 1
            be[gj] = jnp.where(below, be[gj], 0.0)
            al[gj] = jnp.where(below, al[gj], jnp.where(sub == sj + 1, p21 * r11, 0.0))
            for i in range(j + 2, 32):
                fu = wide(u[i // 8][i % 8 : i % 8 + 1, :])
                fv = wide(v[i // 8][i % 8 : i % 8 + 1, :])
                for g in range(i // 8, 4):
                    col[i][g] = col[i][g] - (al[g] * fu + be[g] * fv)
            for t in range(2):
                one = wide(wk[gj][t][sj : sj + 1, :])
                two = wide(wk[gj][t][sj + 1 : sj + 2, :])
                for g in range(gj, 4):
                    wk[g][t] = wk[g][t] - (al[g] * one + be[g] * two)
        for g in range(4):
            scale = lax.rsqrt(pivots[g])
            for t in range(2):
                wk[g][t] = wk[g][t] * scale
        u = jnp.concatenate([jnp.concatenate(wk[g], axis=1) for g in range(4)], axis=0)
        lanes = lax.broadcasted_iota(jnp.int32, (32, 256), 1)
        work[base : base + 32, :] = jnp.where(lanes < base + 32, u, 0.0)
        if k < 7:
            u_high, u_low = split2(u)
            one = jnp.concatenate([u_high, u_low, u_high], axis=0)
            two = jnp.concatenate([u_high, u_high, u_low], axis=0)
            edge = base + 32
            start = edge // 128 * 128
            change = dot(one[:, start:].T, two)[edge - start :]
            rest = work[edge:, :]
            lanes = lax.broadcasted_iota(jnp.int32, rest.shape, 1)
            rest = jnp.where((lanes >= base) & (lanes < edge), 0.0, rest)
            work[edge:, :] = rest - change


VM = pl.BlockSpec(memory_space=pltpu.VMEM)
ANY = pl.BlockSpec(memory_space=pl.ANY)
DMA = pltpu.SemaphoreType.DMA


def call(kernel, args, outs, scratch, number, name):
    return pl.pallas_call(
        kernel,
        out_shape=[jax.ShapeDtypeStruct(s, d) for s, d in outs],
        in_specs=[ANY] * len(args),
        out_specs=[VM] * len(outs),
        scratch_shapes=scratch,
        compiler_params=pltpu.CompilerParams(
            vmem_limit_bytes=60 * 1024 * 1024, collective_id=number, has_side_effects=True
        ),
        name=name,
    )(*args)


def on_device(orbitals, occupation):
    planes = orbitals.reshape(2, 10, NY, NZ)
    vm = pltpu.VMEM
    both = call(
        main_kernel, (planes, orbitals, occupation, permutations(), *tables()),
        (((2, 2, HALF), F32),),
        [vm((2, 10, NY, NZ), BF16), vm((2, HALF), BF16), vm((2,), BF16),
         vm((128, 128), F32), vm((2, 2, NY, 128), F32), vm((16, 8, 128), F32), vm((128, 128), F32), vm((128, 128), F32), vm((NORB, 512), BF16), vm((128, 3 * MODES), BF16),
         vm((128, 128), BF16), vm((MODES, 1024), BF16), vm((32, 128), F32), DMA((8,)),
         vm((2, NORB, 768), BF16), vm((NORB, ROWS), BF16), vm((128, 128), F32), vm((128, 128), F32),
         vm((2, ROWS, 768), F32), vm((ROWS, MODES), F32), vm((ROWS, 128), F32),
         vm((2, 128, ROWS), F32), vm((2, 2, 128, ROWS), BF16), vm((NORB, NORB), F32),
         vm((128, NORB), F32), vm((128, NORB), F32), vm((16, 8, NORB), F32),
         vm((2, 8, 2, 16, ROWS), BF16), vm((8, NORB), F32), vm((8, 8, NORB), F32),
         vm((NORB, NORB), F32), vm((2, 128, 2 * ROWS), BF16), vm((2, 3, 32, 128), F32),
         vm((2, 128, 128), F32), vm((2, 128, 128), F32),
         DMA((8,)), DMA((8,)), DMA((16,)), DMA((16,)), DMA((16,)), DMA((16,)), DMA((16,)), DMA((16,)),
         DMA((8,)), DMA((8,)), DMA, DMA, DMA((16,)), DMA((16,)), DMA((3, 8)), DMA((3, 8)),
         DMA((8,)), DMA((8,)), DMA((16,)), DMA((16,)), DMA((16,)), DMA((16,)),
         DMA((8,)), DMA((8,)), DMA((2, 16)), DMA((2, 16))],
        0, "exchange",
    )[0]
    return -both[0], -both[1]


def solution(mesh):
    torus = Mesh(mesh.devices.reshape(2, 8, 4, 2, mesh.shape["grid"]), AXES)
    return jax.shard_map(
        on_device,
        mesh=torus,
        in_specs=(P(ORB, "h"), P(ORB)),
        out_specs=(P(ORB, "h"), P(ORB, "h")),
        check_vma=False,
    )
```
